32 devices in a mesh: tm: 16 (over z, x, core), grp: 2 (over y).
Axes of the slice: x: 2, y: 2, z: 4, core: 2. Of those that a mesh axis runs over, the one named last changes fastest.
Arguments:
- residual: float32 [16, 2, 3072], P('tm', 'grp'), may hold values from -6 to 6
- weight: float32 [16, 2, 3072], P('tm', 'grp'), may hold values from 0.25 to 4
- source_part: float32 [5, 16, 2, 3072], P(None, 'tm', 'grp'), may hold values from -2.5 to 2.5
- source_index: int32 [16, 2, 3072], P('tm', 'grp'), may hold values from 0 to 4095
- source_delta: float32 [5, 16, 4096], P(None, 'tm'), may hold values from -6 to 6
- attitude_part: float32 [3, 16, 2, 3072], P(None, 'tm', 'grp'), may hold values from -6 to 6
- spline_phase: float32 [16, 2, 3072], P('tm', 'grp'), may hold values from 0 to 1
- knot_index: int32 [16, 2, 3072], P('tm', 'grp'), may hold values from 0 to 1535, as said below
- calib_part: float32 [6, 16, 2, 3072], P(None, 'tm', 'grp'), may hold values from -6 to 6
- calib_index: int32 [16, 2, 3072], P('tm', 'grp'), may hold values from 0 to 2047
- global_part: float32 [4, 16, 2, 3072], P(None, 'tm', 'grp'), may hold values from -6 to 6
Outputs:
- residual_new: float32 [16, 2, 3072], P('tm', 'grp')
- attitude_step: float32 [3, 1536], P(None, 'tm')
- calib_step: float32 [6, 2048], replicated
- global_step: float32 [4], replicated
The draws below stay inside these ranges and needn't reach their ends.
Inputs may be any that keep to these rules, and one draw needn't show every extreme that they name: `knot_index`: observation r of interval t (in any group) lies in knot interval t * 96 + 4 * (r // 128) + j for some j in 0 .. 3.
All inputs are finite; a program needn't handle non-finite values.
Results may differ from the reference program's by a relative error of at most 0.00012.
Values sent between devices are 32-bit elements; how exact they have to be, the bound alone decides.
A program may use at most 128 MiB of HBM per device.

```python
import math
import jax
import jax.numpy as jnp
from jax import lax

ROWS_DEV = 3072
TILE = 128
KPT = 4
SRC_DEV = 4096
UNITS = 2048
CPAR = 6
GPAR = 4
ATT_SWEEPS = 4
ND = 96
INTERVALS = 16
GROUPS = 2


def draw_knot_index(key, part):
    within = jax.random.randint(key, (INTERVALS, GROUPS, ROWS_DEV), 0, KPT, dtype=jnp.int32)
    tile_base = KPT * (jnp.arange(ROWS_DEV, dtype=jnp.int32) // TILE)
    interval_base = jnp.arange(INTERVALS, dtype=jnp.int32) * ND
    return (interval_base[:, None, None] + tile_base[None, None, :] + within).astype(jnp.int32)


def with_ends(drawn, rng, low, top_value):
    longest = drawn.shape.index(max(drawn.shape))
    spots = []
    for shift in (0, 1):
        where = [jax.random.randint(jax.random.fold_in(rng, axis), (), 0, length) for axis, length in enumerate(drawn.shape)]
        where[longest] = (where[longest] + shift) % drawn.shape[longest]
        spots.append(tuple(where))
    return drawn.at[spots[0]].set(low).at[spots[1]].set(top_value)


def level_of(stream_key, shape, cuts, least, top_value):
    loudness, own = 1.0, jax.random.fold_in(stream_key, 6)
    for dim, parts in cuts:
        steps = jnp.exp(jax.random.uniform(jax.random.fold_in(own, dim), (parts,), jnp.float32, least / len(cuts), top_value / len(cuts)))
        loudness = loudness * jnp.repeat(steps, shape[dim] // parts).reshape([-1 if axis == dim else 1 for axis in range(len(shape))])
    return loudness


def scatter_about(own_key, dims, scale, limit, split=(), kind=jnp.bfloat16):
    array = scale * jax.random.normal(own_key, dims, jnp.float32)
    if split:
        array = array * level_of(own_key, dims, split, -0.22, 0.18)
    return jnp.clip(array, -limit, limit).astype(kind)


def setup_inputs(seed: int = 0) -> dict:
    streams_of = jax.random.split(jax.random.key(seed), 12)
    return {
        "residual": scatter_about(streams_of[0], (INTERVALS, GROUPS, ROWS_DEV), 1.0, 6.0, ((0, 16), (1, 2)), jnp.float32),
        "weight": jnp.clip(jnp.exp(math.log(4.0) - 2.7725887 * jax.random.uniform(streams_of[1], (INTERVALS, GROUPS, ROWS_DEV), jnp.float32) ** level_of(streams_of[1], (INTERVALS, GROUPS, ROWS_DEV), ((0, 16), (1, 2)), -0.2, 0.2)), 0.25, 4.0),
        "source_part": scatter_about(streams_of[2], (5, INTERVALS, GROUPS, ROWS_DEV), 5 ** -0.5, 2.5, ((1, 16), (2, 2)), jnp.float32),
        "source_index": with_ends(jax.random.randint(streams_of[3], (INTERVALS, GROUPS, ROWS_DEV), 0, SRC_DEV), jax.random.fold_in(streams_of[3], 1), 0, SRC_DEV - 1).astype(jnp.int32),
        "source_delta": scatter_about(streams_of[4], (5, INTERVALS, SRC_DEV), 1.0, 6.0, ((1, 16),), jnp.float32),
        "attitude_part": scatter_about(streams_of[5], (3, INTERVALS, GROUPS, ROWS_DEV), 1.0, 6.0, ((1, 16), (2, 2)), jnp.float32),
        "spline_phase": jnp.clip(1.0 * jax.random.uniform(streams_of[6], (INTERVALS, GROUPS, ROWS_DEV), jnp.float32) ** level_of(streams_of[6], (INTERVALS, GROUPS, ROWS_DEV), ((0, 16), (1, 2)), -0.2, 0.2), 0.0, 1.0),
        "knot_index": draw_knot_index(jax.random.fold_in(streams_of[11], 71), 0),
        "calib_part": scatter_about(streams_of[8], (CPAR, INTERVALS, GROUPS, ROWS_DEV), 1.0, 6.0, ((1, 16), (2, 2)), jnp.float32),
        "calib_index": with_ends(jax.random.randint(streams_of[9], (INTERVALS, GROUPS, ROWS_DEV), 0, UNITS), jax.random.fold_in(streams_of[9], 1), 0, UNITS - 1).astype(jnp.int32),
        "global_part": scatter_about(streams_of[10], (GPAR, INTERVALS, GROUPS, ROWS_DEV), 1.0, 6.0, ((1, 16), (2, 2)), jnp.float32),
    }


OMEGA = 0.6
RIDGE = 1.0

def spline_basis(phase):
    inverse = 1.0 - phase
    square = phase * phase
    cubed = square * phase
    return [inverse * inverse * inverse / 6.0, (3.0 * cubed - 6.0 * square + 4.0) / 6.0, (-3.0 * cubed + 3.0 * square + 3.0 * phase + 1.0) / 6.0, cubed / 6.0]

def cholesky_lists(matrix, extent):
    lower_tri = [[None for column in range(extent)] for target in range(extent)]
    for column in range(extent):
        pivot_sq = matrix[column][column]
        for inner_k in range(column):
            pivot_sq = pivot_sq - lower_tri[column][inner_k] * lower_tri[column][inner_k]
        pivot_val = jnp.sqrt(pivot_sq)
        lower_tri[column][column] = pivot_val
        for target in range(column + 1, extent):
            entry_val = matrix[target][column]
            for inner_k in range(column):
                entry_val = entry_val - lower_tri[target][inner_k] * lower_tri[column][inner_k]
            lower_tri[target][column] = entry_val / pivot_val
    return lower_tri

def solve_lower(lower_tri, vector):
    result = []
    for target in range(len(vector)):
        running = vector[target]
        for inner_k in range(target):
            running = running - lower_tri[target][inner_k] * result[inner_k]
        result.append(running / lower_tri[target][target])
    return result

def solve_upper(lower_tri, vector):
    extent = len(vector)
    result = [None for target in range(extent)]
    for target in reversed(range(extent)):
        running = vector[target]
        for inner_k in range(target + 1, extent):
            running = running - lower_tri[inner_k][target] * result[inner_k]
        result[target] = running / lower_tri[target][target]
    return result

def upper_pairs(extent):
    return [(first, second) for first in range(extent) for second in range(first, extent)]

def symmetric_lists(upper_values, extent):
    matrix = [[None for second in range(extent)] for first in range(extent)]
    for position, index_pair in enumerate(upper_pairs(extent)):
        first, second = index_pair
        value_now = upper_values[position] + (RIDGE if first == second else 0.0)
        matrix[first][second] = value_now
        matrix[second][first] = value_now
    return matrix

def solve_blocks(upper_values, rhs_values, extent):
    lower_tri = cholesky_lists(symmetric_lists(upper_values, extent), extent)
    whitened = solve_lower(lower_tri, rhs_values)
    solution = solve_upper(lower_tri, whitened)
    return (jnp.stack(whitened), jnp.stack(solution))

def apply_band(band_own, band_left, padded):
    extent = band_own.shape[-1]
    result = padded[:, 3:3 + extent]
    for offset in range(4):
        ahead_x = padded[:, 3 + offset:3 + offset + extent]
        result = result + lax.optimization_barrier(jnp.sum(band_own[offset] * ahead_x[None, :, :], axis=1))
    for offset in range(1, 4):
        behind = padded[:, 3 - offset:3 - offset + extent]
        blocks = band_left[offset][:, :, 3 - offset:3 - offset + extent]
        result = result + lax.optimization_barrier(jnp.sum(blocks * behind[:, None, :], axis=0))
    return result

def node_sweeps(band_own, band_left, rhs_att, extend):
    diagonal = [[band_own[0][first, second] + (RIDGE if first == second else 0.0) for second in range(3)] for first in range(3)]
    lower_tri = cholesky_lists(diagonal, 3)

    def precondition(vector):
        return jnp.stack(solve_upper(lower_tri, solve_lower(lower_tri, [vector[axis_k] for axis_k in range(3)])))
    answer = OMEGA * precondition(rhs_att)
    for sweep_no in range(1, ATT_SWEEPS):
        padded = extend(answer)
        answer = answer + OMEGA * precondition(rhs_att - apply_band(band_own, band_left, padded))
    padded = extend(answer)
    scaled = jnp.stack([sum((lower_tri[inner_k][target] * answer[inner_k] for inner_k in range(target, 3))) for target in range(3)])
    return (answer, padded, scaled)

def node_features(vectors, weights, first_res, basis_no):
    term_list = []
    for offset in range(4 - basis_no):
        for first in range(3):
            for second in range(3):
                term_list.append(weights * vectors[basis_no][first] * vectors[basis_no + offset][second])
    for first in range(3):
        term_list.append(weights * vectors[basis_no][first] * first_res)
    return jnp.stack(term_list)

def spread_terms(stacked, basis_no):
    band_rows = (4 - basis_no) * 9
    filler = jnp.zeros((basis_no * 9,) + stacked.shape[1:], jnp.float32)
    return jnp.concatenate([stacked[:band_rows], filler, stacked[band_rows:]], axis=0)

def unit_matrix_terms(rows_part, weights):
    return [weights * rows_part[first] * rows_part[second] for first, second in upper_pairs(rows_part.shape[0])]

def rhs_terms(rows_part, weights, resid_now):
    return [weights * rows_part[first] * resid_now for first in range(rows_part.shape[0])]

def reference(residual, weight, source_part, source_index, source_delta, attitude_part, spline_phase, knot_index, calib_part, calib_index, global_part):
    nodes_dev = ND
    interval_ids = jnp.arange(INTERVALS, dtype=jnp.int32)

    def interval_rows(index_t):
        weights = weight[index_t].reshape(-1)
        source_rows = source_part[:, index_t].reshape(5, -1)
        picked = jnp.take(source_delta[:, index_t], source_index[index_t].reshape(-1), axis=1)
        first_res = residual[index_t].reshape(-1) - lax.optimization_barrier(jnp.sum(source_rows * picked, axis=0))
        basis_list = spline_basis(spline_phase[index_t].reshape(-1))
        att_rows = attitude_part[:, index_t].reshape(3, -1)
        vectors = [basis_val[None, :] * att_rows for basis_val in basis_list]
        local_knot = knot_index[index_t].reshape(-1) - index_t * nodes_dev
        return (weights, first_res, vectors, local_knot)

    def first_pass(index_t):
        weights, first_res, vectors, local_knot = interval_rows(index_t)
        local_sums = jnp.zeros((39, nodes_dev + 3), jnp.float32)
        for basis_no in range(4):
            stacked = node_features(vectors, weights, first_res, basis_no)
            binned = jax.ops.segment_sum(stacked.T, local_knot + basis_no, num_segments=nodes_dev + 3).T
            local_sums = local_sums + spread_terms(binned, basis_no)
        return local_sums
    local_all = lax.map(first_pass, interval_ids)
    spill_out = local_all[:, :, nodes_dev:]
    shifted = jnp.concatenate([jnp.zeros((1, 39, 3), jnp.float32), spill_out[:-1]], axis=0)
    main_part = local_all[:, :, :nodes_dev]
    main_part = jnp.concatenate([main_part[:, :, :3] + shifted, main_part[:, :, 3:]], axis=2)
    totals = jnp.transpose(main_part, (1, 0, 2)).reshape(39, INTERVALS * nodes_dev)
    band_own = totals[:36].reshape(4, 3, 3, -1)
    band_left = jnp.concatenate([jnp.zeros((4, 3, 3, 3), jnp.float32), band_own], axis=3)

    def extend(vector):
        return jnp.pad(vector, ((0, 0), (3, 3)))
    answer, padded, attitude_step = node_sweeps(band_own, band_left, totals[36:], extend)
    node_values = padded[:, 3:]

    def second_pass(index_t):
        weights, first_res, vectors, local_knot = interval_rows(index_t)
        global_knot = knot_index[index_t].reshape(-1)
        second_res = first_res
        for basis_no in range(4):
            picked_nodes = jnp.take(node_values, global_knot + basis_no, axis=1)
            second_res = second_res - lax.optimization_barrier(jnp.sum(vectors[basis_no] * picked_nodes, axis=0))
        calib_rows = calib_part[:, index_t].reshape(CPAR, -1)
        global_rows = global_part[:, index_t].reshape(GPAR, -1)
        unit_ids = calib_index[index_t].reshape(-1)
        features = jnp.stack(unit_matrix_terms(calib_rows, weights) + rhs_terms(calib_rows, weights, second_res))
        unit_terms = jax.ops.segment_sum(features.T, unit_ids, num_segments=UNITS).T
        global_terms = jnp.stack([jnp.sum(term_row) for term_row in unit_matrix_terms(global_rows, weights) + rhs_terms(global_rows, weights, second_res)])
        return (second_res, unit_terms, global_terms)
    second_all, unit_all, global_all = lax.map(second_pass, interval_ids)
    unit_total = lax.optimization_barrier(jnp.sum(unit_all, axis=0))
    global_total = lax.optimization_barrier(jnp.sum(global_all, axis=0))
    pair_count = CPAR * (CPAR + 1) // 2
    pair_global = GPAR * (GPAR + 1) // 2
    calib_step, calib_solution = solve_blocks(unit_total[:pair_count], [unit_total[pair_count + first] for first in range(CPAR)], CPAR)
    global_step, global_solution = solve_blocks(global_total[:pair_global], [global_total[pair_global + first] for first in range(GPAR)], GPAR)

    def third_pass(carried):
        index_t, second_res = carried
        calib_rows = calib_part[:, index_t].reshape(CPAR, -1)
        global_rows = global_part[:, index_t].reshape(GPAR, -1)
        unit_values = jnp.take(calib_solution, calib_index[index_t].reshape(-1), axis=1)
        final_res = second_res - lax.optimization_barrier(jnp.sum(calib_rows * unit_values, axis=0)) - lax.optimization_barrier(jnp.sum(global_rows * global_solution[:, None], axis=0))
        return final_res.reshape(GROUPS, ROWS_DEV)
    residual_new = lax.map(third_pass, (interval_ids, second_all))
    return (residual_new, attitude_step, calib_step, global_step)
```

```python
import functools
import math

import jax
import jax.numpy as jnp
from jax import lax
from jax.experimental import pallas as pl
from jax.experimental.pallas import tpu as pltpu
from jax.sharding import PartitionSpec as P

TILE = 128
KPT = 4
UNITS = 2048
CPAR = 6
GPAR = 4
ATT_SWEEPS = 4

OMEGA = 0.6
RIDGE = 1.0
LANES = 128
LOW = 256
HALO = 3 * ATT_SWEEPS
MESH = pl.DeviceIdType.MESH
F32 = jnp.float32
BF16 = jnp.bfloat16

ATT_ROWS = 72
UNIT_ROWS = 24
PAIRS = CPAR * (CPAR + 1) // 2
HALF = 64
NORMAL_ROWS = 32


def pairs_of(extent):
    return [(a, b) for a in range(extent) for b in range(a, extent)]


def lane_pick(table, index):
    return lax.gather(
        table,
        index[..., None],
        lax.GatherDimensionNumbers(
            offset_dims=(),
            collapsed_slice_dims=(1,),
            start_index_map=(1,),
            operand_batching_dims=(0,),
            start_indices_batching_dims=(0,),
        ),
        (1, 1),
        mode=lax.GatherScatterMode.PROMISE_IN_BOUNDS,
    )


def spline_basis(phase):
    inverse = 1.0 - phase
    square = phase * phase
    cubed = square * phase
    return [
        inverse * inverse * inverse / 6.0,
        (3.0 * cubed - 6.0 * square + 4.0) / 6.0,
        (-3.0 * cubed + 3.0 * square + 3.0 * phase + 1.0) / 6.0,
        cubed / 6.0,
    ]


def cholesky_lists(matrix, extent):
    lower = [[None] * extent for _ in range(extent)]
    inverse = [None] * extent
    for column in range(extent):
        pivot = matrix[column][column]
        for k in range(column):
            pivot = pivot - lower[column][k] * lower[column][k]
        root = jnp.sqrt(pivot)
        lower[column][column] = root
        inverse[column] = 1.0 / root
        for row in range(column + 1, extent):
            entry = matrix[row][column]
            for k in range(column):
                entry = entry - lower[row][k] * lower[column][k]
            lower[row][column] = entry * inverse[column]
    return lower, inverse


def solve_lower(lower, inverse, vector):
    result = []
    for row in range(len(vector)):
        running = vector[row]
        for k in range(row):
            running = running - lower[row][k] * result[k]
        result.append(running * inverse[row])
    return result


def solve_upper(lower, inverse, vector):
    extent = len(vector)
    result = [None] * extent
    for row in reversed(range(extent)):
        running = vector[row]
        for k in range(row + 1, extent):
            running = running - lower[k][row] * result[k]
        result[row] = running * inverse[row]
    return result


def symmetric(upper, extent):
    matrix = [[None] * extent for _ in range(extent)]
    for position, (a, b) in enumerate(pairs_of(extent)):
        value = upper[position] + (RIDGE if a == b else 0.0)
        matrix[a][b] = value
        matrix[b][a] = value
    return matrix


def split_two(value):
    first = value.astype(BF16)
    return [first, (value - first.astype(F32)).astype(BF16)]


def dot_nt(left, right):
    return lax.dot_general(
        left, right, (((1,), (1,)), ((), ())), preferred_element_type=F32
    )


def two_tiles(ref, tile, rows, tiles):
    return jnp.concatenate(
        [ref[pl.ds(tile, rows, stride=tiles), :], ref[pl.ds(tile + 1, rows, stride=tiles), :]],
        axis=1,
    )


def two_rows(ref, tile):
    return jnp.concatenate([ref[pl.ds(tile, 1), :], ref[pl.ds(tile + 1, 1), :]], axis=1)


def one_hot(row, extent):
    spots = lax.broadcasted_iota(jnp.int32, (extent, row.shape[1]), 0)
    return jnp.where(spots == row, 1.0, 0.0).astype(BF16)


def by_high(part, high):
    return jnp.concatenate(
        [jnp.where(high == h, part, 0.0) for h in range(UNITS // LOW)], axis=0
    ).astype(BF16)


def block_pieces(blocks):
    width = UNITS // blocks
    for piece in range(UNITS // LANES):
        unit = piece * LANES
        yield unit // width, unit % width, unit // LOW, unit % LOW


def round_up(value, unit):
    return -(-value // unit) * unit


def layout(shape):
    count, groups, inner = shape
    plane = groups * inner
    blocks = min(plane, UNITS // LANES)
    width = UNITS // blocks
    slots = width // HALF
    mats_rows = round_up(PAIRS + -(-(GPAR * (GPAR + 1) // 2) // slots), 8)
    rhs_rows = round_up(CPAR + -(-GPAR // slots), 8)
    parts = width // LANES
    ready_rows = round_up(2 * CPAR * parts, 8)
    return plane, blocks, width, slots, mats_rows, rhs_rows, parts, ready_rows


def solved_rows(parts, ready_rows):
    spare = [8 * j + r for j in range(parts) for r in range(CPAR, 8)]
    return spare + list(range(8 * parts, ready_rows))


def fold_slots(rows, slots):
    lane = lax.broadcasted_iota(jnp.int32, (1, LANES), 1)
    folded = [row + pltpu.roll(row, HALF, 1) for row in rows]
    folded.append(jnp.zeros((1, LANES), F32))
    packed = []
    for start in range(0, len(rows), slots):
        parts = []
        for k in range(start, start + slots, 2):
            left, right = folded[min(k, len(rows))], folded[min(k + 1, len(rows))]
            parts.append(jnp.where(lane < HALF, left, right))
        packed.append(parts)
    return packed


def slot_sum(table, first_row, no, slots):
    row, at = first_row + no // slots, no % slots
    start = (at // 2) * LANES
    lane = lax.broadcasted_iota(jnp.int32, (1, LANES), 1)
    half = (lane < HALF) if at % 2 == 0 else (lane >= HALF)
    values = jnp.where(half, table[row : row + 1, start : start + LANES], 0.0)
    return jnp.broadcast_to(jnp.sum(values, axis=1, keepdims=True), (1, LANES))


def step_kernel(
    shape, nodes_dev,
    res_h, w_h, sp_h, si_h, sd_h, ap_h, ph_h, kn_h, cp_h, ci_h, gp_h,
    out_ref, step_ref, cstep_ref, glob_ref,
    res_ref, w_ref, sp_ref, si_ref, sd_ref, ap_ref, ph_ref, kn_ref, cp_ref, ci_ref, gp_ref,
    att, cal, rcal, acc_att, acc_cal, acc_rhs, normal_ref, mats_ref, rhs_ref,
    near, pmat, prhs, zmat, zrhs, ready, spread,
    load_s, near_s, near_r, pmat_s, pmat_r, prhs_s, prhs_r,
    zmat_s, zmat_r, zrhs_s, zrhs_r, spread_s, spread_r,
):
    count, groups, inner = shape
    plane, blocks, width, slots, mats_rows, rhs_rows, parts, ready_rows = layout(shape)
    depth = count // inner
    t, g = lax.axis_index("tm"), lax.axis_index("grp")
    has_before, has_after = t > 0, t < count - 1
    z, i = lax.div(t, inner), lax.rem(t, inner)
    m = g * inner + i
    block = lax.rem(m, blocks)
    family = m - block

    pairs = [
        (si_h, si_ref), (sd_h, sd_ref), (sp_h, sp_ref), (res_h, res_ref), (w_h, w_ref),
        (ap_h, ap_ref), (ph_h, ph_ref), (kn_h, kn_ref), (cp_h, cp_ref), (ci_h, ci_ref),
        (gp_h, gp_ref),
    ]
    loads = [
        pltpu.make_async_copy(source, target, load_s.at[no])
        for no, (source, target) in enumerate(pairs)
    ]
    for load in loads:
        load.start()

    def peer_tm(k):
        return lax.rem(t + k, count)

    def peer_grp(k):
        return lax.rem(g + k, groups)

    def member(p):
        return {"tm": z * inner + lax.rem(p, inner), "grp": lax.div(p, inner)}

    def level(k):
        return {"tm": lax.rem(t + k * inner, count), "grp": g}

    barrier = pltpu.get_barrier_semaphore()

    def greet(where):
        pl.semaphore_signal(barrier, inc=1, device_id=where, device_id_type=MESH)

    for k in range(1, depth):
        greet(level(k))
    for k in range(groups):
        greet({"tm": peer_tm(1), "grp": peer_grp(k)})
        greet({"tm": peer_tm(count - 1), "grp": peer_grp(k)})
    for k in range(1, plane):
        greet(member(lax.rem(m + k, plane)))

    for load in loads[:8]:
        load.wait()
    tiles = res_ref.shape[0]
    weights = w_ref[...]
    sources = si_ref[...]
    high, low = lax.shift_right_logical(sources, 7), lax.bitwise_and(sources, 127)
    picked = [jnp.zeros((tiles, LANES), F32) for _ in range(5)]
    for row in range(sd_ref.shape[1]):
        here = high == row
        for c in range(5):
            table = jnp.broadcast_to(sd_ref[c, row : row + 1, :], (tiles, LANES))
            picked[c] = jnp.where(here, lane_pick(table, low), picked[c])
    total = sp_ref[0] * picked[0]
    for c in range(1, 5):
        total = total + sp_ref[c] * picked[c]
    first = res_ref[...] - total
    basis = spline_basis(ph_ref[...])
    axes = [ap_ref[c] for c in range(3)]
    products = [weights * axes[a] * axes[b] for a, b in pairs_of(3)]
    rights = [weights * axes[a] * first for a in range(3)]
    place = 0
    for i_ in range(4):
        for d in range(4 - i_):
            both = basis[i_] * basis[i_ + d]
            for product in products:
                att[place * tiles : (place + 1) * tiles, :] = both * product
                place += 1
    for i_ in range(4):
        for right in rights:
            att[place * tiles : (place + 1) * tiles, :] = basis[i_] * right
            place += 1
    acc_att[...] = jnp.zeros_like(acc_att)
    base = t * (tiles * KPT)

    def bin_nodes(no, carry):
        tile = no * 2
        knots = two_rows(kn_ref, tile) - base
        nodes = one_hot(knots, LANES)
        part = acc_att[...]
        for piece in split_two(two_tiles(att, tile, ATT_ROWS, tiles)):
            part = part + dot_nt(piece, nodes)
        acc_att[...] = part
        return carry

    lax.fori_loop(0, tiles // 2, bin_nodes, 0, unroll=6)
    band = [None] * 5
    place = 0
    for i_ in range(4):
        for d in list(range(4 - i_)):
            rows = acc_att[place : place + 6, :]
            rows = pltpu.roll(rows, i_, 1) if i_ else rows
            band[d] = rows if band[d] is None else band[d] + rows
            place += 6
    for i_ in range(4):
        rows = acc_att[place : place + 3, :]
        rows = pltpu.roll(rows, i_, 1) if i_ else rows
        band[4] = rows if band[4] is None else band[4] + rows
        place += 3
    for d in range(4):
        normal_ref[d * 6 : (d + 1) * 6, :] = band[d]
    normal_ref[24:27, :] = band[4]
    normal_ref[27:, :] = jnp.zeros((NORMAL_ROWS - 27, LANES), F32)
    pl.semaphore_wait(barrier, depth - 1 + 2 * groups + plane - 1)

    def near_copy(offset, k):
        slot = (1 - offset) * groups + g
        return pltpu.make_async_remote_copy(
            src_ref=normal_ref,
            dst_ref=near.at[slot],
            send_sem=near_s.at[(offset + 1) * groups + k],
            recv_sem=near_r.at[slot],
            device_id={"tm": t + offset, "grp": peer_grp(k)},
            device_id_type=MESH,
        )

    def near_arrival(offset, k):
        slot = (offset + 1) * groups + peer_grp(k)
        return pltpu.make_async_remote_copy(
            src_ref=normal_ref,
            dst_ref=near.at[slot],
            send_sem=near_s.at[(offset + 1) * groups + k],
            recv_sem=near_r.at[slot],
            device_id={"tm": t + offset, "grp": peer_grp(k)},
            device_id_type=MESH,
        )

    def each_near(do):
        @pl.when(has_before)
        def _():
            for k in reversed(range(groups)):
                do(-1, k)

        @pl.when(has_after)
        def _():
            for k in reversed(range(groups)):
                do(1, k)

        for k in range(1, groups):
            do(0, k)

    each_near(lambda offset, k: near_copy(offset, k).start())

    for load in loads[8:]:
        load.wait()
    place = 0
    for a, b in pairs_of(CPAR):
        cal[place * tiles : (place + 1) * tiles, :] = weights * cp_ref[a] * cp_ref[b]
        place += 1
    cal[place * tiles :, :] = jnp.zeros(((UNIT_ROWS - place) * tiles, LANES), F32)
    global_rows = fold_slots(
        [
            jnp.sum(weights * gp_ref[a] * gp_ref[b], axis=0, keepdims=True)
            for a, b in pairs_of(GPAR)
        ],
        slots,
    )
    acc_cal[...] = jnp.zeros_like(acc_cal)

    def bin_units(no, carry):
        tile = no * 2
        units = two_rows(ci_ref, tile)
        upper, lower = lax.shift_right_logical(units, 8), lax.bitwise_and(units, 255)
        spots = one_hot(lower, LOW)
        part = acc_cal[...]
        for piece in split_two(two_tiles(cal, tile, UNIT_ROWS, tiles)):
            part = part + dot_nt(by_high(piece.astype(F32), upper), spots)
        acc_cal[...] = part
        return carry

    lax.fori_loop(0, tiles // 2, bin_units, 0, unroll=6)
    for b_, at, h, start in block_pieces(blocks):
        mats_ref[b_, 0:UNIT_ROWS, at : at + LANES] = acc_cal[
            h * UNIT_ROWS : (h + 1) * UNIT_ROWS, start : start + LANES
        ]
    if mats_rows > UNIT_ROWS:
        mats_ref[:, UNIT_ROWS:, :] = jnp.zeros((blocks, mats_rows - UNIT_ROWS, width), F32)
    for b_ in range(blocks):
        for no, pieces in enumerate(global_rows):
            for j, piece in enumerate(pieces):
                mats_ref[b_, PAIRS + no : PAIRS + no + 1, j * LANES : (j + 1) * LANES] = piece

    def plane_copy(source, target, send, recv, k, slot):
        p = lax.rem(m + k, plane)
        return pltpu.make_async_remote_copy(
            src_ref=source.at[lax.rem(p, blocks)],
            dst_ref=target.at[slot],
            send_sem=send.at[k],
            recv_sem=recv.at[slot],
            device_id=member(p),
            device_id_type=MESH,
        )

    def level_copy(target, send, recv, k, slot):
        return pltpu.make_async_remote_copy(
            src_ref=target.at[slot],
            dst_ref=target.at[slot],
            send_sem=send.at[k],
            recv_sem=recv.at[slot],
            device_id=level(k),
            device_id_type=MESH,
        )

    def slots_total(buffer, number):
        out = buffer[0]
        for k in range(1, number):
            out = out + buffer[k]
        return out

    for k in range(1, plane):
        plane_copy(mats_ref, pmat, pmat_s, pmat_r, k, m).start()
    pmat[m] = mats_ref[block]
    near[groups + g] = normal_ref[...]

    @pl.when(jnp.logical_not(has_before))
    def _():
        near[0:groups] = jnp.zeros((groups, NORMAL_ROWS, LANES), F32)

    @pl.when(jnp.logical_not(has_after))
    def _():
        near[2 * groups :] = jnp.zeros((groups, NORMAL_ROWS, LANES), F32)

    each_near(lambda offset, k: near_arrival(offset, k).wait_recv())
    sums = []
    for s in range(3):
        part = near[s * groups]
        for q in range(1, groups):
            part = part + near[s * groups + q]
        sums.append(part)
    lane = lax.broadcasted_iota(jnp.int32, (NORMAL_ROWS, LANES), 1)
    before = pltpu.roll(sums[0], (HALO - nodes_dev) % LANES, 1)
    own = pltpu.roll(sums[1], HALO, 1)
    after = pltpu.roll(sums[2], (HALO + nodes_dev) % LANES, 1)
    end = nodes_dev + HALO
    normals = (
        own
        + jnp.where((lane >= 3) & (lane < HALO + 3), before, 0.0)
        + jnp.where((lane >= end) & (lane < end + HALO), after, 0.0)
    )
    spot = lax.broadcasted_iota(jnp.int32, (1, LANES), 1)
    exists = (spot >= jnp.where(has_before, 0, HALO)) & (
        spot < jnp.where(has_after, LANES, end)
    )
    normals = jnp.where(exists, normals, 0.0)
    index = {}
    for position, (a, b) in enumerate(pairs_of(3)):
        index[a, b] = index[b, a] = position
    band = [[normals[d * 6 + p : d * 6 + p + 1, :] for p in range(6)] for d in range(4)]
    right = [normals[24 + c : 25 + c, :] for c in range(3)]
    lower, inverse = cholesky_lists(symmetric(band[0], 3), 3)

    def precondition(vector):
        return solve_upper(lower, inverse, solve_lower(lower, inverse, vector))

    x = [OMEGA * value for value in precondition(right)]
    for _ in range(1, ATT_SWEEPS):
        out = [right[c] - x[c] for c in range(3)]
        for d in range(4):
            ahead = [pltpu.roll(x[c], LANES - d, 1) for c in range(3)] if d else x
            for a in range(3):
                for b in range(3):
                    out[a] = out[a] - band[d][index[a, b]] * ahead[b]
        for d in range(1, 4):
            for a in range(3):
                term = band[d][index[a, 0]] * x[0]
                for b in range(1, 3):
                    term = term + band[d][index[a, b]] * x[b]
                out[a] = out[a] - pltpu.roll(term, d, 1)
        change = precondition(out)
        x = [jnp.where(exists, x[c] + OMEGA * change[c], 0.0) for c in range(3)]

    local = kn_ref[...] - base + HALO
    tables = [jnp.broadcast_to(x[c], (tiles, LANES)) for c in range(3)]
    second = first
    for i_ in range(4):
        moved = ap_ref[0] * lane_pick(tables[0], local + i_)
        for c in range(1, 3):
            moved = moved + ap_ref[c] * lane_pick(tables[c], local + i_)
        second = second - basis[i_] * moved
    out_ref[...] = second
    weighted = weights * second
    for a in range(CPAR):
        rcal[a * tiles : (a + 1) * tiles, :] = weighted * cp_ref[a]
    rcal[CPAR * tiles :, :] = jnp.zeros(((8 - CPAR) * tiles, LANES), F32)
    global_rows = fold_slots(
        [jnp.sum(weighted * gp_ref[a], axis=0, keepdims=True) for a in range(GPAR)], slots
    )
    acc_rhs[...] = jnp.zeros_like(acc_rhs)

    def bin_rhs(no, carry):
        tile = no * 2
        units = two_rows(ci_ref, tile)
        upper, lower = lax.shift_right_logical(units, 8), lax.bitwise_and(units, 255)
        pieces = [
            by_high(p.astype(F32), upper) for p in split_two(two_tiles(rcal, tile, 8, tiles))
        ]
        lhs = jnp.concatenate(pieces, axis=0)
        acc_rhs[...] = acc_rhs[...] + dot_nt(lhs, one_hot(lower, LOW))
        return carry

    lax.fori_loop(0, tiles // 2, bin_rhs, 0, unroll=6)
    rows = 8 * (UNITS // LOW)
    total = acc_rhs[0:rows, :] + acc_rhs[rows : 2 * rows, :]
    for b_, at, h, start in block_pieces(blocks):
        rhs_ref[b_, 0:8, at : at + LANES] = total[h * 8 : h * 8 + 8, start : start + LANES]
    for b_ in range(blocks):
        for no, pieces in enumerate(global_rows):
            for j, piece in enumerate(pieces):
                rhs_ref[b_, CPAR + no : CPAR + no + 1, j * LANES : (j + 1) * LANES] = piece
    for k in range(1, plane):
        plane_copy(rhs_ref, prhs, prhs_s, prhs_r, k, m).start()
    prhs[m] = rhs_ref[block]

    for c in range(3):
        scaled = lower[c][c] * x[c]
        for k in range(c + 1, 3):
            scaled = scaled + lower[k][c] * x[k]
        moved = pltpu.roll(scaled, LANES - HALO, 1)
        step_ref[c : c + 1, :] = moved[:, 0:nodes_dev]

    for k in range(1, plane):
        plane_copy(mats_ref, pmat, pmat_s, pmat_r, k, lax.rem(m + k, plane)).wait_recv()
    zmat[z] = slots_total(pmat, plane)
    for k in range(1, depth):
        level_copy(zmat, zmat_s, zmat_r, k, z).start()

    for k in range(1, plane):
        plane_copy(rhs_ref, prhs, prhs_s, prhs_r, k, lax.rem(m + k, plane)).wait_recv()
    zrhs[z] = slots_total(prhs, plane)
    for k in range(1, depth):
        level_copy(zrhs, zrhs_s, zrhs_r, k, z).start()

    for k in range(1, depth):
        level_copy(zmat, zmat_s, zmat_r, k, lax.rem(z + k, depth)).wait_recv()
    unit_total = slots_total(zmat, depth)
    matrix = [unit_total[p : p + 1, :] for p in range(PAIRS)]
    lower, inverse = cholesky_lists(symmetric(matrix, CPAR), CPAR)
    upper_g = [
        slot_sum(unit_total, PAIRS, p, slots) for p in range(GPAR * (GPAR + 1) // 2)
    ]
    lower_g, inverse_g = cholesky_lists(symmetric(upper_g, GPAR), GPAR)

    for k in range(1, depth):
        level_copy(zrhs, zrhs_s, zrhs_r, k, lax.rem(z + k, depth)).wait_recv()
    total = slots_total(zrhs, depth)
    right = [total[c : c + 1, :] for c in range(CPAR)]
    white = solve_lower(lower, inverse, right)
    solved = solve_upper(lower, inverse, white)
    where_solved = solved_rows(parts, ready_rows)
    for j in range(parts):
        span = slice(j * LANES, (j + 1) * LANES)
        for c in range(CPAR):
            ready[8 * j + c : 8 * j + c + 1, :] = white[c][:, span]
            row = where_solved[c * parts + j]
            ready[row : row + 1, :] = solved[c][:, span]
    for row in where_solved[CPAR * parts :]:
        ready[row : row + 1, :] = jnp.zeros((1, LANES), F32)

    def spread_copy(k, slot):
        return pltpu.make_async_remote_copy(
            src_ref=ready,
            dst_ref=spread.at[slot],
            send_sem=spread_s.at[k],
            recv_sem=spread_r.at[slot],
            device_id=member(family + lax.rem(block + k, blocks)),
            device_id_type=MESH,
        )

    for k in range(1, blocks):
        spread_copy(k, block).start()
    spread[block] = ready[...]
    right_g = [slot_sum(total, CPAR, c, slots) for c in range(GPAR)]
    white_g = solve_lower(lower_g, inverse_g, right_g)
    solved_g = solve_upper(lower_g, inverse_g, white_g)
    spot = lax.broadcasted_iota(jnp.int32, (1, LANES), 1)
    packed = jnp.zeros((1, LANES), F32)
    for c in range(GPAR):
        packed = jnp.where(spot == c, white_g[c], packed)
    glob_ref[...] = packed[:, 0:GPAR]
    out = out_ref[...]
    for c in range(GPAR):
        out = out - gp_ref[c] * solved_g[c]
    units = ci_ref[...]
    high, low = lax.shift_right_logical(units, 7), lax.bitwise_and(units, 127)
    for k in range(1, blocks):
        spread_copy(k, lax.rem(block + k, blocks)).wait_recv()
    picked = [jnp.zeros((tiles, LANES), F32) for _ in range(CPAR)]
    for b_ in range(blocks):
        for j in range(parts):
            row = b_ * parts + j
            here = high == row
            cstep_ref[:, row * LANES : (row + 1) * LANES] = spread[b_, 8 * j : 8 * j + CPAR, :]
            for c in range(CPAR):
                at = where_solved[c * parts + j]
                table = jnp.broadcast_to(spread[b_, at : at + 1, :], (tiles, LANES))
                picked[c] = jnp.where(here, lane_pick(table, low), picked[c])
    for c in range(CPAR):
        out = out - cp_ref[c] * picked[c]
    out_ref[...] = out
    each_near(lambda offset, k: near_copy(offset, k).wait_send())
    for k in range(1, plane):
        plane_copy(mats_ref, pmat, pmat_s, pmat_r, k, m).wait_send()
        plane_copy(rhs_ref, prhs, prhs_s, prhs_r, k, m).wait_send()
    for k in range(1, depth):
        level_copy(zmat, zmat_s, zmat_r, k, z).wait_send()
        level_copy(zrhs, zrhs_s, zrhs_r, k, z).wait_send()
    for k in range(1, blocks):
        spread_copy(k, block).wait_send()


def final_kernel(*refs):
    half = len(refs) // 2
    copies = [
        pltpu.make_async_copy(refs[no], refs[half + no], refs[-1].at[no]) for no in range(half)
    ]
    for copy in copies:
        copy.start()
    for copy in copies:
        copy.wait()


def per_device(
    shape, residual, weight, source_part, source_index, source_delta, attitude_part,
    spline_phase, knot_index, calib_part, calib_index, global_part,
):
    count, groups, inner = shape
    plane, blocks, width, slots, mats_rows, rhs_rows, parts, ready_rows = layout(shape)
    depth = count // inner
    row_count = residual.shape[-1]
    tiles = row_count // TILE
    nodes_dev = tiles * KPT

    def flat(value):
        return value.reshape(tiles, TILE)

    def deep(value):
        return value.reshape(value.shape[0], -1, LANES)

    args = (
        flat(residual), flat(weight), deep(source_part), flat(source_index),
        deep(source_delta), deep(attitude_part), flat(spline_phase), flat(knot_index),
        deep(calib_part), flat(calib_index), deep(global_part),
    )

    def vmem(*dims):
        return pltpu.VMEM(dims, F32)

    dma = pltpu.SemaphoreType.DMA
    results = pl.pallas_call(
        functools.partial(step_kernel, shape, nodes_dev),
        out_shape=(
            vmem(tiles, LANES), vmem(3, nodes_dev), vmem(CPAR, UNITS), vmem(1, GPAR),
        ),
        scratch_shapes=[pltpu.VMEM(arg.shape, arg.dtype) for arg in args] + [
            vmem(ATT_ROWS * tiles, LANES),
            vmem(UNIT_ROWS * tiles, LANES),
            vmem(8 * tiles, LANES),
            vmem(ATT_ROWS, LANES),
            vmem(UNIT_ROWS * (UNITS // LOW), LOW),
            vmem(2 * 8 * (UNITS // LOW), LOW),
            vmem(NORMAL_ROWS, LANES),
            vmem(blocks, mats_rows, width),
            vmem(blocks, rhs_rows, width),
            vmem(3 * groups, NORMAL_ROWS, LANES),
            vmem(plane, mats_rows, width),
            vmem(plane, rhs_rows, width),
            vmem(depth, mats_rows, width),
            vmem(depth, rhs_rows, width),
            vmem(ready_rows, LANES),
            vmem(blocks, ready_rows, LANES),
            dma((len(args),)),
            dma((3 * groups,)), dma((3 * groups,)),
            dma((plane,)), dma((plane,)),
            dma((plane,)), dma((plane,)),
            dma((depth,)), dma((depth,)),
            dma((depth,)), dma((depth,)),
            dma((blocks,)), dma((blocks,)),
        ],
        in_specs=[pl.BlockSpec(memory_space=pl.ANY)] * len(args),
        compiler_params=pltpu.CompilerParams(collective_id=0, has_side_effects=True),
        name="step",
    )(*args)
    final, attitude_out, calib_step, global_step = pl.pallas_call(
        final_kernel,
        out_shape=tuple(jax.ShapeDtypeStruct(value.shape, F32) for value in results),
        in_specs=[pl.BlockSpec(memory_space=pltpu.VMEM)] * len(results),
        out_specs=(pl.BlockSpec(memory_space=pltpu.HBM),) * len(results),
        scratch_shapes=[dma((len(results),))],
        name="final",
    )(*[pltpu.with_memory_space_constraint(value, pltpu.VMEM) for value in results])
    return final.reshape(residual.shape), attitude_out, calib_step, global_step.reshape(GPAR)


def solution(mesh):
    count, groups = mesh.shape["tm"], mesh.shape["grp"]
    inner = 1 << (int(math.log2(count)) // 2)
    return jax.shard_map(
        functools.partial(per_device, (count, groups, inner)),
        mesh=mesh,
        in_specs=(
            P("tm", "grp", None),
            P("tm", "grp", None),
            P(None, "tm", "grp", None),
            P("tm", "grp", None),
            P(None, "tm", None),
            P(None, "tm", "grp", None),
            P("tm", "grp", None),
            P("tm", "grp", None),
            P(None, "tm", "grp", None),
            P("tm", "grp", None),
            P(None, "tm", "grp", None),
        ),
        out_specs=(P("tm", "grp", None), P(None, "tm"), P(), P()),
        check_vma=False,
    )
```

```python
import functools
import math

import jax
import jax.numpy as jnp
from jax import lax
from jax.experimental import pallas as pl
from jax.experimental.pallas import tpu as pltpu
from jax.sharding import PartitionSpec as P

TILE = 128
KPT = 4
UNITS = 2048
CPAR = 6
GPAR = 4
ATT_SWEEPS = 4

OMEGA = 0.6
RIDGE = 1.0
LANES = 128
LOW = 256
HALO = 3 * ATT_SWEEPS
MESH = pl.DeviceIdType.MESH
F32 = jnp.float32
BF16 = jnp.bfloat16

ATT_ROWS = 72
UNIT_ROWS = 24
PAIRS = CPAR * (CPAR + 1) // 2
HALF = 64
NORMAL_ROWS = 32


def pairs_of(extent):
    return [(a, b) for a in range(extent) for b in range(a, extent)]


def lane_pick(table, index):
    return lax.gather(
        table,
        index[..., None],
        lax.GatherDimensionNumbers(
            offset_dims=(),
            collapsed_slice_dims=(1,),
            start_index_map=(1,),
            operand_batching_dims=(0,),
            start_indices_batching_dims=(0,),
        ),
        (1, 1),
        mode=lax.GatherScatterMode.PROMISE_IN_BOUNDS,
    )


def spline_basis(phase):
    inverse = 1.0 - phase
    square = phase * phase
    cubed = square * phase
    return [
        inverse * inverse * inverse / 6.0,
        (3.0 * cubed - 6.0 * square + 4.0) / 6.0,
        (-3.0 * cubed + 3.0 * square + 3.0 * phase + 1.0) / 6.0,
        cubed / 6.0,
    ]


def cholesky_lists(matrix, extent):
    lower = [[None] * extent for _ in range(extent)]
    inverse = [None] * extent
    for column in range(extent):
        pivot = matrix[column][column]
        for k in range(column):
            pivot = pivot - lower[column][k] * lower[column][k]
        root = jnp.sqrt(pivot)
        lower[column][column] = root
        inverse[column] = 1.0 / root
        for row in range(column + 1, extent):
            entry = matrix[row][column]
            for k in range(column):
                entry = entry - lower[row][k] * lower[column][k]
            lower[row][column] = entry * inverse[column]
    return lower, inverse


def solve_lower(lower, inverse, vector):
    result = []
    for row in range(len(vector)):
        running = vector[row]
        for k in range(row):
            running = running - lower[row][k] * result[k]
        result.append(running * inverse[row])
    return result


def solve_upper(lower, inverse, vector):
    extent = len(vector)
    result = [None] * extent
    for row in reversed(range(extent)):
        running = vector[row]
        for k in range(row + 1, extent):
            running = running - lower[k][row] * result[k]
        result[row] = running * inverse[row]
    return result


def symmetric(upper, extent):
    matrix = [[None] * extent for _ in range(extent)]
    for position, (a, b) in enumerate(pairs_of(extent)):
        value = upper[position] + (RIDGE if a == b else 0.0)
        matrix[a][b] = value
        matrix[b][a] = value
    return matrix


def split_two(value):
    first = value.astype(BF16)
    return [first, (value - first.astype(F32)).astype(BF16)]


def dot_nt(left, right):
    return lax.dot_general(
        left, right, (((1,), (1,)), ((), ())), preferred_element_type=F32
    )


def two_tiles(ref, tile, rows, tiles):
    return jnp.concatenate(
        [ref[pl.ds(tile, rows, stride=tiles), :], ref[pl.ds(tile + 1, rows, stride=tiles), :]],
        axis=1,
    )


def two_rows(ref, tile):
    return jnp.concatenate([ref[pl.ds(tile, 1), :], ref[pl.ds(tile + 1, 1), :]], axis=1)


def one_hot(row, extent):
    spots = lax.broadcasted_iota(jnp.int32, (extent, row.shape[1]), 0)
    return jnp.where(spots == row, 1.0, 0.0).astype(BF16)


def by_high(part, high):
    return jnp.concatenate(
        [jnp.where(high == h, part, 0.0) for h in range(UNITS // LOW)], axis=0
    ).astype(BF16)


def block_pieces(blocks):
    width = UNITS // blocks
    for piece in range(UNITS // LANES):
        unit = piece * LANES
        yield unit // width, unit % width, unit // LOW, unit % LOW


def round_up(value, unit):
    return -(-value // unit) * unit


def layout(shape):
    count, groups, inner = shape
    plane = groups * inner
    blocks = min(plane, UNITS // LANES)
    width = UNITS // blocks
    slots = width // HALF
    mats_rows = round_up(PAIRS + -(-(GPAR * (GPAR + 1) // 2) // slots), 8)
    rhs_rows = round_up(CPAR + -(-GPAR // slots), 8)
    parts = width // LANES
    return plane, blocks, width, slots, mats_rows, rhs_rows, parts


def partner(place, k, size):
    if size & (size - 1):
        return lax.rem(place + k, size)
    other, bit = place, 1
    while bit < size:
        if k & bit:
            other = other + bit - 2 * bit * lax.rem(lax.div(place, bit), 2)
        bit *= 2
    return other


def fold_slots(rows, slots):
    lane = lax.broadcasted_iota(jnp.int32, (1, LANES), 1)
    folded = [row + pltpu.roll(row, HALF, 1) for row in rows]
    folded.append(jnp.zeros((1, LANES), F32))
    packed = []
    for start in range(0, len(rows), slots):
        parts = []
        for k in range(start, start + slots, 2):
            left, right = folded[min(k, len(rows))], folded[min(k + 1, len(rows))]
            parts.append(jnp.where(lane < HALF, left, right))
        packed.append(parts)
    return packed


def slot_sum(table, first_row, no, slots):
    row, at = first_row + no // slots, no % slots
    start = (at // 2) * LANES
    lane = lax.broadcasted_iota(jnp.int32, (1, LANES), 1)
    half = (lane < HALF) if at % 2 == 0 else (lane >= HALF)
    values = jnp.where(half, table[row : row + 1, start : start + LANES], 0.0)
    return jnp.broadcast_to(jnp.sum(values, axis=1, keepdims=True), (1, LANES))


def step_kernel(
    shape, nodes_dev,
    res_h, w_h, sp_h, si_h, sd_h, ap_h, ph_h, kn_h, cp_h, ci_h, gp_h,
    out_ref, step_ref, cstep_ref, glob_ref,
    res_ref, w_ref, sp_ref, si_ref, sd_ref, ap_ref, ph_ref, kn_ref, cp_ref, ci_ref, gp_ref,
    first_ref, att, att_two, node_spots, unit_spots, cal, rcal, acc_att, acc_cal,
    normal_ref, mats_ref, rhs_ref,
    near, pmat, prhs, zmat, zrhs, solved_ref, solved_all, white_ref, white_all,
    load_s, near_s, near_r, pmat_s, pmat_r, prhs_s, prhs_r,
    zmat_s, zmat_r, zrhs_s, zrhs_r, solved_s, solved_r, white_s, white_r,
):
    count, groups, inner = shape
    plane, blocks, width, slots, mats_rows, rhs_rows, parts = layout(shape)
    depth = count // inner
    t, g = lax.axis_index("tm"), lax.axis_index("grp")
    has_before, has_after = t > 0, t < count - 1
    z, i = lax.div(t, inner), lax.rem(t, inner)
    m = g * inner + i
    block = lax.rem(m, blocks)
    family = m - block

    pairs = [
        (si_h, si_ref), (sd_h, sd_ref), (sp_h, sp_ref), (res_h, res_ref), (w_h, w_ref),
        (ap_h, ap_ref), (ph_h, ph_ref), (kn_h, kn_ref), (cp_h, cp_ref), (ci_h, ci_ref),
        (gp_h, gp_ref),
    ]
    loads = [
        pltpu.make_async_copy(source, target, load_s.at[no])
        for no, (source, target) in enumerate(pairs)
    ]
    for load in loads:
        load.start()

    def peer_tm(k):
        return lax.rem(t + k, count)

    def peer_grp(k):
        return lax.rem(g + k, groups)

    def member(p):
        return {"tm": z * inner + lax.rem(p, inner), "grp": lax.div(p, inner)}

    def level(k):
        return {"tm": lax.rem(t + k * inner, count), "grp": g}

    barrier = pltpu.get_barrier_semaphore()

    def greet(where):
        pl.semaphore_signal(barrier, inc=1, device_id=where, device_id_type=MESH)

    for k in range(1, depth):
        greet(level(k))
    for k in range(groups):
        greet({"tm": peer_tm(1), "grp": peer_grp(k)})
        greet({"tm": peer_tm(count - 1), "grp": peer_grp(k)})
    for k in range(1, plane):
        greet(member(partner(m, k, plane)))

    for load in loads[:4]:
        load.wait()
    tiles = res_ref.shape[0]
    source_rows = sd_ref.shape[1]
    table = jnp.concatenate(
        split_two(sd_ref[...].reshape(5 * source_rows, LANES)), axis=1
    )
    for tile in range(0, tiles, 2):
        sources = two_rows(si_ref, tile)
        high, low = lax.shift_right_logical(sources, 7), lax.bitwise_and(sources, 127)
        spots = one_hot(low, LANES)
        found = jnp.dot(
            table, jnp.concatenate([spots, spots], axis=0), preferred_element_type=F32
        )
        total = None
        for c in range(5):
            factor = jnp.concatenate(
                [sp_ref[c, tile : tile + 1, :], sp_ref[c, tile + 1 : tile + 2, :]], axis=1
            )
            term = found[c * source_rows : (c + 1) * source_rows, :] * factor
            total = term if total is None else total + term
        levels = lax.broadcasted_iota(jnp.int32, (source_rows, 2 * LANES), 0)
        total = jnp.sum(jnp.where(levels == high, total, 0.0), axis=0, keepdims=True)
        first_ref[tile : tile + 1, :] = res_ref[tile : tile + 1, :] - total[:, :LANES]
        first_ref[tile + 1 : tile + 2, :] = res_ref[tile + 1 : tile + 2, :] - total[:, LANES:]
    for load in loads[4:8]:
        load.wait()
    weights = w_ref[...]
    first = first_ref[...]
    basis = spline_basis(ph_ref[...])
    axes = [ap_ref[c] for c in range(3)]
    products = [weights * axes[a] * axes[b] for a, b in pairs_of(3)]
    rights = [weights * axes[a] * first for a in range(3)]
    place = 0
    for i_ in range(4):
        for d in range(4 - i_):
            both = basis[i_] * basis[i_ + d]
            for product in products:
                att[place * tiles : (place + 1) * tiles, :] = both * product
                place += 1
    for i_ in range(4):
        for right in rights:
            att[place * tiles : (place + 1) * tiles, :] = basis[i_] * right
            place += 1
    base = t * (tiles * KPT)
    for tile in range(tiles):
        span = slice(tile * LANES, (tile + 1) * LANES)
        value = att[pl.ds(tile, ATT_ROWS, stride=tiles), :]
        att_two[:, span] = jnp.concatenate(split_two(value), axis=0)
        node_spots[:, span] = one_hot(kn_ref[tile : tile + 1, :] - base, LANES)
    sums = dot_nt(att_two[...], node_spots[...])
    acc_att[...] = sums[:ATT_ROWS] + sums[ATT_ROWS:]
    band = [None] * 5
    place = 0
    for i_ in range(4):
        for d in list(range(4 - i_)):
            rows = acc_att[place : place + 6, :]
            rows = pltpu.roll(rows, i_, 1) if i_ else rows
            band[d] = rows if band[d] is None else band[d] + rows
            place += 6
    for i_ in range(4):
        rows = acc_att[place : place + 3, :]
        rows = pltpu.roll(rows, i_, 1) if i_ else rows
        band[4] = rows if band[4] is None else band[4] + rows
        place += 3
    for d in range(4):
        normal_ref[d * 6 : (d + 1) * 6, :] = band[d]
    normal_ref[24:27, :] = band[4]
    normal_ref[27:, :] = jnp.zeros((NORMAL_ROWS - 27, LANES), F32)
    pl.semaphore_wait(barrier, depth - 1 + 2 * groups + plane - 1)

    def near_copy(offset, k):
        slot = (1 - offset) * groups + g
        return pltpu.make_async_remote_copy(
            src_ref=normal_ref,
            dst_ref=near.at[slot],
            send_sem=near_s.at[(offset + 1) * groups + k],
            recv_sem=near_r.at[slot],
            device_id={"tm": t + offset, "grp": peer_grp(k)},
            device_id_type=MESH,
        )

    def near_arrival(offset, k):
        slot = (offset + 1) * groups + peer_grp(k)
        return pltpu.make_async_remote_copy(
            src_ref=normal_ref,
            dst_ref=near.at[slot],
            send_sem=near_s.at[(offset + 1) * groups + k],
            recv_sem=near_r.at[slot],
            device_id={"tm": t + offset, "grp": peer_grp(k)},
            device_id_type=MESH,
        )

    def each_near(do):
        @pl.when(has_before)
        def _():
            for k in reversed(range(groups)):
                do(-1, k)

        @pl.when(has_after)
        def _():
            for k in reversed(range(groups)):
                do(1, k)

        for k in range(1, groups):
            do(0, k)

    each_near(lambda offset, k: near_copy(offset, k).start())

    for load in loads[8:]:
        load.wait()
    place = 0
    for a, b in pairs_of(CPAR):
        cal[place * tiles : (place + 1) * tiles, :] = weights * cp_ref[a] * cp_ref[b]
        place += 1
    cal[place * tiles :, :] = jnp.zeros(((UNIT_ROWS - place) * tiles, LANES), F32)
    global_rows = fold_slots(
        [
            jnp.sum(weights * gp_ref[a] * gp_ref[b], axis=0, keepdims=True)
            for a, b in pairs_of(GPAR)
        ],
        slots,
    )
    acc_cal[...] = jnp.zeros_like(acc_cal)

    def bin_units(no, carry):
        tile = no * 2
        units = two_rows(ci_ref, tile)
        upper, lower = lax.shift_right_logical(units, 8), lax.bitwise_and(units, 255)
        spots = one_hot(lower, LOW)
        unit_spots[no] = spots
        part = acc_cal[...]
        for piece in split_two(two_tiles(cal, tile, UNIT_ROWS, tiles)):
            part = part + dot_nt(by_high(piece.astype(F32), upper), spots)
        acc_cal[...] = part
        return carry

    lax.fori_loop(0, tiles // 2, bin_units, 0, unroll=6)
    for b_, at, h, start in block_pieces(blocks):
        mats_ref[b_, 0:UNIT_ROWS, at : at + LANES] = acc_cal[
            h * UNIT_ROWS : (h + 1) * UNIT_ROWS, start : start + LANES
        ]
    if mats_rows > UNIT_ROWS:
        mats_ref[:, UNIT_ROWS:, :] = jnp.zeros((blocks, mats_rows - UNIT_ROWS, width), F32)
    for b_ in range(blocks):
        for no, pieces in enumerate(global_rows):
            for j, piece in enumerate(pieces):
                mats_ref[b_, PAIRS + no : PAIRS + no + 1, j * LANES : (j + 1) * LANES] = piece

    def plane_copy(source, target, send, recv, k, slot):
        p = partner(m, k, plane)
        return pltpu.make_async_remote_copy(
            src_ref=source.at[lax.rem(p, blocks)],
            dst_ref=target.at[slot],
            send_sem=send.at[k],
            recv_sem=recv.at[slot],
            device_id=member(p),
            device_id_type=MESH,
        )

    def level_copy(target, send, recv, k, slot):
        return pltpu.make_async_remote_copy(
            src_ref=target.at[slot],
            dst_ref=target.at[slot],
            send_sem=send.at[k],
            recv_sem=recv.at[slot],
            device_id=level(k),
            device_id_type=MESH,
        )

    def slots_total(buffer, number):
        out = buffer[0]
        for k in range(1, number):
            out = out + buffer[k]
        return out

    for k in reversed(range(1, plane)):
        plane_copy(mats_ref, pmat, pmat_s, pmat_r, k, m).start()
    pmat[m] = mats_ref[block]
    near[groups + g] = normal_ref[...]

    @pl.when(jnp.logical_not(has_before))
    def _():
        near[0:groups] = jnp.zeros((groups, NORMAL_ROWS, LANES), F32)

    @pl.when(jnp.logical_not(has_after))
    def _():
        near[2 * groups :] = jnp.zeros((groups, NORMAL_ROWS, LANES), F32)

    each_near(lambda offset, k: near_arrival(offset, k).wait_recv())
    sums = []
    for s in range(3):
        part = near[s * groups]
        for q in range(1, groups):
            part = part + near[s * groups + q]
        sums.append(part)
    lane = lax.broadcasted_iota(jnp.int32, (NORMAL_ROWS, LANES), 1)
    before = pltpu.roll(sums[0], (HALO - nodes_dev) % LANES, 1)
    own = pltpu.roll(sums[1], HALO, 1)
    after = pltpu.roll(sums[2], (HALO + nodes_dev) % LANES, 1)
    end = nodes_dev + HALO
    normals = (
        own
        + jnp.where((lane >= 3) & (lane < HALO + 3), before, 0.0)
        + jnp.where((lane >= end) & (lane < end + HALO), after, 0.0)
    )
    spot = lax.broadcasted_iota(jnp.int32, (1, LANES), 1)
    exists = (spot >= jnp.where(has_before, 0, HALO)) & (
        spot < jnp.where(has_after, LANES, end)
    )
    normals = jnp.where(exists, normals, 0.0)
    index = {}
    for position, (a, b) in enumerate(pairs_of(3)):
        index[a, b] = index[b, a] = position
    band = [[normals[d * 6 + p : d * 6 + p + 1, :] for p in range(6)] for d in range(4)]
    right = [normals[24 + c : 25 + c, :] for c in range(3)]
    lower, inverse = cholesky_lists(symmetric(band[0], 3), 3)

    def precondition(vector):
        return solve_upper(lower, inverse, solve_lower(lower, inverse, vector))

    x = [OMEGA * value for value in precondition(right)]
    for _ in range(1, ATT_SWEEPS):
        out = [right[c] - x[c] for c in range(3)]
        for d in range(4):
            ahead = [pltpu.roll(x[c], LANES - d, 1) for c in range(3)] if d else x
            for a in range(3):
                for b in range(3):
                    out[a] = out[a] - band[d][index[a, b]] * ahead[b]
        for d in range(1, 4):
            for a in range(3):
                term = band[d][index[a, 0]] * x[0]
                for b in range(1, 3):
                    term = term + band[d][index[a, b]] * x[b]
                out[a] = out[a] - pltpu.roll(term, d, 1)
        change = precondition(out)
        x = [jnp.where(exists, x[c] + OMEGA * change[c], 0.0) for c in range(3)]

    local = kn_ref[...] - base + HALO
    tables = [jnp.broadcast_to(x[c], (tiles, LANES)) for c in range(3)]
    second = first
    for i_ in range(4):
        moved = ap_ref[0] * lane_pick(tables[0], local + i_)
        for c in range(1, 3):
            moved = moved + ap_ref[c] * lane_pick(tables[c], local + i_)
        second = second - basis[i_] * moved
    out_ref[...] = second
    weighted = weights * second
    for a in range(CPAR):
        rcal[a * tiles : (a + 1) * tiles, :] = weighted * cp_ref[a]
    rcal[CPAR * tiles :, :] = jnp.zeros(((8 - CPAR) * tiles, LANES), F32)
    global_rows = fold_slots(
        [jnp.sum(weighted * gp_ref[a], axis=0, keepdims=True) for a in range(GPAR)], slots
    )
    acc = None
    for no in range(tiles // 2):
        tile = no * 2
        upper = lax.shift_right_logical(two_rows(ci_ref, tile), 8)
        pieces = [
            by_high(p.astype(F32), upper) for p in split_two(two_tiles(rcal, tile, 8, tiles))
        ]
        part = dot_nt(jnp.concatenate(pieces, axis=0), unit_spots[no])
        acc = part if acc is None else acc + part
    rows = 8 * (UNITS // LOW)
    total = acc[0:rows, :] + acc[rows : 2 * rows, :]
    for b_, at, h, start in block_pieces(blocks):
        rhs_ref[b_, 0:8, at : at + LANES] = total[h * 8 : h * 8 + 8, start : start + LANES]
    for b_ in range(blocks):
        for no, pieces in enumerate(global_rows):
            for j, piece in enumerate(pieces):
                rhs_ref[b_, CPAR + no : CPAR + no + 1, j * LANES : (j + 1) * LANES] = piece
    for k in reversed(range(1, plane)):
        plane_copy(rhs_ref, prhs, prhs_s, prhs_r, k, m).start()
    prhs[m] = rhs_ref[block]

    for c in range(3):
        scaled = lower[c][c] * x[c]
        for k in range(c + 1, 3):
            scaled = scaled + lower[k][c] * x[k]
        moved = pltpu.roll(scaled, LANES - HALO, 1)
        step_ref[c : c + 1, :] = moved[:, 0:nodes_dev]

    for k in range(1, plane):
        plane_copy(mats_ref, pmat, pmat_s, pmat_r, k, partner(m, k, plane)).wait_recv()
    zmat[z] = slots_total(pmat, plane)
    for k in range(1, depth):
        level_copy(zmat, zmat_s, zmat_r, k, z).start()

    for k in range(1, plane):
        plane_copy(rhs_ref, prhs, prhs_s, prhs_r, k, partner(m, k, plane)).wait_recv()
    zrhs[z] = slots_total(prhs, plane)
    for k in range(1, depth):
        level_copy(zrhs, zrhs_s, zrhs_r, k, z).start()

    for k in range(1, depth):
        level_copy(zmat, zmat_s, zmat_r, k, lax.rem(z + k, depth)).wait_recv()
    unit_total = slots_total(zmat, depth)
    matrix = [unit_total[p : p + 1, :] for p in range(PAIRS)]
    lower, inverse = cholesky_lists(symmetric(matrix, CPAR), CPAR)
    upper_g = [
        slot_sum(unit_total, PAIRS, p, slots) for p in range(GPAR * (GPAR + 1) // 2)
    ]
    lower_g, inverse_g = cholesky_lists(symmetric(upper_g, GPAR), GPAR)

    for k in range(1, depth):
        level_copy(zrhs, zrhs_s, zrhs_r, k, lax.rem(z + k, depth)).wait_recv()
    total = slots_total(zrhs, depth)
    right = [total[c : c + 1, :] for c in range(CPAR)]
    white = solve_lower(lower, inverse, right)
    solved = solve_upper(lower, inverse, white)
    for c in range(CPAR):
        for j in range(parts):
            row = c * parts + j
            solved_ref[row : row + 1, :] = solved[c][:, j * LANES : (j + 1) * LANES]

    def spread_copy(source, target, send, recv, k, slot):
        return pltpu.make_async_remote_copy(
            src_ref=source,
            dst_ref=target.at[slot],
            send_sem=send.at[k],
            recv_sem=recv.at[slot],
            device_id=member(family + partner(block, k, blocks)),
            device_id_type=MESH,
        )

    for k in reversed(range(1, blocks)):
        spread_copy(solved_ref, solved_all, solved_s, solved_r, k, block).start()
    for c in range(CPAR):
        white_ref[c : c + 1, :] = white[c]
    for k in reversed(range(1, blocks)):
        spread_copy(white_ref, white_all, white_s, white_r, k, block).start()
    solved_all[block] = solved_ref[...]
    white_all[block] = white_ref[...]
    right_g = [slot_sum(total, CPAR, c, slots) for c in range(GPAR)]
    white_g = solve_lower(lower_g, inverse_g, right_g)
    solved_g = solve_upper(lower_g, inverse_g, white_g)
    spot = lax.broadcasted_iota(jnp.int32, (1, LANES), 1)
    packed = jnp.zeros((1, LANES), F32)
    for c in range(GPAR):
        packed = jnp.where(spot == c, white_g[c], packed)
    glob_ref[...] = packed[:, 0:GPAR]
    out = out_ref[...]
    for c in range(GPAR):
        out = out - gp_ref[c] * solved_g[c]
    units = ci_ref[...]
    high, low = lax.shift_right_logical(units, 7), lax.bitwise_and(units, 127)
    picked = [jnp.zeros((tiles, LANES), F32) for _ in range(CPAR)]
    for k in range(blocks):
        source = partner(block, k, blocks)
        if k:
            spread_copy(solved_ref, solved_all, solved_s, solved_r, k, source).wait_recv()
        for j in range(parts):
            here = high == source * parts + j
            for c in range(CPAR):
                row = c * parts + j
                table = jnp.broadcast_to(
                    solved_all[source, row : row + 1, :], (tiles, LANES)
                )
                picked[c] = jnp.where(here, lane_pick(table, low), picked[c])
    for c in range(CPAR):
        out = out - cp_ref[c] * picked[c]
    out_ref[...] = out
    for k in range(1, blocks):
        source = partner(block, k, blocks)
        spread_copy(white_ref, white_all, white_s, white_r, k, source).wait_recv()
    for b_ in range(blocks):
        cstep_ref[:, b_ * width : (b_ + 1) * width] = white_all[b_]
    each_near(lambda offset, k: near_copy(offset, k).wait_send())
    for k in range(1, plane):
        plane_copy(mats_ref, pmat, pmat_s, pmat_r, k, m).wait_send()
        plane_copy(rhs_ref, prhs, prhs_s, prhs_r, k, m).wait_send()
    for k in range(1, depth):
        level_copy(zmat, zmat_s, zmat_r, k, z).wait_send()
        level_copy(zrhs, zrhs_s, zrhs_r, k, z).wait_send()
    for k in range(1, blocks):
        spread_copy(solved_ref, solved_all, solved_s, solved_r, k, block).wait_send()
        spread_copy(white_ref, white_all, white_s, white_r, k, block).wait_send()


def final_kernel(*refs):
    half = len(refs) // 2
    copies = [
        pltpu.make_async_copy(refs[no], refs[half + no], refs[-1].at[no]) for no in range(half)
    ]
    for copy in copies:
        copy.start()
    for copy in copies:
        copy.wait()


def per_device(
    shape, residual, weight, source_part, source_index, source_delta, attitude_part,
    spline_phase, knot_index, calib_part, calib_index, global_part,
):
    count, groups, inner = shape
    plane, blocks, width, slots, mats_rows, rhs_rows, parts = layout(shape)
    depth = count // inner
    row_count = residual.shape[-1]
    tiles = row_count // TILE
    nodes_dev = tiles * KPT

    def flat(value):
        return value.reshape(tiles, TILE)

    def deep(value):
        return value.reshape(value.shape[0], -1, LANES)

    args = (
        flat(residual), flat(weight), deep(source_part), flat(source_index),
        deep(source_delta), deep(attitude_part), flat(spline_phase), flat(knot_index),
        deep(calib_part), flat(calib_index), deep(global_part),
    )

    def vmem(*dims):
        return pltpu.VMEM(dims, F32)

    dma = pltpu.SemaphoreType.DMA
    results = pl.pallas_call(
        functools.partial(step_kernel, shape, nodes_dev),
        out_shape=(
            vmem(tiles, LANES), vmem(3, nodes_dev), vmem(CPAR, UNITS), vmem(1, GPAR),
        ),
        scratch_shapes=[pltpu.VMEM(arg.shape, arg.dtype) for arg in args] + [
            vmem(tiles, LANES),
            vmem(ATT_ROWS * tiles, LANES),
            pltpu.VMEM((2 * ATT_ROWS, row_count), BF16),
            pltpu.VMEM((LANES, row_count), BF16),
            pltpu.VMEM((tiles // 2, LOW, 2 * LANES), BF16),
            vmem(UNIT_ROWS * tiles, LANES),
            vmem(8 * tiles, LANES),
            vmem(ATT_ROWS, LANES),
            vmem(UNIT_ROWS * (UNITS // LOW), LOW),
            vmem(NORMAL_ROWS, LANES),
            vmem(blocks, mats_rows, width),
            vmem(blocks, rhs_rows, width),
            vmem(3 * groups, NORMAL_ROWS, LANES),
            vmem(plane, mats_rows, width),
            vmem(plane, rhs_rows, width),
            vmem(depth, mats_rows, width),
            vmem(depth, rhs_rows, width),
            vmem(CPAR * parts, LANES),
            vmem(blocks, CPAR * parts, LANES),
            vmem(CPAR, width),
            vmem(blocks, CPAR, width),
            dma((len(args),)),
            dma((3 * groups,)), dma((3 * groups,)),
            dma((plane,)), dma((plane,)),
            dma((plane,)), dma((plane,)),
            dma((depth,)), dma((depth,)),
            dma((depth,)), dma((depth,)),
            dma((blocks,)), dma((blocks,)),
            dma((blocks,)), dma((blocks,)),
        ],
        in_specs=[pl.BlockSpec(memory_space=pl.ANY)] * len(args),
        compiler_params=pltpu.CompilerParams(collective_id=0, has_side_effects=True),
        name="step",
    )(*args)
    final, attitude_out, calib_step, global_step = pl.pallas_call(
        final_kernel,
        out_shape=tuple(jax.ShapeDtypeStruct(value.shape, F32) for value in results),
        in_specs=[pl.BlockSpec(memory_space=pltpu.VMEM)] * len(results),
        out_specs=(pl.BlockSpec(memory_space=pltpu.HBM),) * len(results),
        scratch_shapes=[dma((len(results),))],
        name="final",
    )(*[pltpu.with_memory_space_constraint(value, pltpu.VMEM) for value in results])
    return final.reshape(residual.shape), attitude_out, calib_step, global_step.reshape(GPAR)


def solution(mesh):
    count, groups = mesh.shape["tm"], mesh.shape["grp"]
    inner = 1 << (int(math.log2(count)) // 2)
    return jax.shard_map(
        functools.partial(per_device, (count, groups, inner)),
        mesh=mesh,
        in_specs=(
            P("tm", "grp", None),
            P("tm", "grp", None),
            P(None, "tm", "grp", None),
            P("tm", "grp", None),
            P(None, "tm", None),
            P(None, "tm", "grp", None),
            P("tm", "grp", None),
            P("tm", "grp", None),
            P(None, "tm", "grp", None),
            P("tm", "grp", None),
            P(None, "tm", "grp", None),
        ),
        out_specs=(P("tm", "grp", None), P(None, "tm"), P(), P()),
        check_vma=False,
    )
```

```python
import functools
import math

import jax
import jax.numpy as jnp
from jax import lax
from jax.experimental import pallas as pl
from jax.experimental.pallas import tpu as pltpu
from jax.sharding import PartitionSpec as P

TILE = 128
KPT = 4
UNITS = 2048
CPAR = 6
GPAR = 4
ATT_SWEEPS = 4

OMEGA = 0.6
RIDGE = 1.0
LANES = 128
LOW = 256
HALO = 3 * ATT_SWEEPS
MESH = pl.DeviceIdType.MESH
F32 = jnp.float32
BF16 = jnp.bfloat16

ATT_ROWS = 72
UNIT_ROWS = 24
PAIRS = CPAR * (CPAR + 1) // 2
HALF = 64
NORMAL_ROWS = 32


def pairs_of(extent):
    return [(a, b) for a in range(extent) for b in range(a, extent)]


def lane_pick(table, index):
    return lax.gather(
        table,
        index[..., None],
        lax.GatherDimensionNumbers(
            offset_dims=(),
            collapsed_slice_dims=(1,),
            start_index_map=(1,),
            operand_batching_dims=(0,),
            start_indices_batching_dims=(0,),
        ),
        (1, 1),
        mode=lax.GatherScatterMode.PROMISE_IN_BOUNDS,
    )


def spline_basis(phase):
    inverse = 1.0 - phase
    square = phase * phase
    cubed = square * phase
    return [
        inverse * inverse * inverse / 6.0,
        (3.0 * cubed - 6.0 * square + 4.0) / 6.0,
        (-3.0 * cubed + 3.0 * square + 3.0 * phase + 1.0) / 6.0,
        cubed / 6.0,
    ]


def cholesky_lists(matrix, extent):
    lower = [[None] * extent for _ in range(extent)]
    inverse = [None] * extent
    for column in range(extent):
        pivot = matrix[column][column]
        for k in range(column):
            pivot = pivot - lower[column][k] * lower[column][k]
        root = jnp.sqrt(pivot)
        lower[column][column] = root
        inverse[column] = 1.0 / root
        for row in range(column + 1, extent):
            entry = matrix[row][column]
            for k in range(column):
                entry = entry - lower[row][k] * lower[column][k]
            lower[row][column] = entry * inverse[column]
    return lower, inverse


def solve_lower(lower, inverse, vector):
    result = []
    for row in range(len(vector)):
        running = vector[row]
        for k in range(row):
            running = running - lower[row][k] * result[k]
        result.append(running * inverse[row])
    return result


def solve_upper(lower, inverse, vector):
    extent = len(vector)
    result = [None] * extent
    for row in reversed(range(extent)):
        running = vector[row]
        for k in range(row + 1, extent):
            running = running - lower[k][row] * result[k]
        result[row] = running * inverse[row]
    return result


def symmetric(upper, extent):
    matrix = [[None] * extent for _ in range(extent)]
    for position, (a, b) in enumerate(pairs_of(extent)):
        value = upper[position] + (RIDGE if a == b else 0.0)
        matrix[a][b] = value
        matrix[b][a] = value
    return matrix


def split_two(value):
    first = value.astype(BF16)
    return [first, (value - first.astype(F32)).astype(BF16)]


def dot_nt(left, right):
    return lax.dot_general(
        left, right, (((1,), (1,)), ((), ())), preferred_element_type=F32
    )


def two_tiles(ref, tile, rows, tiles):
    return jnp.concatenate(
        [ref[pl.ds(tile, rows, stride=tiles), :], ref[pl.ds(tile + 1, rows, stride=tiles), :]],
        axis=1,
    )


def two_rows(ref, tile):
    return jnp.concatenate([ref[pl.ds(tile, 1), :], ref[pl.ds(tile + 1, 1), :]], axis=1)


def one_hot(row, extent):
    spots = lax.broadcasted_iota(jnp.int32, (extent, row.shape[1]), 0)
    return jnp.where(spots == row, 1.0, 0.0).astype(BF16)


def by_high(part, high):
    return jnp.concatenate(
        [jnp.where(high == h, part, 0.0) for h in range(UNITS // LOW)], axis=0
    ).astype(BF16)


def block_pieces(blocks):
    width = UNITS // blocks
    for piece in range(UNITS // LANES):
        unit = piece * LANES
        yield unit // width, unit % width, unit // LOW, unit % LOW


def round_up(value, unit):
    return -(-value // unit) * unit


def layout(shape):
    count, groups, inner = shape
    plane = groups * inner
    blocks = plane // 2
    width = UNITS // blocks
    slots = width // HALF
    mats_rows = round_up(PAIRS + -(-(GPAR * (GPAR + 1) // 2) // slots), 8)
    rhs_rows = round_up(CPAR + -(-GPAR // slots), 8)
    parts = width // LANES
    return plane, blocks, width, slots, mats_rows, rhs_rows, parts


def partner(place, k, size):
    if size & (size - 1):
        return lax.rem(place + k, size)
    other, bit = place, 1
    while bit < size:
        if k & bit:
            other = other + bit - 2 * bit * lax.rem(lax.div(place, bit), 2)
        bit *= 2
    return other


def fold_slots(rows, slots):
    lane = lax.broadcasted_iota(jnp.int32, (1, LANES), 1)
    folded = [row + pltpu.roll(row, HALF, 1) for row in rows]
    folded.append(jnp.zeros((1, LANES), F32))
    packed = []
    for start in range(0, len(rows), slots):
        parts = []
        for k in range(start, start + slots, 2):
            left, right = folded[min(k, len(rows))], folded[min(k + 1, len(rows))]
            parts.append(jnp.where(lane < HALF, left, right))
        packed.append(parts)
    return packed


def slot_sum(table, first_row, no, slots):
    row, at = first_row + no // slots, no % slots
    start = (at // 2) * LANES
    lane = lax.broadcasted_iota(jnp.int32, (1, LANES), 1)
    half = (lane < HALF) if at % 2 == 0 else (lane >= HALF)
    values = jnp.where(half, table[row : row + 1, start : start + LANES], 0.0)
    return jnp.broadcast_to(jnp.sum(values, axis=1, keepdims=True), (1, LANES))


def step_kernel(
    shape, nodes_dev,
    res_h, w_h, sp_h, si_h, sd_h, ap_h, ph_h, kn_h, cp_h, ci_h, gp_h,
    out_ref, step_ref, cstep_ref, glob_ref,
    res_ref, w_ref, sp_ref, si_ref, sd_ref, ap_ref, ph_ref, kn_ref, cp_ref, ci_ref, gp_ref,
    first_ref, att, att_two, node_spots, unit_spots, cal, rcal, acc_att, acc_cal,
    normal_ref, mats_ref, rhs_ref,
    near, pmat, prhs, zmat, zrhs, solved_ref, solved_all, white_ref, white_all,
    load_s, near_s, near_r, pmat_s, pmat_r, prhs_s, prhs_r,
    zmat_s, zmat_r, zrhs_s, zrhs_r, solved_s, solved_r, white_s, white_r,
):
    count, groups, inner = shape
    plane, blocks, width, slots, mats_rows, rhs_rows, parts = layout(shape)
    depth = count // inner
    t, g = lax.axis_index("tm"), lax.axis_index("grp")
    has_before, has_after = t > 0, t < count - 1
    z, i = lax.div(t, inner), lax.rem(t, inner)
    m = g * inner + i
    block = lax.div(m, 2)
    owner = lax.rem(m, 2) == 1
    follower = jnp.logical_not(owner)

    pairs = [
        (si_h, si_ref), (sd_h, sd_ref), (sp_h, sp_ref), (res_h, res_ref), (w_h, w_ref),
        (ap_h, ap_ref), (ph_h, ph_ref), (kn_h, kn_ref), (cp_h, cp_ref), (ci_h, ci_ref),
        (gp_h, gp_ref),
    ]
    stages = [pairs[:4], pairs[4:8], pairs[8:]]
    loads = [
        pltpu.make_async_copy(source, target, load_s.at[no])
        for no, stage in enumerate(stages)
        for source, target in stage
    ]
    for load in loads:
        load.start()

    def drain(ref, sem):
        pltpu.make_async_copy(ref, ref, sem).wait()

    def loaded(no):
        size = sum(math.prod(target.shape) for _, target in stages[no]) // LANES
        drain(att.at[0:size], load_s.at[no])

    def peer_grp(k):
        return lax.rem(g + k, groups)

    def member(p):
        return {"tm": z * inner + lax.rem(p, inner), "grp": lax.div(p, inner)}

    def level(k):
        return {"tm": lax.rem(t + k * inner, count), "grp": g}

    barrier = pltpu.get_barrier_semaphore()

    def greet(where):
        pl.semaphore_signal(barrier, inc=1, device_id=where, device_id_type=MESH)

    for k in range(1, depth):
        greet(level(k))

    @pl.when(has_before)
    def _():
        for k in range(groups):
            greet({"tm": t - 1, "grp": peer_grp(k)})

    @pl.when(has_after)
    def _():
        for k in range(groups):
            greet({"tm": t + 1, "grp": peer_grp(k)})

    for k in range(1, plane):
        greet(member(partner(m, k, plane)))

    loaded(0)
    tiles = res_ref.shape[0]
    source_rows = sd_ref.shape[1]
    table = jnp.concatenate(
        split_two(sd_ref[...].reshape(5 * source_rows, LANES)), axis=1
    )
    for tile in range(0, tiles, 2):
        sources = two_rows(si_ref, tile)
        high, low = lax.shift_right_logical(sources, 7), lax.bitwise_and(sources, 127)
        spots = one_hot(low, LANES)
        found = jnp.dot(
            table, jnp.concatenate([spots, spots], axis=0), preferred_element_type=F32
        )
        total = None
        for c in range(5):
            factor = jnp.concatenate(
                [sp_ref[c, tile : tile + 1, :], sp_ref[c, tile + 1 : tile + 2, :]], axis=1
            )
            term = found[c * source_rows : (c + 1) * source_rows, :] * factor
            total = term if total is None else total + term
        levels = lax.broadcasted_iota(jnp.int32, (source_rows, 2 * LANES), 0)
        total = jnp.sum(jnp.where(levels == high, total, 0.0), axis=0, keepdims=True)
        first_ref[tile : tile + 1, :] = res_ref[tile : tile + 1, :] - total[:, :LANES]
        first_ref[tile + 1 : tile + 2, :] = res_ref[tile + 1 : tile + 2, :] - total[:, LANES:]
    loaded(1)
    weights = w_ref[...]
    first = first_ref[...]
    basis = spline_basis(ph_ref[...])
    axes = [ap_ref[c] for c in range(3)]
    products = [weights * axes[a] * axes[b] for a, b in pairs_of(3)]
    rights = [weights * axes[a] * first for a in range(3)]
    place = 0
    for i_ in range(4):
        for d in range(4 - i_):
            both = basis[i_] * basis[i_ + d]
            for product in products:
                att[place * tiles : (place + 1) * tiles, :] = both * product
                place += 1
    for i_ in range(4):
        for right in rights:
            att[place * tiles : (place + 1) * tiles, :] = basis[i_] * right
            place += 1
    base = t * (tiles * KPT)
    for tile in range(tiles):
        span = slice(tile * LANES, (tile + 1) * LANES)
        value = att[pl.ds(tile, ATT_ROWS, stride=tiles), :]
        att_two[:, span] = jnp.concatenate(split_two(value), axis=0)
        node_spots[:, span] = one_hot(kn_ref[tile : tile + 1, :] - base, LANES)
    sums = dot_nt(att_two[...], node_spots[...])
    acc_att[...] = sums[:ATT_ROWS] + sums[ATT_ROWS:]
    band = [None] * 5
    place = 0
    for i_ in range(4):
        for d in list(range(4 - i_)):
            rows = acc_att[place : place + 6, :]
            rows = pltpu.roll(rows, i_, 1) if i_ else rows
            band[d] = rows if band[d] is None else band[d] + rows
            place += 6
    for i_ in range(4):
        rows = acc_att[place : place + 3, :]
        rows = pltpu.roll(rows, i_, 1) if i_ else rows
        band[4] = rows if band[4] is None else band[4] + rows
        place += 3
    for d in range(4):
        normal_ref[d * 6 : (d + 1) * 6, :] = band[d]
    normal_ref[24:27, :] = band[4]
    normal_ref[27:, :] = jnp.zeros((NORMAL_ROWS - 27, LANES), F32)
    sides = has_before.astype(jnp.int32) + has_after.astype(jnp.int32)
    pl.semaphore_wait(barrier, depth - 1 + plane - 1 + groups * sides)

    def near_copy(offset, k):
        slot = (1 - offset) * groups + g
        return pltpu.make_async_remote_copy(
            src_ref=normal_ref,
            dst_ref=near.at[slot],
            send_sem=near_s.at[offset + 1],
            recv_sem=near_r.at[1 - offset],
            device_id={"tm": t + offset, "grp": peer_grp(k)},
            device_id_type=MESH,
        )

    def each_near(do):
        @pl.when(has_before)
        def _():
            for k in reversed(range(groups)):
                do(-1, k)

        @pl.when(has_after)
        def _():
            for k in reversed(range(groups)):
                do(1, k)

        for k in range(1, groups):
            do(0, k)

    def drain_near(sems):
        @pl.when(has_before)
        def _():
            drain(near.at[0:groups], sems.at[0])

        @pl.when(has_after)
        def _():
            drain(near.at[0:groups], sems.at[2])

        if groups > 1:
            drain(near.at[0 : groups - 1], sems.at[1])

    each_near(lambda offset, k: near_copy(offset, k).start())

    loaded(2)
    place = 0
    for a, b in pairs_of(CPAR):
        cal[place * tiles : (place + 1) * tiles, :] = weights * cp_ref[a] * cp_ref[b]
        place += 1
    cal[place * tiles :, :] = jnp.zeros(((UNIT_ROWS - place) * tiles, LANES), F32)
    global_rows = fold_slots(
        [
            jnp.sum(weights * gp_ref[a] * gp_ref[b], axis=0, keepdims=True)
            for a, b in pairs_of(GPAR)
        ],
        slots,
    )
    acc_cal[...] = jnp.zeros_like(acc_cal)

    def bin_units(no, carry):
        tile = no * 2
        units = two_rows(ci_ref, tile)
        upper, lower = lax.shift_right_logical(units, 8), lax.bitwise_and(units, 255)
        spots = one_hot(lower, LOW)
        unit_spots[no] = spots
        part = acc_cal[...]
        for piece in split_two(two_tiles(cal, tile, UNIT_ROWS, tiles)):
            part = part + dot_nt(by_high(piece.astype(F32), upper), spots)
        acc_cal[...] = part
        return carry

    lax.fori_loop(0, tiles // 2, bin_units, 0, unroll=6)
    for b_, at, h, start in block_pieces(blocks):
        mats_ref[b_, 0:UNIT_ROWS, at : at + LANES] = acc_cal[
            h * UNIT_ROWS : (h + 1) * UNIT_ROWS, start : start + LANES
        ]
    if mats_rows > UNIT_ROWS:
        mats_ref[:, UNIT_ROWS:, :] = jnp.zeros((blocks, mats_rows - UNIT_ROWS, width), F32)
    for b_ in range(blocks):
        for no, pieces in enumerate(global_rows):
            for j, piece in enumerate(pieces):
                mats_ref[b_, PAIRS + no : PAIRS + no + 1, j * LANES : (j + 1) * LANES] = piece

    def to_owners(source, target, send, recv):
        def copy(k):
            p = partner(block, k, blocks)
            pltpu.make_async_remote_copy(
                src_ref=source.at[p],
                dst_ref=target.at[m],
                send_sem=send.at[min(k, 1)],
                recv_sem=recv.at[0],
                device_id=member(2 * p + 1),
                device_id_type=MESH,
            ).start()

        for k in reversed(range(1, blocks)):
            copy(k)

        @pl.when(follower)
        def _():
            copy(0)

        @pl.when(owner)
        def _():
            target[m] = source[block]

    def sent_to_owners(source, send):
        drain(source.at[0 : blocks - 1], send.at[1])

        @pl.when(follower)
        def _():
            drain(source.at[0:1], send.at[0])

    def to_levels(target, send, recv):
        for k in range(1, depth):
            pltpu.make_async_remote_copy(
                src_ref=target.at[z],
                dst_ref=target.at[z],
                send_sem=send.at[0],
                recv_sem=recv.at[0],
                device_id=level(k),
                device_id_type=MESH,
            ).start()

    def slots_total(buffer, number):
        out = buffer[0]
        for k in range(1, number):
            out = out + buffer[k]
        return out

    to_owners(mats_ref, pmat, pmat_s, pmat_r)
    near[groups + g] = normal_ref[...]

    @pl.when(jnp.logical_not(has_before))
    def _():
        near[0:groups] = jnp.zeros((groups, NORMAL_ROWS, LANES), F32)

    @pl.when(jnp.logical_not(has_after))
    def _():
        near[2 * groups :] = jnp.zeros((groups, NORMAL_ROWS, LANES), F32)

    drain_near(near_r)
    sums = []
    for s in range(3):
        part = near[s * groups]
        for q in range(1, groups):
            part = part + near[s * groups + q]
        sums.append(part)
    lane = lax.broadcasted_iota(jnp.int32, (NORMAL_ROWS, LANES), 1)
    before = pltpu.roll(sums[0], (HALO - nodes_dev) % LANES, 1)
    own = pltpu.roll(sums[1], HALO, 1)
    after = pltpu.roll(sums[2], (HALO + nodes_dev) % LANES, 1)
    end = nodes_dev + HALO
    normals = (
        own
        + jnp.where((lane >= 3) & (lane < HALO + 3), before, 0.0)
        + jnp.where((lane >= end) & (lane < end + HALO), after, 0.0)
    )
    spot = lax.broadcasted_iota(jnp.int32, (1, LANES), 1)
    exists = (spot >= jnp.where(has_before, 0, HALO)) & (
        spot < jnp.where(has_after, LANES, end)
    )
    normals = jnp.where(exists, normals, 0.0)
    index = {}
    for position, (a, b) in enumerate(pairs_of(3)):
        index[a, b] = index[b, a] = position
    band = [[normals[d * 6 + p : d * 6 + p + 1, :] for p in range(6)] for d in range(4)]
    right = [normals[24 + c : 25 + c, :] for c in range(3)]
    lower, inverse = cholesky_lists(symmetric(band[0], 3), 3)

    def precondition(vector):
        return solve_upper(lower, inverse, solve_lower(lower, inverse, vector))

    x = [OMEGA * value for value in precondition(right)]
    for _ in range(1, ATT_SWEEPS):
        out = [right[c] - x[c] for c in range(3)]
        for d in range(4):
            ahead = [pltpu.roll(x[c], LANES - d, 1) for c in range(3)] if d else x
            for a in range(3):
                for b in range(3):
                    out[a] = out[a] - band[d][index[a, b]] * ahead[b]
        for d in range(1, 4):
            for a in range(3):
                term = band[d][index[a, 0]] * x[0]
                for b in range(1, 3):
                    term = term + band[d][index[a, b]] * x[b]
                out[a] = out[a] - pltpu.roll(term, d, 1)
        change = precondition(out)
        x = [jnp.where(exists, x[c] + OMEGA * change[c], 0.0) for c in range(3)]

    local = kn_ref[...] - base + HALO
    tables = [jnp.broadcast_to(x[c], (tiles, LANES)) for c in range(3)]
    second = first
    for i_ in range(4):
        moved = ap_ref[0] * lane_pick(tables[0], local + i_)
        for c in range(1, 3):
            moved = moved + ap_ref[c] * lane_pick(tables[c], local + i_)
        second = second - basis[i_] * moved
    out_ref[...] = second
    weighted = weights * second
    for a in range(CPAR):
        rcal[a * tiles : (a + 1) * tiles, :] = weighted * cp_ref[a]
    rcal[CPAR * tiles :, :] = jnp.zeros(((8 - CPAR) * tiles, LANES), F32)
    global_rows = fold_slots(
        [jnp.sum(weighted * gp_ref[a], axis=0, keepdims=True) for a in range(GPAR)], slots
    )
    acc = None
    for no in range(tiles // 2):
        tile = no * 2
        upper = lax.shift_right_logical(two_rows(ci_ref, tile), 8)
        pieces = [
            by_high(p.astype(F32), upper) for p in split_two(two_tiles(rcal, tile, 8, tiles))
        ]
        part = dot_nt(jnp.concatenate(pieces, axis=0), unit_spots[no])
        acc = part if acc is None else acc + part
    rows = 8 * (UNITS // LOW)
    total = acc[0:rows, :] + acc[rows : 2 * rows, :]
    for b_, at, h, start in block_pieces(blocks):
        rhs_ref[b_, 0:8, at : at + LANES] = total[h * 8 : h * 8 + 8, start : start + LANES]
    for b_ in range(blocks):
        for no, pieces in enumerate(global_rows):
            for j, piece in enumerate(pieces):
                rhs_ref[b_, CPAR + no : CPAR + no + 1, j * LANES : (j + 1) * LANES] = piece
    to_owners(rhs_ref, prhs, prhs_s, prhs_r)

    for c in range(3):
        scaled = lower[c][c] * x[c]
        for k in range(c + 1, 3):
            scaled = scaled + lower[k][c] * x[k]
        moved = pltpu.roll(scaled, LANES - HALO, 1)
        step_ref[c : c + 1, :] = moved[:, 0:nodes_dev]

    def spread(source, target, send, recv):
        for p in reversed(range(1, plane)):
            to = partner(m, p, plane)
            pltpu.make_async_remote_copy(
                src_ref=source,
                dst_ref=target.at[block],
                send_sem=send.at[0],
                recv_sem=recv.at[p // 2],
                device_id=member(to),
                device_id_type=MESH,
            ).start()

    @pl.when(owner)
    def _():
        drain(pmat.at[0 : plane - 1], pmat_r.at[0])
        zmat[z] = slots_total(pmat, plane)
        to_levels(zmat, zmat_s, zmat_r)

        drain(prhs.at[0 : plane - 1], prhs_r.at[0])
        zrhs[z] = slots_total(prhs, plane)
        to_levels(zrhs, zrhs_s, zrhs_r)

        drain(zmat.at[0 : depth - 1], zmat_r.at[0])
        unit_total = slots_total(zmat, depth)
        matrix = [unit_total[p : p + 1, :] for p in range(PAIRS)]
        lower, inverse = cholesky_lists(symmetric(matrix, CPAR), CPAR)
        upper_g = [
            slot_sum(unit_total, PAIRS, p, slots) for p in range(GPAR * (GPAR + 1) // 2)
        ]
        lower_g, inverse_g = cholesky_lists(symmetric(upper_g, GPAR), GPAR)

        drain(zrhs.at[0 : depth - 1], zrhs_r.at[0])
        total = slots_total(zrhs, depth)
        right = [total[c : c + 1, :] for c in range(CPAR)]
        white = solve_lower(lower, inverse, right)
        solved = solve_upper(lower, inverse, white)
        for c in range(CPAR):
            for j in range(parts):
                row = c * parts + j
                solved_ref[row : row + 1, :] = solved[c][:, j * LANES : (j + 1) * LANES]
        spread(solved_ref, solved_all, solved_s, solved_r)
        for c in range(CPAR):
            white_ref[c : c + 1, :] = white[c]
        right_g = [slot_sum(total, CPAR, c, slots) for c in range(GPAR)]
        white_g = solve_lower(lower_g, inverse_g, right_g)
        solved_g = solve_upper(lower_g, inverse_g, white_g)
        white_ref[CPAR:, :] = jnp.zeros((8 - CPAR, width), F32)
        spot = lax.broadcasted_iota(jnp.int32, (1, LANES), 1)
        packed = jnp.zeros((1, LANES), F32)
        for c in range(GPAR):
            packed = jnp.where(spot == c, white_g[c], packed)
            packed = jnp.where(spot == GPAR + c, solved_g[c], packed)
        white_ref[CPAR : CPAR + 1, 0:LANES] = packed
        spread(white_ref, white_all, white_s, white_r)
        solved_all[block] = solved_ref[...]
        white_all[block] = white_ref[...]

    units = ci_ref[...]
    high, low = lax.shift_right_logical(units, 7), lax.bitwise_and(units, 127)
    picked = [jnp.zeros((tiles, LANES), F32) for _ in range(CPAR)]
    for k in range(blocks):
        source = partner(block, k, blocks)
        if k:
            drain(solved_ref, solved_r.at[k])
        else:
            @pl.when(follower)
            def _():
                drain(solved_ref, solved_r.at[0])
        for j in range(parts):
            here = high == source * parts + j
            for c in range(CPAR):
                row = c * parts + j
                table = jnp.broadcast_to(
                    solved_all[source, row : row + 1, :], (tiles, LANES)
                )
                picked[c] = jnp.where(here, lane_pick(table, low), picked[c])
    out = out_ref[...]
    for c in range(CPAR):
        out = out - cp_ref[c] * picked[c]
    for k in range(blocks):
        if k:
            drain(white_ref, white_r.at[k])
        else:
            @pl.when(follower)
            def _():
                drain(white_ref, white_r.at[0])
    for b_ in range(blocks):
        cstep_ref[:, b_ * width : (b_ + 1) * width] = white_all[b_, 0:CPAR, :]
    packed = white_all[0, CPAR : CPAR + 1, 0:LANES]
    glob_ref[...] = packed[:, 0:GPAR]
    for c in range(GPAR):
        value = packed[:, GPAR + c : GPAR + c + 1]
        out = out - gp_ref[c] * jnp.broadcast_to(value, (1, LANES))
    out_ref[...] = out
    drain_near(near_s)
    sent_to_owners(mats_ref, pmat_s)
    sent_to_owners(rhs_ref, prhs_s)

    @pl.when(owner)
    def _():
        drain(zmat.at[0 : depth - 1], zmat_s.at[0])
        drain(zrhs.at[0 : depth - 1], zrhs_s.at[0])
        size = (plane - 1) * math.prod(solved_ref.shape) // LANES
        drain(att.at[0:size], solved_s.at[0])
        size = (plane - 1) * math.prod(white_ref.shape) // LANES
        drain(att.at[0:size], white_s.at[0])


def final_kernel(*refs):
    half = len(refs) // 2
    copies = [
        pltpu.make_async_copy(refs[no], refs[half + no], refs[-1].at[no]) for no in range(half)
    ]
    for copy in copies:
        copy.start()
    for copy in copies:
        copy.wait()


def per_device(
    shape, residual, weight, source_part, source_index, source_delta, attitude_part,
    spline_phase, knot_index, calib_part, calib_index, global_part,
):
    count, groups, inner = shape
    plane, blocks, width, slots, mats_rows, rhs_rows, parts = layout(shape)
    depth = count // inner
    row_count = residual.shape[-1]
    tiles = row_count // TILE
    nodes_dev = tiles * KPT

    def flat(value):
        return value.reshape(tiles, TILE)

    def deep(value):
        return value.reshape(value.shape[0], -1, LANES)

    args = (
        flat(residual), flat(weight), deep(source_part), flat(source_index),
        deep(source_delta), deep(attitude_part), flat(spline_phase), flat(knot_index),
        deep(calib_part), flat(calib_index), deep(global_part),
    )

    def vmem(*dims):
        return pltpu.VMEM(dims, F32)

    dma = pltpu.SemaphoreType.DMA
    results = pl.pallas_call(
        functools.partial(step_kernel, shape, nodes_dev),
        out_shape=(
            vmem(tiles, LANES), vmem(3, nodes_dev), vmem(CPAR, UNITS), vmem(1, GPAR),
        ),
        scratch_shapes=[pltpu.VMEM(arg.shape, arg.dtype) for arg in args] + [
            vmem(tiles, LANES),
            vmem(ATT_ROWS * tiles, LANES),
            pltpu.VMEM((2 * ATT_ROWS, row_count), BF16),
            pltpu.VMEM((LANES, row_count), BF16),
            pltpu.VMEM((tiles // 2, LOW, 2 * LANES), BF16),
            vmem(UNIT_ROWS * tiles, LANES),
            vmem(8 * tiles, LANES),
            vmem(ATT_ROWS, LANES),
            vmem(UNIT_ROWS * (UNITS // LOW), LOW),
            vmem(NORMAL_ROWS, LANES),
            vmem(blocks, mats_rows, width),
            vmem(blocks, rhs_rows, width),
            vmem(3 * groups, NORMAL_ROWS, LANES),
            vmem(plane, mats_rows, width),
            vmem(plane, rhs_rows, width),
            vmem(depth, mats_rows, width),
            vmem(depth, rhs_rows, width),
            vmem(CPAR * parts, LANES),
            vmem(blocks, CPAR * parts, LANES),
            vmem(8, width),
            vmem(blocks, 8, width),
            dma((3,)),
            dma((3,)), dma((3,)),
            dma((2,)), dma((1,)),
            dma((2,)), dma((1,)),
            dma((1,)), dma((1,)),
            dma((1,)), dma((1,)),
            dma((1,)), dma((blocks,)),
            dma((1,)), dma((blocks,)),
        ],
        in_specs=[pl.BlockSpec(memory_space=pl.ANY)] * len(args),
        compiler_params=pltpu.CompilerParams(collective_id=0, has_side_effects=True),
        name="step",
    )(*args)
    final, attitude_out, calib_step, global_step = pl.pallas_call(
        final_kernel,
        out_shape=tuple(jax.ShapeDtypeStruct(value.shape, F32) for value in results),
        in_specs=[pl.BlockSpec(memory_space=pltpu.VMEM)] * len(results),
        out_specs=(pl.BlockSpec(memory_space=pltpu.HBM),) * len(results),
        scratch_shapes=[dma((len(results),))],
        name="final",
    )(*[pltpu.with_memory_space_constraint(value, pltpu.VMEM) for value in results])
    return final.reshape(residual.shape), attitude_out, calib_step, global_step.reshape(GPAR)


def solution(mesh):
    count, groups = mesh.shape["tm"], mesh.shape["grp"]
    inner = 1 << (int(math.log2(count)) // 2)
    return jax.shard_map(
        functools.partial(per_device, (count, groups, inner)),
        mesh=mesh,
        in_specs=(
            P("tm", "grp", None),
            P("tm", "grp", None),
            P(None, "tm", "grp", None),
            P("tm", "grp", None),
            P(None, "tm", None),
            P(None, "tm", "grp", None),
            P("tm", "grp", None),
            P("tm", "grp", None),
            P(None, "tm", "grp", None),
            P("tm", "grp", None),
            P(None, "tm", "grp", None),
        ),
        out_specs=(P("tm", "grp", None), P(None, "tm"), P(), P()),
        check_vma=False,
    )
```

```python
import functools
import math

import jax
import jax.numpy as jnp
from jax import lax
from jax.experimental import pallas as pl
from jax.experimental.pallas import tpu as pltpu
from jax.sharding import PartitionSpec as P

TILE = 128
KPT = 4
UNITS = 2048
CPAR = 6
GPAR = 4
ATT_SWEEPS = 4

OMEGA = 0.6
RIDGE = 1.0
LANES = 128
LOW = 256
HALO = 3 * ATT_SWEEPS
MESH = pl.DeviceIdType.MESH
F32 = jnp.float32
BF16 = jnp.bfloat16

ATT_ROWS = 72
UNIT_ROWS = 24
PAIRS = CPAR * (CPAR + 1) // 2
HALF = 64
NORMAL_ROWS = 32


def pairs_of(extent):
    return [(a, b) for a in range(extent) for b in range(a, extent)]


def lane_pick(table, index):
    return lax.gather(
        table,
        index[..., None],
        lax.GatherDimensionNumbers(
            offset_dims=(),
            collapsed_slice_dims=(1,),
            start_index_map=(1,),
            operand_batching_dims=(0,),
            start_indices_batching_dims=(0,),
        ),
        (1, 1),
        mode=lax.GatherScatterMode.PROMISE_IN_BOUNDS,
    )


def spline_basis(phase):
    inverse = 1.0 - phase
    square = phase * phase
    cubed = square * phase
    return [
        inverse * inverse * inverse / 6.0,
        (3.0 * cubed - 6.0 * square + 4.0) / 6.0,
        (-3.0 * cubed + 3.0 * square + 3.0 * phase + 1.0) / 6.0,
        cubed / 6.0,
    ]


def cholesky_lists(matrix, extent):
    lower = [[None] * extent for _ in range(extent)]
    inverse = [None] * extent
    for column in range(extent):
        pivot = matrix[column][column]
        for k in range(column):
            pivot = pivot - lower[column][k] * lower[column][k]
        root = jnp.sqrt(pivot)
        lower[column][column] = root
        inverse[column] = 1.0 / root
        for row in range(column + 1, extent):
            entry = matrix[row][column]
            for k in range(column):
                entry = entry - lower[row][k] * lower[column][k]
            lower[row][column] = entry * inverse[column]
    return lower, inverse


def solve_lower(lower, inverse, vector):
    result = []
    for row in range(len(vector)):
        running = vector[row]
        for k in range(row):
            running = running - lower[row][k] * result[k]
        result.append(running * inverse[row])
    return result


def solve_upper(lower, inverse, vector):
    extent = len(vector)
    result = [None] * extent
    for row in reversed(range(extent)):
        running = vector[row]
        for k in range(row + 1, extent):
            running = running - lower[k][row] * result[k]
        result[row] = running * inverse[row]
    return result


def symmetric(upper, extent):
    matrix = [[None] * extent for _ in range(extent)]
    for position, (a, b) in enumerate(pairs_of(extent)):
        value = upper[position] + (RIDGE if a == b else 0.0)
        matrix[a][b] = value
        matrix[b][a] = value
    return matrix


def split_two(value):
    first = value.astype(BF16)
    return [first, (value - first.astype(F32)).astype(BF16)]


def dot_nt(left, right):
    return lax.dot_general(
        left, right, (((1,), (1,)), ((), ())), preferred_element_type=F32
    )


def two_tiles(ref, tile, rows, tiles):
    return jnp.concatenate(
        [ref[pl.ds(tile, rows, stride=tiles), :], ref[pl.ds(tile + 1, rows, stride=tiles), :]],
        axis=1,
    )


def two_rows(ref, tile):
    return jnp.concatenate([ref[pl.ds(tile, 1), :], ref[pl.ds(tile + 1, 1), :]], axis=1)


def one_hot(row, extent):
    spots = lax.broadcasted_iota(jnp.int32, (extent, row.shape[1]), 0)
    return jnp.where(spots == row, 1.0, 0.0).astype(BF16)


def by_high(part, high):
    return jnp.concatenate(
        [jnp.where(high == h, part, 0.0) for h in range(UNITS // LOW)], axis=0
    ).astype(BF16)


def block_pieces(blocks):
    width = UNITS // blocks
    for piece in range(UNITS // LANES):
        unit = piece * LANES
        yield unit // width, unit % width, unit // LOW, unit % LOW


def round_up(value, unit):
    return -(-value // unit) * unit


def layout(shape):
    count, groups, inner = shape
    plane = groups * inner
    blocks = plane // 2
    width = UNITS // blocks
    slots = width // HALF
    mats_rows = round_up(PAIRS + -(-(GPAR * (GPAR + 1) // 2) // slots), 8)
    parts = width // LANES
    rhs_rows = round_up(CPAR * parts + -(-GPAR // 2), 8)
    return plane, blocks, width, slots, mats_rows, rhs_rows, parts


def partner(place, k, size):
    if size & (size - 1):
        return lax.rem(place + k, size)
    other, bit = place, 1
    while bit < size:
        if k & bit:
            other = other + bit - 2 * bit * lax.rem(lax.div(place, bit), 2)
        bit *= 2
    return other


def fold_slots(rows, slots):
    lane = lax.broadcasted_iota(jnp.int32, (1, LANES), 1)
    folded = [row + pltpu.roll(row, HALF, 1) for row in rows]
    folded.append(jnp.zeros((1, LANES), F32))
    packed = []
    for start in range(0, len(rows), slots):
        parts = []
        for k in range(start, start + slots, 2):
            left, right = folded[min(k, len(rows))], folded[min(k + 1, len(rows))]
            parts.append(jnp.where(lane < HALF, left, right))
        packed.append(parts)
    return packed


def slot_sum(table, first_row, no, slots):
    row, at = first_row + no // slots, no % slots
    start = (at // 2) * LANES
    lane = lax.broadcasted_iota(jnp.int32, (1, LANES), 1)
    half = (lane < HALF) if at % 2 == 0 else (lane >= HALF)
    values = jnp.where(half, table[row : row + 1, start : start + LANES], 0.0)
    return jnp.broadcast_to(jnp.sum(values, axis=1, keepdims=True), (1, LANES))


def step_kernel(
    shape, nodes_dev,
    res_h, w_h, sp_h, si_h, sd_h, ap_h, ph_h, kn_h, cp_h, ci_h, gp_h,
    out_ref, step_ref, cstep_ref, glob_ref,
    res_ref, w_ref, sp_ref, si_ref, sd_ref, ap_ref, ph_ref, kn_ref, cp_ref, ci_ref, gp_ref,
    first_ref, att, unit_spots, cal, rcal, acc_att, acc_cal,
    normal_ref, mats_ref, rhs_ref,
    near, pmat, prhs, zmat, zrhs, solved_ref, solved_all, white_ref, white_all,
    load_s, near_s, near_r, sent, pmat_r, prhs_r, zmat_r, zrhs_r, solved_r, white_r,
):
    count, groups, inner = shape
    plane, blocks, width, slots, mats_rows, rhs_rows, parts = layout(shape)
    depth = count // inner
    t, g = lax.axis_index("tm"), lax.axis_index("grp")
    has_before, has_after = t > 0, t < count - 1
    z, i = lax.div(t, inner), lax.rem(t, inner)
    m = g * inner + i
    block = lax.div(m, 2)
    owner = lax.rem(m, 2) == 1
    follower = jnp.logical_not(owner)

    pairs = [
        (si_h, si_ref), (sd_h, sd_ref), (sp_h, sp_ref), (res_h, res_ref), (w_h, w_ref),
        (ap_h, ap_ref), (ph_h, ph_ref), (kn_h, kn_ref), (cp_h, cp_ref), (ci_h, ci_ref),
        (gp_h, gp_ref),
    ]
    stages = [pairs[:4], pairs[4:8], pairs[8:]]
    loads = [
        pltpu.make_async_copy(source, target, load_s.at[no])
        for no, stage in enumerate(stages)
        for source, target in stage
    ]
    for load in loads:
        load.start()

    def drain(ref, sem):
        pltpu.make_async_copy(ref, ref, sem).wait()

    def loaded(no):
        size = sum(math.prod(target.shape) for _, target in stages[no]) // LANES
        drain(att.at[0:size], load_s.at[no])

    def peer_grp(k):
        return lax.rem(g + k, groups)

    def member(p):
        return {"tm": z * inner + lax.rem(p, inner), "grp": lax.div(p, inner)}

    def level(k):
        return {"tm": lax.rem(t + k * inner, count), "grp": g}

    barrier = pltpu.get_barrier_semaphore()

    def greet(where):
        pl.semaphore_signal(barrier, inc=1, device_id=where, device_id_type=MESH)

    for k in range(1, depth):
        greet(level(k))

    @pl.when(has_before)
    def _():
        for k in range(groups):
            greet({"tm": t - 1, "grp": peer_grp(k)})

    @pl.when(has_after)
    def _():
        for k in range(groups):
            greet({"tm": t + 1, "grp": peer_grp(k)})

    for k in range(1, plane):
        greet(member(partner(m, k, plane)))

    loaded(0)
    loaded(1)
    tiles = res_ref.shape[0]
    source_rows = sd_ref.shape[1]
    table = jnp.concatenate(
        split_two(sd_ref[...].reshape(5 * source_rows, LANES)), axis=1
    )
    for tile in range(0, tiles, 2):
        sources = two_rows(si_ref, tile)
        high, low = lax.shift_right_logical(sources, 7), lax.bitwise_and(sources, 127)
        spots = one_hot(low, LANES)
        found = jnp.dot(
            table, jnp.concatenate([spots, spots], axis=0), preferred_element_type=F32
        )
        total = None
        for c in range(5):
            factor = jnp.concatenate(
                [sp_ref[c, tile : tile + 1, :], sp_ref[c, tile + 1 : tile + 2, :]], axis=1
            )
            term = found[c * source_rows : (c + 1) * source_rows, :] * factor
            total = term if total is None else total + term
        levels = lax.broadcasted_iota(jnp.int32, (source_rows, 2 * LANES), 0)
        total = jnp.sum(jnp.where(levels == high, total, 0.0), axis=0, keepdims=True)
        first_ref[tile : tile + 1, :] = res_ref[tile : tile + 1, :] - total[:, :LANES]
        first_ref[tile + 1 : tile + 2, :] = res_ref[tile + 1 : tile + 2, :] - total[:, LANES:]
    weights = w_ref[...]
    first = first_ref[...]
    basis = spline_basis(ph_ref[...])
    axes = [ap_ref[c] for c in range(3)]
    products = [weights * axes[a] * axes[b] for a, b in pairs_of(3)]
    rights = [weights * axes[a] * first for a in range(3)]
    place = 0
    for i_ in range(4):
        for d in range(4 - i_):
            both = basis[i_] * basis[i_ + d]
            for product in products:
                att[place * tiles : (place + 1) * tiles, :] = both * product
                place += 1
    for i_ in range(4):
        for right in rights:
            att[place * tiles : (place + 1) * tiles, :] = basis[i_] * right
            place += 1
    base = t * (tiles * KPT)
    sums = None
    for tile in range(0, tiles, 2):
        lhs = jnp.concatenate(split_two(two_tiles(att, tile, ATT_ROWS, tiles)), axis=0)
        part = dot_nt(lhs, one_hot(two_rows(kn_ref, tile) - base, LANES))
        sums = part if sums is None else sums + part
    acc_att[...] = sums[:ATT_ROWS] + sums[ATT_ROWS:]
    band = [None] * 5
    place = 0
    for i_ in range(4):
        for d in list(range(4 - i_)):
            rows = acc_att[place : place + 6, :]
            rows = pltpu.roll(rows, i_, 1) if i_ else rows
            band[d] = rows if band[d] is None else band[d] + rows
            place += 6
    for i_ in range(4):
        rows = acc_att[place : place + 3, :]
        rows = pltpu.roll(rows, i_, 1) if i_ else rows
        band[4] = rows if band[4] is None else band[4] + rows
        place += 3
    for d in range(4):
        normal_ref[d * 6 : (d + 1) * 6, :] = band[d]
    normal_ref[24:27, :] = band[4]
    normal_ref[27:, :] = jnp.zeros((NORMAL_ROWS - 27, LANES), F32)
    sides = has_before.astype(jnp.int32) + has_after.astype(jnp.int32)
    pl.semaphore_wait(barrier, depth - 1 + plane - 1 + groups * sides)

    def near_copy(offset, k):
        slot = (1 - offset) * groups + g
        return pltpu.make_async_remote_copy(
            src_ref=normal_ref,
            dst_ref=near.at[slot],
            send_sem=near_s.at[0],
            recv_sem=near_r.at[0],
            device_id={"tm": t + offset, "grp": peer_grp(k)},
            device_id_type=MESH,
        )

    def each_near(do):
        @pl.when(has_before)
        def _():
            for k in reversed(range(groups)):
                do(-1, k)

        @pl.when(has_after)
        def _():
            for k in reversed(range(groups)):
                do(1, k)

        for k in range(1, groups):
            do(0, k)

    def drain_near(sem):
        inside = jnp.logical_and(has_before, has_after)

        @pl.when(inside)
        def _():
            drain(near.at[0 : 3 * groups - 1], sem)

        @pl.when(jnp.logical_not(inside))
        def _():
            drain(near.at[0 : 2 * groups - 1], sem)

    each_near(lambda offset, k: near_copy(offset, k).start())

    loaded(2)
    place = 0
    for a, b in pairs_of(CPAR):
        cal[place * tiles : (place + 1) * tiles, :] = weights * cp_ref[a] * cp_ref[b]
        place += 1
    cal[place * tiles :, :] = jnp.zeros(((UNIT_ROWS - place) * tiles, LANES), F32)
    global_rows = fold_slots(
        [
            jnp.sum(weights * gp_ref[a] * gp_ref[b], axis=0, keepdims=True)
            for a, b in pairs_of(GPAR)
        ],
        slots,
    )
    acc_cal[...] = jnp.zeros_like(acc_cal)

    def bin_units(no, carry):
        tile = no * 2
        units = two_rows(ci_ref, tile)
        upper, lower = lax.shift_right_logical(units, 8), lax.bitwise_and(units, 255)
        spots = one_hot(lower, LOW)
        unit_spots[no] = one_hot(lax.bitwise_and(units, LANES - 1), LANES)
        part = acc_cal[...]
        for piece in split_two(two_tiles(cal, tile, UNIT_ROWS, tiles)):
            part = part + dot_nt(by_high(piece.astype(F32), upper), spots)
        acc_cal[...] = part
        return carry

    lax.fori_loop(0, tiles // 2, bin_units, 0, unroll=6)
    for b_, at, h, start in block_pieces(blocks):
        mats_ref[b_, 0:UNIT_ROWS, at : at + LANES] = acc_cal[
            h * UNIT_ROWS : (h + 1) * UNIT_ROWS, start : start + LANES
        ]
    if mats_rows > UNIT_ROWS:
        mats_ref[:, UNIT_ROWS:, :] = jnp.zeros((blocks, mats_rows - UNIT_ROWS, width), F32)
    for b_ in range(blocks):
        for no, pieces in enumerate(global_rows):
            for j, piece in enumerate(pieces):
                mats_ref[b_, PAIRS + no : PAIRS + no + 1, j * LANES : (j + 1) * LANES] = piece

    def to_owners(source, target, recv):
        def copy(k):
            p = partner(block, k, blocks)
            pltpu.make_async_remote_copy(
                src_ref=source.at[p],
                dst_ref=target.at[m],
                send_sem=sent.at[0],
                recv_sem=recv.at[0],
                device_id=member(2 * p + 1),
                device_id_type=MESH,
            ).start()

        for k in reversed(range(1, blocks)):
            copy(k)

        @pl.when(follower)
        def _():
            copy(0)

        @pl.when(owner)
        def _():
            target[m] = source[block]

    def to_levels(target, recv):
        for k in range(1, depth):
            pltpu.make_async_remote_copy(
                src_ref=target.at[z],
                dst_ref=target.at[z],
                send_sem=sent.at[0],
                recv_sem=recv.at[0],
                device_id=level(k),
                device_id_type=MESH,
            ).start()

    def slots_total(buffer, number):
        out = buffer[0]
        for k in range(1, number):
            out = out + buffer[k]
        return out

    to_owners(mats_ref, pmat, pmat_r)
    near[groups + g] = normal_ref[...]

    @pl.when(jnp.logical_not(has_before))
    def _():
        near[0:groups] = jnp.zeros((groups, NORMAL_ROWS, LANES), F32)

    @pl.when(jnp.logical_not(has_after))
    def _():
        near[2 * groups :] = jnp.zeros((groups, NORMAL_ROWS, LANES), F32)

    drain_near(near_r.at[0])
    sums = []
    for s in range(3):
        part = near[s * groups]
        for q in range(1, groups):
            part = part + near[s * groups + q]
        sums.append(part)
    lane = lax.broadcasted_iota(jnp.int32, (NORMAL_ROWS, LANES), 1)
    before = pltpu.roll(sums[0], (HALO - nodes_dev) % LANES, 1)
    own = pltpu.roll(sums[1], HALO, 1)
    after = pltpu.roll(sums[2], (HALO + nodes_dev) % LANES, 1)
    end = nodes_dev + HALO
    normals = (
        own
        + jnp.where((lane >= 3) & (lane < HALO + 3), before, 0.0)
        + jnp.where((lane >= end) & (lane < end + HALO), after, 0.0)
    )
    spot = lax.broadcasted_iota(jnp.int32, (1, LANES), 1)
    exists = (spot >= jnp.where(has_before, 0, HALO)) & (
        spot < jnp.where(has_after, LANES, end)
    )
    normals = jnp.where(exists, normals, 0.0)
    index = {}
    for position, (a, b) in enumerate(pairs_of(3)):
        index[a, b] = index[b, a] = position
    band = [[normals[d * 6 + p : d * 6 + p + 1, :] for p in range(6)] for d in range(4)]
    right = [normals[24 + c : 25 + c, :] for c in range(3)]
    lower, inverse = cholesky_lists(symmetric(band[0], 3), 3)

    def precondition(vector):
        return solve_upper(lower, inverse, solve_lower(lower, inverse, vector))

    turned = [
        pltpu.roll(normals[d * 6 : (d + 1) * 6], d, 1) if d else None for d in range(4)
    ]
    behind = [
        [turned[d][p : p + 1, :] for p in range(6)] if d else None for d in range(4)
    ]
    x = [OMEGA * value for value in precondition(right)]
    for _ in range(1, ATT_SWEEPS):
        out = [right[c] - x[c] for c in range(3)]
        for d in range(4):
            ahead = [pltpu.roll(x[c], LANES - d, 1) for c in range(3)] if d else x
            for a in range(3):
                for b in range(3):
                    out[a] = out[a] - band[d][index[a, b]] * ahead[b]
        for d in range(1, 4):
            back = [pltpu.roll(x[c], d, 1) for c in range(3)]
            for a in range(3):
                term = behind[d][index[a, 0]] * back[0]
                for b in range(1, 3):
                    term = term + behind[d][index[a, b]] * back[b]
                out[a] = out[a] - term
        change = precondition(out)
        x = [jnp.where(exists, x[c] + OMEGA * change[c], 0.0) for c in range(3)]

    local = kn_ref[...] - base + HALO
    tables = [jnp.broadcast_to(x[c], (tiles, LANES)) for c in range(3)]
    second = first
    for i_ in range(4):
        moved = ap_ref[0] * lane_pick(tables[0], local + i_)
        for c in range(1, 3):
            moved = moved + ap_ref[c] * lane_pick(tables[c], local + i_)
        second = second - basis[i_] * moved
    out_ref[...] = second
    weighted = weights * second
    for a in range(CPAR):
        rcal[a * tiles : (a + 1) * tiles, :] = weighted * cp_ref[a]
    global_rows = fold_slots(
        [jnp.sum(weighted * gp_ref[a], axis=0, keepdims=True) for a in range(GPAR)], 2
    )
    unit_rows = lax.broadcasted_iota(jnp.int32, (CPAR * parts, 2 * LANES), 0)
    level_of_row = lax.rem(unit_rows, parts)
    acc = None
    for no in range(tiles // 2):
        tile = no * 2
        upper = lax.shift_right_logical(two_rows(ci_ref, tile), 7)
        value = None
        for c in range(CPAR):
            row = jnp.concatenate(
                [
                    rcal[c * tiles + tile : c * tiles + tile + 1, :],
                    rcal[c * tiles + tile + 1 : c * tiles + tile + 2, :],
                ],
                axis=1,
            )
            row = jnp.broadcast_to(row, (CPAR * parts, 2 * LANES))
            value = row if c == 0 else jnp.where(unit_rows >= c * parts, row, value)
        lhs = jnp.concatenate(
            [
                jnp.where(level_of_row + b_ * parts == upper, piece.astype(F32), 0.0)
                for piece in split_two(value)
                for b_ in range(blocks)
            ],
            axis=0,
        ).astype(BF16)
        part = dot_nt(lhs, unit_spots[no])
        acc = part if acc is None else acc + part
    rows = CPAR * parts
    total = acc[0 : blocks * rows, :] + acc[blocks * rows :, :]
    for b_ in range(blocks):
        rhs_ref[b_, 0:rows, :] = total[b_ * rows : (b_ + 1) * rows, :]
        for no, pieces in enumerate(global_rows):
            rhs_ref[b_, rows + no : rows + no + 1, :] = pieces[0]
        first_free = rows + len(global_rows)
        if first_free < rhs_rows:
            rhs_ref[b_, first_free:, :] = jnp.zeros((rhs_rows - first_free, LANES), F32)
    to_owners(rhs_ref, prhs, prhs_r)

    for c in range(3):
        scaled = lower[c][c] * x[c]
        for k in range(c + 1, 3):
            scaled = scaled + lower[k][c] * x[k]
        moved = pltpu.roll(scaled, LANES - HALO, 1)
        step_ref[c : c + 1, :] = moved[:, 0:nodes_dev]

    def spread(source, target, recv, shared):
        for p in reversed(range(1, plane)):
            to = partner(m, p, plane)
            pltpu.make_async_remote_copy(
                src_ref=source,
                dst_ref=target.at[block],
                send_sem=sent.at[0],
                recv_sem=recv.at[0 if shared else p // 2],
                device_id=member(to),
                device_id_type=MESH,
            ).start()

    @pl.when(owner)
    def _():
        drain(pmat.at[0 : plane - 1], pmat_r.at[0])
        zmat[z] = slots_total(pmat, plane)
        to_levels(zmat, zmat_r)

        drain(prhs.at[0 : plane - 1], prhs_r.at[0])
        zrhs[z] = slots_total(prhs, plane)
        to_levels(zrhs, zrhs_r)

        drain(zmat.at[0 : depth - 1], zmat_r.at[0])
        unit_total = slots_total(zmat, depth)
        matrix = [unit_total[p : p + 1, :] for p in range(PAIRS)]
        lower, inverse = cholesky_lists(symmetric(matrix, CPAR), CPAR)
        upper_g = [
            slot_sum(unit_total, PAIRS, p, slots) for p in range(GPAR * (GPAR + 1) // 2)
        ]
        lower_g, inverse_g = cholesky_lists(symmetric(upper_g, GPAR), GPAR)

        drain(zrhs.at[0 : depth - 1], zrhs_r.at[0])
        total = slots_total(zrhs, depth)
        right = [
            jnp.concatenate(
                [total[c * parts + j : c * parts + j + 1, :] for j in range(parts)], axis=1
            )
            for c in range(CPAR)
        ]
        white = solve_lower(lower, inverse, right)
        solved = solve_upper(lower, inverse, white)
        for c in range(CPAR):
            for j in range(parts):
                row = c * parts + j
                solved_ref[row : row + 1, :] = solved[c][:, j * LANES : (j + 1) * LANES]
        spread(solved_ref, solved_all, solved_r, False)
        for c in range(CPAR):
            for j in range(parts):
                row = c * parts + j
                white_ref[row : row + 1, :] = white[c][:, j * LANES : (j + 1) * LANES]
        right_g = [slot_sum(total, CPAR * parts, c, 2) for c in range(GPAR)]
        white_g = solve_lower(lower_g, inverse_g, right_g)
        solved_g = solve_upper(lower_g, inverse_g, white_g)
        spot = lax.broadcasted_iota(jnp.int32, (1, LANES), 1)
        packed = jnp.zeros((1, LANES), F32)
        for c in range(GPAR):
            packed = jnp.where(spot == c, white_g[c], packed)
            packed = jnp.where(spot == GPAR + c, solved_g[c], packed)
        white_ref[CPAR * parts : CPAR * parts + 1, :] = packed
        spread(white_ref, white_all, white_r, True)
        solved_all[block] = solved_ref[...]
        white_all[block] = white_ref[...]

    units = ci_ref[...]
    high, low = lax.shift_right_logical(units, 7), lax.bitwise_and(units, 127)
    slices = [(at, min(8, tiles - at)) for at in range(0, tiles, 8)]
    highs = [high[at : at + size] for at, size in slices]
    lows = [low[at : at + size] for at, size in slices]
    picked = [[jnp.zeros((size, LANES), F32) for _, size in slices] for _ in range(CPAR)]
    for k in range(blocks):
        source = partner(block, k, blocks)
        if k:
            drain(solved_ref, solved_r.at[k])
        else:
            @pl.when(follower)
            def _():
                drain(solved_ref, solved_r.at[0])
        for n, (_, size) in enumerate(slices):
            for j in range(parts):
                here = highs[n] == source * parts + j
                for c in range(CPAR):
                    row = c * parts + j
                    table = jnp.broadcast_to(
                        solved_all[source, row : row + 1, :], (size, LANES)
                    )
                    picked[c][n] = jnp.where(here, lane_pick(table, lows[n]), picked[c][n])
    picked = [jnp.concatenate(rows, axis=0) for rows in picked]
    out = out_ref[...]
    for c in range(CPAR):
        out = out - cp_ref[c] * picked[c]

    @pl.when(owner)
    def _():
        drain(white_all.at[0 : blocks - 1], white_r.at[0])

    @pl.when(follower)
    def _():
        drain(white_all, white_r.at[0])

    for b_ in range(blocks):
        for c in range(CPAR):
            for j in range(parts):
                start = b_ * width + j * LANES
                row = c * parts + j
                cstep_ref[c : c + 1, start : start + LANES] = white_all[b_, row : row + 1, :]
    packed = white_all[0, CPAR * parts : CPAR * parts + 1, :]
    glob_ref[...] = packed[:, 0:GPAR]
    for c in range(GPAR):
        value = packed[:, GPAR + c : GPAR + c + 1]
        out = out - gp_ref[c] * jnp.broadcast_to(value, (1, LANES))
    out_ref[...] = out
    drain_near(near_s.at[0])
    size = width // LANES * mats_rows + rhs_rows

    @pl.when(owner)
    def _():
        ready = 2 * CPAR * parts + 1
        drain(
            att.at[0 : (blocks - 1 + depth - 1) * size + (plane - 1) * ready], sent.at[0]
        )

    @pl.when(follower)
    def _():
        drain(att.at[0 : blocks * size], sent.at[0])


def final_kernel(*refs):
    half = len(refs) // 2
    copies = [
        pltpu.make_async_copy(refs[no], refs[half + no], refs[-1].at[no]) for no in range(half)
    ]
    for copy in copies:
        copy.start()
    for copy in copies:
        copy.wait()


def per_device(
    shape, residual, weight, source_part, source_index, source_delta, attitude_part,
    spline_phase, knot_index, calib_part, calib_index, global_part,
):
    count, groups, inner = shape
    plane, blocks, width, slots, mats_rows, rhs_rows, parts = layout(shape)
    depth = count // inner
    row_count = residual.shape[-1]
    tiles = row_count // TILE
    nodes_dev = tiles * KPT

    def flat(value):
        return value.reshape(tiles, TILE)

    def deep(value):
        return value.reshape(value.shape[0], -1, LANES)

    args = (
        flat(residual), flat(weight), deep(source_part), flat(source_index),
        deep(source_delta), deep(attitude_part), flat(spline_phase), flat(knot_index),
        deep(calib_part), flat(calib_index), deep(global_part),
    )

    def vmem(*dims):
        return pltpu.VMEM(dims, F32)

    dma = pltpu.SemaphoreType.DMA
    results = pl.pallas_call(
        functools.partial(step_kernel, shape, nodes_dev),
        out_shape=(
            vmem(tiles, LANES), vmem(3, nodes_dev), vmem(CPAR, UNITS), vmem(1, GPAR),
        ),
        scratch_shapes=[pltpu.VMEM(arg.shape, arg.dtype) for arg in args] + [
            vmem(tiles, LANES),
            vmem(ATT_ROWS * tiles, LANES),
            pltpu.VMEM((tiles // 2, LANES, 2 * LANES), BF16),
            vmem(UNIT_ROWS * tiles, LANES),
            vmem(CPAR * tiles, LANES),
            vmem(ATT_ROWS, LANES),
            vmem(UNIT_ROWS * (UNITS // LOW), LOW),
            vmem(NORMAL_ROWS, LANES),
            vmem(blocks, mats_rows, width),
            vmem(blocks, rhs_rows, LANES),
            vmem(3 * groups, NORMAL_ROWS, LANES),
            vmem(plane, mats_rows, width),
            vmem(plane, rhs_rows, LANES),
            vmem(depth, mats_rows, width),
            vmem(depth, rhs_rows, LANES),
            vmem(CPAR * parts, LANES),
            vmem(blocks, CPAR * parts, LANES),
            vmem(CPAR * parts + 1, LANES),
            vmem(blocks, CPAR * parts + 1, LANES),
            dma((3,)), dma((1,)), dma((1,)), dma((1,)),
            dma((1,)), dma((1,)), dma((1,)), dma((1,)),
            dma((blocks,)), dma((1,)),
        ],
        in_specs=[pl.BlockSpec(memory_space=pl.ANY)] * len(args),
        compiler_params=pltpu.CompilerParams(collective_id=0, has_side_effects=True),
        name="step",
    )(*args)
    final, attitude_out, calib_step, global_step = pl.pallas_call(
        final_kernel,
        out_shape=tuple(jax.ShapeDtypeStruct(value.shape, F32) for value in results),
        in_specs=[pl.BlockSpec(memory_space=pltpu.VMEM)] * len(results),
        out_specs=(pl.BlockSpec(memory_space=pltpu.HBM),) * len(results),
        scratch_shapes=[dma((len(results),))],
        name="final",
    )(*[pltpu.with_memory_space_constraint(value, pltpu.VMEM) for value in results])
    return final.reshape(residual.shape), attitude_out, calib_step, global_step.reshape(GPAR)


def solution(mesh):
    count, groups = mesh.shape["tm"], mesh.shape["grp"]
    inner = 1 << (int(math.log2(count)) // 2)
    return jax.shard_map(
        functools.partial(per_device, (count, groups, inner)),
        mesh=mesh,
        in_specs=(
            P("tm", "grp", None),
            P("tm", "grp", None),
            P(None, "tm", "grp", None),
            P("tm", "grp", None),
            P(None, "tm", None),
            P(None, "tm", "grp", None),
            P("tm", "grp", None),
            P("tm", "grp", None),
            P(None, "tm", "grp", None),
            P("tm", "grp", None),
            P(None, "tm", "grp", None),
        ),
        out_specs=(P("tm", "grp", None), P(None, "tm"), P(), P()),
        check_vma=False,
    )
```

```python
import functools
import math

import jax
import jax.numpy as jnp
from jax import lax
from jax.experimental import pallas as pl
from jax.experimental.pallas import tpu as pltpu
from jax.sharding import PartitionSpec as P

TILE = 128
KPT = 4
UNITS = 2048
CPAR = 6
GPAR = 4
ATT_SWEEPS = 4

OMEGA = 0.6
RIDGE = 1.0
LANES = 128
LOW = 256
HALO = 3 * ATT_SWEEPS
MESH = pl.DeviceIdType.MESH
F32 = jnp.float32
BF16 = jnp.bfloat16

ATT_ROWS = 72
UNIT_ROWS = 24
PAIRS = CPAR * (CPAR + 1) // 2
HALF = 64
NORMAL_ROWS = 32


def pairs_of(extent):
    return [(a, b) for a in range(extent) for b in range(a, extent)]


def lane_pick(table, index):
    return lax.gather(
        table,
        index[..., None],
        lax.GatherDimensionNumbers(
            offset_dims=(),
            collapsed_slice_dims=(1,),
            start_index_map=(1,),
            operand_batching_dims=(0,),
            start_indices_batching_dims=(0,),
        ),
        (1, 1),
        mode=lax.GatherScatterMode.PROMISE_IN_BOUNDS,
    )


def spline_basis(phase):
    inverse = 1.0 - phase
    square = phase * phase
    cubed = square * phase
    return [
        inverse * inverse * inverse / 6.0,
        (3.0 * cubed - 6.0 * square + 4.0) / 6.0,
        (-3.0 * cubed + 3.0 * square + 3.0 * phase + 1.0) / 6.0,
        cubed / 6.0,
    ]


def cholesky_lists(matrix, extent):
    lower = [[None] * extent for _ in range(extent)]
    inverse = [None] * extent
    for column in range(extent):
        pivot = matrix[column][column]
        for k in range(column):
            pivot = pivot - lower[column][k] * lower[column][k]
        root = jnp.sqrt(pivot)
        lower[column][column] = root
        inverse[column] = 1.0 / root
        for row in range(column + 1, extent):
            entry = matrix[row][column]
            for k in range(column):
                entry = entry - lower[row][k] * lower[column][k]
            lower[row][column] = entry * inverse[column]
    return lower, inverse


def tree_sum(values):
    while len(values) > 1:
        values = [
            values[k] + values[k + 1] if k + 1 < len(values) else values[k]
            for k in range(0, len(values), 2)
        ]
    return values[0]


def solve_lower(lower, inverse, vector):
    result = []
    for row in range(len(vector)):
        running = vector[row]
        for k in range(row):
            running = running - lower[row][k] * result[k]
        result.append(running * inverse[row])
    return result


def solve_upper(lower, inverse, vector):
    extent = len(vector)
    result = [None] * extent
    for row in reversed(range(extent)):
        running = vector[row]
        for k in range(row + 1, extent):
            running = running - lower[k][row] * result[k]
        result[row] = running * inverse[row]
    return result


def symmetric(upper, extent):
    matrix = [[None] * extent for _ in range(extent)]
    for position, (a, b) in enumerate(pairs_of(extent)):
        value = upper[position] + (RIDGE if a == b else 0.0)
        matrix[a][b] = value
        matrix[b][a] = value
    return matrix


def split_two(value):
    first = value.astype(BF16)
    return [first, (value - first.astype(F32)).astype(BF16)]


def dot_nt(left, right):
    return lax.dot_general(
        left, right, (((1,), (1,)), ((), ())), preferred_element_type=F32
    )


def two_tiles(ref, tile, rows, tiles):
    return jnp.concatenate(
        [ref[pl.ds(tile, rows, stride=tiles), :], ref[pl.ds(tile + 1, rows, stride=tiles), :]],
        axis=1,
    )


def two_rows(ref, tile):
    return jnp.concatenate([ref[pl.ds(tile, 1), :], ref[pl.ds(tile + 1, 1), :]], axis=1)


def one_hot(row, extent):
    spots = lax.broadcasted_iota(jnp.int32, (extent, row.shape[1]), 0)
    return jnp.where(spots == row, 1.0, 0.0).astype(BF16)


def by_high(part, high):
    return jnp.concatenate(
        [jnp.where(high == h, part, 0.0) for h in range(UNITS // LOW)], axis=0
    ).astype(BF16)


def block_pieces(blocks):
    width = UNITS // blocks
    for piece in range(UNITS // LANES):
        unit = piece * LANES
        yield unit // width, unit % width, unit // LOW, unit % LOW


def round_up(value, unit):
    return -(-value // unit) * unit


def layout(shape):
    count, groups, inner = shape
    plane = groups * inner
    blocks = plane // 2
    width = UNITS // blocks
    slots = width // HALF
    mats_rows = round_up(PAIRS + -(-(GPAR * (GPAR + 1) // 2) // slots), 8)
    parts = width // LANES
    rhs_rows = round_up(CPAR * parts + -(-GPAR // 2), 8)
    return plane, blocks, width, slots, mats_rows, rhs_rows, parts


def partner(place, k, size):
    if size & (size - 1):
        return lax.rem(place + k, size)
    other, bit = place, 1
    while bit < size:
        if k & bit:
            other = other + bit - 2 * bit * lax.rem(lax.div(place, bit), 2)
        bit *= 2
    return other


def fold_slots(rows, slots):
    lane = lax.broadcasted_iota(jnp.int32, (1, LANES), 1)
    folded = [row + pltpu.roll(row, HALF, 1) for row in rows]
    folded.append(jnp.zeros((1, LANES), F32))
    packed = []
    for start in range(0, len(rows), slots):
        parts = []
        for k in range(start, start + slots, 2):
            left, right = folded[min(k, len(rows))], folded[min(k + 1, len(rows))]
            parts.append(jnp.where(lane < HALF, left, right))
        packed.append(parts)
    return packed


def slot_sum(table, first_row, no, slots):
    row, at = first_row + no // slots, no % slots
    start = (at // 2) * LANES
    lane = lax.broadcasted_iota(jnp.int32, (1, LANES), 1)
    half = (lane < HALF) if at % 2 == 0 else (lane >= HALF)
    values = jnp.where(half, table[row : row + 1, start : start + LANES], 0.0)
    return jnp.broadcast_to(jnp.sum(values, axis=1, keepdims=True), (1, LANES))


def step_kernel(
    shape, nodes_dev,
    res_h, w_h, sp_h, si_h, sd_h, ap_h, ph_h, kn_h, cp_h, ci_h, gp_h,
    out_ref, step_ref, cstep_ref, glob_ref,
    res_ref, w_ref, sp_ref, si_ref, sd_ref, ap_ref, ph_ref, kn_ref, cp_ref, ci_ref, gp_ref,
    first_ref, att, unit_spots, cal, rcal, acc_att, acc_cal,
    normal_ref, mats_ref, rhs_ref,
    near, pmat, prhs, zmat, zrhs, solved_ref, solved_all, white_ref, white_all,
    load_s, near_s, near_r, sent, pmat_r, prhs_r, zmat_r, zrhs_r, solved_r, white_r,
):
    count, groups, inner = shape
    plane, blocks, width, slots, mats_rows, rhs_rows, parts = layout(shape)
    depth = count // inner
    t, g = lax.axis_index("tm"), lax.axis_index("grp")
    has_before, has_after = t > 0, t < count - 1
    z, i = lax.div(t, inner), lax.rem(t, inner)
    m = g * inner + i
    block = lax.div(m, 2)
    owner = lax.rem(m, 2) == 1
    follower = jnp.logical_not(owner)

    pairs = [
        (si_h, si_ref), (sd_h, sd_ref), (sp_h, sp_ref), (res_h, res_ref), (w_h, w_ref),
        (ap_h, ap_ref), (ph_h, ph_ref), (kn_h, kn_ref), (cp_h, cp_ref), (ci_h, ci_ref),
        (gp_h, gp_ref),
    ]
    stages = [pairs[:4], pairs[4:8], pairs[8:]]
    loads = [
        pltpu.make_async_copy(source, target, load_s.at[no])
        for no, stage in enumerate(stages)
        for source, target in stage
    ]
    for load in loads:
        load.start()

    def drain(ref, sem):
        pltpu.make_async_copy(ref, ref, sem).wait()

    def loaded(no):
        size = sum(math.prod(target.shape) for _, target in stages[no]) // LANES
        drain(att.at[0:size], load_s.at[no])

    def peer_grp(k):
        return lax.rem(g + k, groups)

    def member(p):
        return {"tm": z * inner + lax.rem(p, inner), "grp": lax.div(p, inner)}

    def level(k):
        return {"tm": partner(z, k, depth) * inner + i, "grp": g}

    barrier = pltpu.get_barrier_semaphore()

    def greet(where):
        pl.semaphore_signal(barrier, inc=1, device_id=where, device_id_type=MESH)

    for k in range(1, depth):
        greet(level(k))

    @pl.when(has_before)
    def _():
        for k in range(groups):
            greet({"tm": t - 1, "grp": peer_grp(k)})

    @pl.when(has_after)
    def _():
        for k in range(groups):
            greet({"tm": t + 1, "grp": peer_grp(k)})

    for k in range(1, plane):
        greet(member(partner(m, k, plane)))

    loaded(0)
    loaded(1)
    tiles = res_ref.shape[0]
    source_rows = sd_ref.shape[1]
    table = jnp.concatenate(
        split_two(sd_ref[...].reshape(5 * source_rows, LANES)), axis=1
    )
    for tile in range(0, tiles, 2):
        sources = two_rows(si_ref, tile)
        high, low = lax.shift_right_logical(sources, 7), lax.bitwise_and(sources, 127)
        spots = one_hot(low, LANES)
        found = jnp.dot(
            table, jnp.concatenate([spots, spots], axis=0), preferred_element_type=F32
        )
        total = None
        for c in range(5):
            factor = jnp.concatenate(
                [sp_ref[c, tile : tile + 1, :], sp_ref[c, tile + 1 : tile + 2, :]], axis=1
            )
            term = found[c * source_rows : (c + 1) * source_rows, :] * factor
            total = term if total is None else total + term
        levels = lax.broadcasted_iota(jnp.int32, (source_rows, 2 * LANES), 0)
        total = jnp.sum(jnp.where(levels == high, total, 0.0), axis=0, keepdims=True)
        first_ref[tile : tile + 1, :] = res_ref[tile : tile + 1, :] - total[:, :LANES]
        first_ref[tile + 1 : tile + 2, :] = res_ref[tile + 1 : tile + 2, :] - total[:, LANES:]
    weights = w_ref[...]
    first = first_ref[...]
    basis = spline_basis(ph_ref[...])
    axes = [ap_ref[c] for c in range(3)]
    products = [weights * axes[a] * axes[b] for a, b in pairs_of(3)]
    rights = [weights * axes[a] * first for a in range(3)]
    place = 0
    for i_ in range(4):
        for d in range(4 - i_):
            both = basis[i_] * basis[i_ + d]
            for product in products:
                att[place * tiles : (place + 1) * tiles, :] = both * product
                place += 1
    for i_ in range(4):
        for right in rights:
            att[place * tiles : (place + 1) * tiles, :] = basis[i_] * right
            place += 1
    base = t * (tiles * KPT)
    sums = None
    for tile in range(0, tiles, 2):
        lhs = jnp.concatenate(split_two(two_tiles(att, tile, ATT_ROWS, tiles)), axis=0)
        part = dot_nt(lhs, one_hot(two_rows(kn_ref, tile) - base, LANES))
        sums = part if sums is None else sums + part
    acc_att[...] = sums[:ATT_ROWS] + sums[ATT_ROWS:]
    band = [None] * 5
    place = 0
    for i_ in range(4):
        for d in list(range(4 - i_)):
            rows = acc_att[place : place + 6, :]
            rows = pltpu.roll(rows, i_, 1) if i_ else rows
            band[d] = rows if band[d] is None else band[d] + rows
            place += 6
    for i_ in range(4):
        rows = acc_att[place : place + 3, :]
        rows = pltpu.roll(rows, i_, 1) if i_ else rows
        band[4] = rows if band[4] is None else band[4] + rows
        place += 3
    for d in range(4):
        normal_ref[d * 6 : (d + 1) * 6, :] = band[d]
    normal_ref[24:27, :] = band[4]
    normal_ref[27:, :] = jnp.zeros((NORMAL_ROWS - 27, LANES), F32)
    sides = has_before.astype(jnp.int32) + has_after.astype(jnp.int32)
    pl.semaphore_wait(barrier, depth - 1 + plane - 1 + groups * sides)

    def near_copy(offset, k):
        slot = (1 - offset) * groups + g
        return pltpu.make_async_remote_copy(
            src_ref=normal_ref,
            dst_ref=near.at[slot],
            send_sem=near_s.at[0],
            recv_sem=near_r.at[0],
            device_id={"tm": t + offset, "grp": peer_grp(k)},
            device_id_type=MESH,
        )

    def each_near(do):
        for k in range(1, groups):
            do(0, k)

        @pl.when(has_before)
        def _():
            for k in reversed(range(groups)):
                do(-1, k)

        @pl.when(has_after)
        def _():
            for k in reversed(range(groups)):
                do(1, k)

    def drain_near(sem):
        inside = jnp.logical_and(has_before, has_after)

        @pl.when(inside)
        def _():
            drain(near.at[0 : 3 * groups - 1], sem)

        @pl.when(jnp.logical_not(inside))
        def _():
            drain(near.at[0 : 2 * groups - 1], sem)

    each_near(lambda offset, k: near_copy(offset, k).start())

    loaded(2)
    place = 0
    for a, b in pairs_of(CPAR):
        cal[place * tiles : (place + 1) * tiles, :] = weights * cp_ref[a] * cp_ref[b]
        place += 1
    cal[place * tiles :, :] = jnp.zeros(((UNIT_ROWS - place) * tiles, LANES), F32)
    global_rows = fold_slots(
        [
            jnp.sum(weights * gp_ref[a] * gp_ref[b], axis=0, keepdims=True)
            for a, b in pairs_of(GPAR)
        ],
        slots,
    )
    acc_cal[...] = jnp.zeros_like(acc_cal)

    def bin_units(no, carry):
        tile = no * 2
        units = two_rows(ci_ref, tile)
        upper, lower = lax.shift_right_logical(units, 8), lax.bitwise_and(units, 255)
        lhs = jnp.concatenate(
            [
                by_high(piece.astype(F32), upper)
                for piece in split_two(two_tiles(cal, tile, UNIT_ROWS, tiles))
            ],
            axis=0,
        )
        acc_cal[...] = acc_cal[...] + dot_nt(lhs, one_hot(lower, LOW))
        return carry

    lax.fori_loop(0, tiles // 2, bin_units, 0, unroll=6)
    lo_rows = UNIT_ROWS * (UNITS // LOW)
    for b_, at, h, start in block_pieces(blocks):
        row = h * UNIT_ROWS
        mats_ref[b_, 0:UNIT_ROWS, at : at + LANES] = (
            acc_cal[row : row + UNIT_ROWS, start : start + LANES]
            + acc_cal[lo_rows + row : lo_rows + row + UNIT_ROWS, start : start + LANES]
        )
    if mats_rows > UNIT_ROWS:
        mats_ref[:, UNIT_ROWS:, :] = jnp.zeros((blocks, mats_rows - UNIT_ROWS, width), F32)
    for b_ in range(blocks):
        for no, pieces in enumerate(global_rows):
            for j, piece in enumerate(pieces):
                mats_ref[b_, PAIRS + no : PAIRS + no + 1, j * LANES : (j + 1) * LANES] = piece

    def to_owners(source, target, recv):
        def copy(k):
            p = partner(block, k, blocks)
            pltpu.make_async_remote_copy(
                src_ref=source.at[p],
                dst_ref=target.at[m],
                send_sem=sent.at[0],
                recv_sem=recv.at[0],
                device_id=member(2 * p + 1),
                device_id_type=MESH,
            ).start()

        for k in reversed(range(1, blocks)):
            copy(k)

        @pl.when(follower)
        def _():
            copy(0)

        @pl.when(owner)
        def _():
            target[m] = source[block]

    def to_levels(target, recv, ks):
        for k in ks:
            pltpu.make_async_remote_copy(
                src_ref=target.at[z],
                dst_ref=target.at[z],
                send_sem=sent.at[0],
                recv_sem=recv.at[0],
                device_id=level(k),
                device_id_type=MESH,
            ).start()

    def slots_total(buffer, number):
        out = buffer[0]
        for k in range(1, number):
            out = out + buffer[k]
        return out

    to_owners(mats_ref, pmat, pmat_r)
    for no in range(tiles // 2):
        unit_spots[no] = one_hot(
            lax.bitwise_and(two_rows(ci_ref, no * 2), LANES - 1), LANES
        )
    near[groups + g] = normal_ref[...]

    @pl.when(jnp.logical_not(has_before))
    def _():
        near[0:groups] = jnp.zeros((groups, NORMAL_ROWS, LANES), F32)

    @pl.when(jnp.logical_not(has_after))
    def _():
        near[2 * groups :] = jnp.zeros((groups, NORMAL_ROWS, LANES), F32)

    drain_near(near_r.at[0])
    sums = []
    for s in range(3):
        part = near[s * groups]
        for q in range(1, groups):
            part = part + near[s * groups + q]
        sums.append(part)
    lane = lax.broadcasted_iota(jnp.int32, (NORMAL_ROWS, LANES), 1)
    before = pltpu.roll(sums[0], (HALO - nodes_dev) % LANES, 1)
    own = pltpu.roll(sums[1], HALO, 1)
    after = pltpu.roll(sums[2], (HALO + nodes_dev) % LANES, 1)
    end = nodes_dev + HALO
    normals = (
        own
        + jnp.where((lane >= 3) & (lane < HALO + 3), before, 0.0)
        + jnp.where((lane >= end) & (lane < end + HALO), after, 0.0)
    )
    spot = lax.broadcasted_iota(jnp.int32, (1, LANES), 1)
    exists = (spot >= jnp.where(has_before, 0, HALO)) & (
        spot < jnp.where(has_after, LANES, end)
    )
    normals = jnp.where(exists, normals, 0.0)
    index = {}
    for position, (a, b) in enumerate(pairs_of(3)):
        index[a, b] = index[b, a] = position
    band = [[normals[d * 6 + p : d * 6 + p + 1, :] for p in range(6)] for d in range(4)]
    right = [normals[24 + c : 25 + c, :] for c in range(3)]
    lower, inverse = cholesky_lists(symmetric(band[0], 3), 3)

    low = [
        [inverse[0]],
        [-lower[1][0] * inverse[0] * inverse[1], inverse[1]],
        [None, -lower[2][1] * inverse[1] * inverse[2], inverse[2]],
    ]
    low[2][0] = -(lower[2][0] * low[0][0] + lower[2][1] * low[1][0]) * inverse[2]
    damped = {}
    for a, b in pairs_of(3):
        entry = tree_sum([low[k][a] * low[k][b] for k in range(b, 3)])
        damped[a, b] = damped[b, a] = OMEGA * entry

    def precondition(vector):
        return [tree_sum([damped[a, b] * vector[b] for b in range(3)]) for a in range(3)]

    turned = [
        pltpu.roll(normals[d * 6 : (d + 1) * 6], d, 1) if d else None for d in range(4)
    ]
    behind = [
        [turned[d][p : p + 1, :] for p in range(6)] if d else None for d in range(4)
    ]
    x = precondition(right)
    for _ in range(1, ATT_SWEEPS):
        out = [
            right[a] - x[a] - tree_sum([band[0][index[a, b]] * x[b] for b in range(3)])
            for a in range(3)
        ]
        terms = [[] for _ in range(3)]
        for d in range(1, 4):
            ahead = [pltpu.roll(x[c], LANES - d, 1) for c in range(3)]
            back = [pltpu.roll(x[c], d, 1) for c in range(3)]
            for a in range(3):
                for b in range(3):
                    terms[a].append(band[d][index[a, b]] * ahead[b])
                    terms[a].append(behind[d][index[a, b]] * back[b])
        out = [out[a] - tree_sum(terms[a]) for a in range(3)]
        change = precondition(out)
        x = [jnp.where(exists, x[c] + change[c], 0.0) for c in range(3)]

    local = kn_ref[...] - base + HALO
    tables = [jnp.broadcast_to(x[c], (tiles, LANES)) for c in range(3)]
    second = first
    for i_ in range(4):
        moved = ap_ref[0] * lane_pick(tables[0], local + i_)
        for c in range(1, 3):
            moved = moved + ap_ref[c] * lane_pick(tables[c], local + i_)
        second = second - basis[i_] * moved
    out_ref[...] = second
    weighted = weights * second
    for a in range(CPAR):
        rcal[a * tiles : (a + 1) * tiles, :] = weighted * cp_ref[a]
    global_rows = fold_slots(
        [jnp.sum(weighted * gp_ref[a], axis=0, keepdims=True) for a in range(GPAR)], 2
    )
    unit_rows = lax.broadcasted_iota(jnp.int32, (CPAR * parts, 2 * LANES), 0)
    level_of_row = lax.rem(unit_rows, parts)
    acc = None
    for no in range(tiles // 2):
        tile = no * 2
        upper = lax.shift_right_logical(two_rows(ci_ref, tile), 7)
        value = None
        for c in range(CPAR):
            row = jnp.concatenate(
                [
                    rcal[c * tiles + tile : c * tiles + tile + 1, :],
                    rcal[c * tiles + tile + 1 : c * tiles + tile + 2, :],
                ],
                axis=1,
            )
            row = jnp.broadcast_to(row, (CPAR * parts, 2 * LANES))
            value = row if c == 0 else jnp.where(unit_rows >= c * parts, row, value)
        lhs = jnp.concatenate(
            [
                jnp.where(level_of_row + b_ * parts == upper, piece.astype(F32), 0.0)
                for piece in split_two(value)
                for b_ in range(blocks)
            ],
            axis=0,
        ).astype(BF16)
        part = dot_nt(lhs, unit_spots[no])
        acc = part if acc is None else acc + part
    rows = CPAR * parts
    total = acc[0 : blocks * rows, :] + acc[blocks * rows :, :]
    for b_ in range(blocks):
        rhs_ref[b_, 0:rows, :] = total[b_ * rows : (b_ + 1) * rows, :]
        for no, pieces in enumerate(global_rows):
            rhs_ref[b_, rows + no : rows + no + 1, :] = pieces[0]
        first_free = rows + len(global_rows)
        if first_free < rhs_rows:
            rhs_ref[b_, first_free:, :] = jnp.zeros((rhs_rows - first_free, LANES), F32)
    to_owners(rhs_ref, prhs, prhs_r)

    for c in range(3):
        scaled = lower[c][c] * x[c]
        for k in range(c + 1, 3):
            scaled = scaled + lower[k][c] * x[k]
        moved = pltpu.roll(scaled, LANES - HALO, 1)
        step_ref[c : c + 1, :] = moved[:, 0:nodes_dev]

    def spread(source, target, recv, shared):
        for p in reversed(range(1, plane)):
            to = partner(m, p, plane)
            pltpu.make_async_remote_copy(
                src_ref=source,
                dst_ref=target.at[block],
                send_sem=sent.at[0],
                recv_sem=recv.at[0 if shared else p // 2],
                device_id=member(to),
                device_id_type=MESH,
            ).start()

    @pl.when(owner)
    def _():
        drain(pmat.at[0 : plane - 1], pmat_r.at[0])
        zmat[z] = slots_total(pmat, plane)
        to_levels(zmat, zmat_r, reversed(range(1, depth)))

        drain(prhs.at[0 : plane - 1], prhs_r.at[0])
        zrhs[z] = slots_total(prhs, plane)
        to_levels(zrhs, zrhs_r, reversed(range(1, depth)))

        drain(zmat.at[0 : depth - 1], zmat_r.at[0])
        unit_total = slots_total(zmat, depth)
        matrix = [unit_total[p : p + 1, :] for p in range(PAIRS)]
        lower, inverse = cholesky_lists(symmetric(matrix, CPAR), CPAR)
        upper_g = [
            slot_sum(unit_total, PAIRS, p, slots) for p in range(GPAR * (GPAR + 1) // 2)
        ]
        lower_g, inverse_g = cholesky_lists(symmetric(upper_g, GPAR), GPAR)

        drain(zrhs.at[0 : depth - 1], zrhs_r.at[0])
        total = slots_total(zrhs, depth)
        right = [
            jnp.concatenate(
                [total[c * parts + j : c * parts + j + 1, :] for j in range(parts)], axis=1
            )
            for c in range(CPAR)
        ]
        white = solve_lower(lower, inverse, right)
        solved = solve_upper(lower, inverse, white)
        for c in range(CPAR):
            for j in range(parts):
                row = c * parts + j
                solved_ref[row : row + 1, :] = solved[c][:, j * LANES : (j + 1) * LANES]
        spread(solved_ref, solved_all, solved_r, False)
        for c in range(CPAR):
            for j in range(parts):
                row = c * parts + j
                white_ref[row : row + 1, :] = white[c][:, j * LANES : (j + 1) * LANES]
        right_g = [slot_sum(total, CPAR * parts, c, 2) for c in range(GPAR)]
        white_g = solve_lower(lower_g, inverse_g, right_g)
        solved_g = solve_upper(lower_g, inverse_g, white_g)
        spot = lax.broadcasted_iota(jnp.int32, (1, LANES), 1)
        packed = jnp.zeros((1, LANES), F32)
        for c in range(GPAR):
            packed = jnp.where(spot == c, white_g[c], packed)
            packed = jnp.where(spot == GPAR + c, solved_g[c], packed)
        white_ref[CPAR * parts : CPAR * parts + 1, :] = packed
        spread(white_ref, white_all, white_r, True)
        solved_all[block] = solved_ref[...]
        white_all[block] = white_ref[...]

    units = ci_ref[...]
    high, low = lax.shift_right_logical(units, 7), lax.bitwise_and(units, 127)
    slices = [(at, min(8, tiles - at)) for at in range(0, tiles, 8)]
    highs = [high[at : at + size] for at, size in slices]
    lows = [low[at : at + size] for at, size in slices]
    picked = [[jnp.zeros((size, LANES), F32) for _, size in slices] for _ in range(CPAR)]
    for k in range(blocks):
        source = partner(block, k, blocks)
        if k:
            drain(solved_ref, solved_r.at[k])
        else:
            @pl.when(follower)
            def _():
                drain(solved_ref, solved_r.at[0])
        for n, (_, size) in enumerate(slices):
            for j in range(parts):
                here = highs[n] == source * parts + j
                for c in range(CPAR):
                    row = c * parts + j
                    table = jnp.broadcast_to(
                        solved_all[source, row : row + 1, :], (size, LANES)
                    )
                    picked[c][n] = jnp.where(here, lane_pick(table, lows[n]), picked[c][n])
    picked = [jnp.concatenate(rows, axis=0) for rows in picked]
    out = out_ref[...]
    for c in range(CPAR):
        out = out - cp_ref[c] * picked[c]

    @pl.when(owner)
    def _():
        drain(white_all.at[0 : blocks - 1], white_r.at[0])

    @pl.when(follower)
    def _():
        drain(white_all, white_r.at[0])

    for b_ in range(blocks):
        for c in range(CPAR):
            for j in range(parts):
                start = b_ * width + j * LANES
                row = c * parts + j
                cstep_ref[c : c + 1, start : start + LANES] = white_all[b_, row : row + 1, :]
    packed = white_all[0, CPAR * parts : CPAR * parts + 1, :]
    glob_ref[...] = packed[:, 0:GPAR]
    for c in range(GPAR):
        value = packed[:, GPAR + c : GPAR + c + 1]
        out = out - gp_ref[c] * jnp.broadcast_to(value, (1, LANES))
    out_ref[...] = out
    drain_near(near_s.at[0])
    size = width // LANES * mats_rows + rhs_rows

    @pl.when(owner)
    def _():
        ready = 2 * CPAR * parts + 1
        drain(
            att.at[0 : (blocks - 1 + depth - 1) * size + (plane - 1) * ready], sent.at[0]
        )

    @pl.when(follower)
    def _():
        drain(att.at[0 : blocks * size], sent.at[0])


def final_kernel(*refs):
    half = len(refs) // 2
    copies = [
        pltpu.make_async_copy(refs[no], refs[half + no], refs[-1].at[no]) for no in range(half)
    ]
    for copy in copies:
        copy.start()
    for copy in copies:
        copy.wait()


def per_device(
    shape, residual, weight, source_part, source_index, source_delta, attitude_part,
    spline_phase, knot_index, calib_part, calib_index, global_part,
):
    count, groups, inner = shape
    plane, blocks, width, slots, mats_rows, rhs_rows, parts = layout(shape)
    depth = count // inner
    row_count = residual.shape[-1]
    tiles = row_count // TILE
    nodes_dev = tiles * KPT

    def flat(value):
        return value.reshape(tiles, TILE)

    def deep(value):
        return value.reshape(value.shape[0], -1, LANES)

    args = (
        flat(residual), flat(weight), deep(source_part), flat(source_index),
        deep(source_delta), deep(attitude_part), flat(spline_phase), flat(knot_index),
        deep(calib_part), flat(calib_index), deep(global_part),
    )

    def vmem(*dims):
        return pltpu.VMEM(dims, F32)

    dma = pltpu.SemaphoreType.DMA
    results = pl.pallas_call(
        functools.partial(step_kernel, shape, nodes_dev),
        out_shape=(
            vmem(tiles, LANES), vmem(3, nodes_dev), vmem(CPAR, UNITS), vmem(1, GPAR),
        ),
        scratch_shapes=[pltpu.VMEM(arg.shape, arg.dtype) for arg in args] + [
            vmem(tiles, LANES),
            vmem(ATT_ROWS * tiles, LANES),
            pltpu.VMEM((tiles // 2, LANES, 2 * LANES), BF16),
            vmem(UNIT_ROWS * tiles, LANES),
            vmem(CPAR * tiles, LANES),
            vmem(ATT_ROWS, LANES),
            vmem(2 * UNIT_ROWS * (UNITS // LOW), LOW),
            vmem(NORMAL_ROWS, LANES),
            vmem(blocks, mats_rows, width),
            vmem(blocks, rhs_rows, LANES),
            vmem(3 * groups, NORMAL_ROWS, LANES),
            vmem(plane, mats_rows, width),
            vmem(plane, rhs_rows, LANES),
            vmem(depth, mats_rows, width),
            vmem(depth, rhs_rows, LANES),
            vmem(CPAR * parts, LANES),
            vmem(blocks, CPAR * parts, LANES),
            vmem(CPAR * parts + 1, LANES),
            vmem(blocks, CPAR * parts + 1, LANES),
            dma((3,)), dma((1,)), dma((1,)), dma((1,)),
            dma((1,)), dma((1,)), dma((1,)), dma((1,)),
            dma((blocks,)), dma((1,)),
        ],
        in_specs=[pl.BlockSpec(memory_space=pl.ANY)] * len(args),
        compiler_params=pltpu.CompilerParams(collective_id=0, has_side_effects=True),
        name="step",
    )(*args)
    final, attitude_out, calib_step, global_step = pl.pallas_call(
        final_kernel,
        out_shape=tuple(jax.ShapeDtypeStruct(value.shape, F32) for value in results),
        in_specs=[pl.BlockSpec(memory_space=pltpu.VMEM)] * len(results),
        out_specs=(pl.BlockSpec(memory_space=pltpu.HBM),) * len(results),
        scratch_shapes=[dma((len(results),))],
        name="final",
    )(*[pltpu.with_memory_space_constraint(value, pltpu.VMEM) for value in results])
    return final.reshape(residual.shape), attitude_out, calib_step, global_step.reshape(GPAR)


def solution(mesh):
    count, groups = mesh.shape["tm"], mesh.shape["grp"]
    inner = 1 << (int(math.log2(count)) // 2)
    return jax.shard_map(
        functools.partial(per_device, (count, groups, inner)),
        mesh=mesh,
        in_specs=(
            P("tm", "grp", None),
            P("tm", "grp", None),
            P(None, "tm", "grp", None),
            P("tm", "grp", None),
            P(None, "tm", None),
            P(None, "tm", "grp", None),
            P("tm", "grp", None),
            P("tm", "grp", None),
            P(None, "tm", "grp", None),
            P("tm", "grp", None),
            P(None, "tm", "grp", None),
        ),
        out_specs=(P("tm", "grp", None), P(None, "tm"), P(), P()),
        check_vma=False,
    )
```

```python
import functools
import math

import jax
import jax.numpy as jnp
from jax import lax
from jax.experimental import pallas as pl
from jax.experimental.pallas import tpu as pltpu
from jax.sharding import PartitionSpec as P

TILE = 128
KPT = 4
UNITS = 2048
CPAR = 6
GPAR = 4
ATT_SWEEPS = 4

OMEGA = 0.6
RIDGE = 1.0
LANES = 128
LOW = 256
HALO = 3 * ATT_SWEEPS
MESH = pl.DeviceIdType.MESH
F32 = jnp.float32
BF16 = jnp.bfloat16

ATT_ROWS = 72
UNIT_ROWS = 24
PAIRS = CPAR * (CPAR + 1) // 2
HALF = 64
NORMAL_ROWS = 32


def pairs_of(extent):
    return [(a, b) for a in range(extent) for b in range(a, extent)]


def lane_pick(table, index):
    return lax.gather(
        table,
        index[..., None],
        lax.GatherDimensionNumbers(
            offset_dims=(),
            collapsed_slice_dims=(1,),
            start_index_map=(1,),
            operand_batching_dims=(0,),
            start_indices_batching_dims=(0,),
        ),
        (1, 1),
        mode=lax.GatherScatterMode.PROMISE_IN_BOUNDS,
    )


def spline_basis(phase):
    inverse = 1.0 - phase
    square = phase * phase
    cubed = square * phase
    return [
        inverse * inverse * inverse / 6.0,
        (3.0 * cubed - 6.0 * square + 4.0) / 6.0,
        (-3.0 * cubed + 3.0 * square + 3.0 * phase + 1.0) / 6.0,
        cubed / 6.0,
    ]


def cholesky_lists(matrix, extent):
    lower = [[None] * extent for _ in range(extent)]
    inverse = [None] * extent
    for column in range(extent):
        pivot = matrix[column][column]
        for k in range(column):
            pivot = pivot - lower[column][k] * lower[column][k]
        root = jnp.sqrt(pivot)
        lower[column][column] = root
        inverse[column] = 1.0 / root
        for row in range(column + 1, extent):
            entry = matrix[row][column]
            for k in range(column):
                entry = entry - lower[row][k] * lower[column][k]
            lower[row][column] = entry * inverse[column]
    return lower, inverse


def tree_sum(values):
    while len(values) > 1:
        values = [
            values[k] + values[k + 1] if k + 1 < len(values) else values[k]
            for k in range(0, len(values), 2)
        ]
    return values[0]


def solve_lower(lower, inverse, vector):
    result = []
    for row in range(len(vector)):
        running = vector[row]
        for k in range(row):
            running = running - lower[row][k] * result[k]
        result.append(running * inverse[row])
    return result


def solve_upper(lower, inverse, vector):
    extent = len(vector)
    result = [None] * extent
    for row in reversed(range(extent)):
        running = vector[row]
        for k in range(row + 1, extent):
            running = running - lower[k][row] * result[k]
        result[row] = running * inverse[row]
    return result


def symmetric(upper, extent):
    matrix = [[None] * extent for _ in range(extent)]
    for position, (a, b) in enumerate(pairs_of(extent)):
        value = upper[position] + (RIDGE if a == b else 0.0)
        matrix[a][b] = value
        matrix[b][a] = value
    return matrix


def split_two(value):
    first = value.astype(BF16)
    return [first, (value - first.astype(F32)).astype(BF16)]


def dot_nt(left, right):
    return lax.dot_general(
        left, right, (((1,), (1,)), ((), ())), preferred_element_type=F32
    )


def two_tiles(ref, tile, rows, tiles):
    return jnp.concatenate(
        [ref[pl.ds(tile, rows, stride=tiles), :], ref[pl.ds(tile + 1, rows, stride=tiles), :]],
        axis=1,
    )


def two_rows(ref, tile):
    return jnp.concatenate([ref[pl.ds(tile, 1), :], ref[pl.ds(tile + 1, 1), :]], axis=1)


def one_hot(row, extent):
    spots = lax.broadcasted_iota(jnp.int32, (extent, row.shape[1]), 0)
    return jnp.where(spots == row, 1.0, 0.0).astype(BF16)


def by_high(part, high):
    return jnp.concatenate(
        [jnp.where(high == h, part, 0.0) for h in range(UNITS // LOW)], axis=0
    ).astype(BF16)


def block_pieces(blocks):
    width = UNITS // blocks
    for piece in range(UNITS // LANES):
        unit = piece * LANES
        yield unit // width, unit % width, unit // LOW, unit % LOW


def round_up(value, unit):
    return -(-value // unit) * unit


def layout(shape):
    count, groups, inner = shape
    plane = groups * inner
    blocks = plane // 2
    width = UNITS // blocks
    slots = width // HALF
    mats_rows = round_up(PAIRS + -(-(GPAR * (GPAR + 1) // 2) // slots), 8)
    parts = width // LANES
    rhs_rows = CPAR * parts + -(-GPAR // 2)
    return plane, blocks, width, slots, mats_rows, rhs_rows, parts


def partner(place, k, size):
    if size & (size - 1):
        return lax.rem(place + k, size)
    other, bit = place, 1
    while bit < size:
        if k & bit:
            other = other + bit - 2 * bit * lax.rem(lax.div(place, bit), 2)
        bit *= 2
    return other


def fold_slots(rows, slots):
    lane = lax.broadcasted_iota(jnp.int32, (1, LANES), 1)
    folded = [row + pltpu.roll(row, HALF, 1) for row in rows]
    folded.append(jnp.zeros((1, LANES), F32))
    packed = []
    for start in range(0, len(rows), slots):
        parts = []
        for k in range(start, start + slots, 2):
            left, right = folded[min(k, len(rows))], folded[min(k + 1, len(rows))]
            parts.append(jnp.where(lane < HALF, left, right))
        packed.append(parts)
    return packed


def slot_sum(table, first_row, no, slots):
    row, at = first_row + no // slots, no % slots
    start = (at // 2) * LANES
    lane = lax.broadcasted_iota(jnp.int32, (1, LANES), 1)
    half = (lane < HALF) if at % 2 == 0 else (lane >= HALF)
    values = jnp.where(half, table[row : row + 1, start : start + LANES], 0.0)
    return jnp.broadcast_to(jnp.sum(values, axis=1, keepdims=True), (1, LANES))


def step_kernel(
    shape, nodes_dev,
    res_h, w_h, sp_h, si_h, sd_h, ap_h, ph_h, kn_h, cp_h, ci_h, gp_h,
    out_ref, step_ref, cstep_ref, glob_ref,
    res_ref, w_ref, sp_ref, si_ref, sd_ref, ap_ref, ph_ref, kn_ref, cp_ref, ci_ref, gp_ref,
    first_ref, att, by_node, unit_spots, cal, rcal, acc_att, acc_cal,
    normal_ref, mats_ref, rhs_ref,
    near, pmat, prhs, zmat, zrhs, solved_ref, solved_all, white_ref, white_all,
    load_s, near_s, near_r, sent, pmat_r, prhs_r, zmat_r, zrhs_r, solved_r, white_r,
):
    count, groups, inner = shape
    plane, blocks, width, slots, mats_rows, rhs_rows, parts = layout(shape)
    depth = count // inner
    t, g = lax.axis_index("tm"), lax.axis_index("grp")
    has_before, has_after = t > 0, t < count - 1
    z, i = lax.div(t, inner), lax.rem(t, inner)
    m = g * inner + i
    block = lax.div(m, 2)
    owner = lax.rem(m, 2) == 1
    follower = jnp.logical_not(owner)

    pairs = [
        (si_h, si_ref), (sd_h, sd_ref), (sp_h, sp_ref), (res_h, res_ref), (w_h, w_ref),
        (ap_h, ap_ref), (ph_h, ph_ref), (kn_h, kn_ref), (cp_h, cp_ref), (ci_h, ci_ref),
        (gp_h, gp_ref),
    ]
    stages = [pairs[:4], pairs[4:8], pairs[8:]]
    loads = [
        pltpu.make_async_copy(source, target, load_s.at[no])
        for no, stage in enumerate(stages)
        for source, target in stage
    ]
    for load in loads:
        load.start()

    def drain(ref, sem):
        pltpu.make_async_copy(ref, ref, sem).wait()

    def loaded(no):
        size = sum(math.prod(target.shape) for _, target in stages[no]) // LANES
        drain(att.at[0:size], load_s.at[no])

    def peer_grp(k):
        return lax.rem(g + k, groups)

    def member(p):
        return {"tm": z * inner + lax.rem(p, inner), "grp": lax.div(p, inner)}

    def level(k):
        return {"tm": partner(z, k, depth) * inner + i, "grp": g}

    barrier = pltpu.get_barrier_semaphore()

    def greet(where):
        pl.semaphore_signal(barrier, inc=1, device_id=where, device_id_type=MESH)

    for k in range(1, depth):
        greet(level(k))

    @pl.when(has_before)
    def _():
        for k in range(groups):
            greet({"tm": t - 1, "grp": peer_grp(k)})

    @pl.when(has_after)
    def _():
        for k in range(groups):
            greet({"tm": t + 1, "grp": peer_grp(k)})

    for k in range(1, plane):
        greet(member(partner(m, k, plane)))

    loaded(0)
    loaded(1)
    tiles = res_ref.shape[0]
    source_rows = sd_ref.shape[1]
    table = jnp.concatenate(
        split_two(sd_ref[...].reshape(5 * source_rows, LANES)), axis=1
    )
    for tile in range(0, tiles, 2):
        sources = two_rows(si_ref, tile)
        high, low = lax.shift_right_logical(sources, 7), lax.bitwise_and(sources, 127)
        spots = one_hot(low, LANES)
        found = jnp.dot(
            table, jnp.concatenate([spots, spots], axis=0), preferred_element_type=F32
        )
        total = None
        for c in range(5):
            factor = jnp.concatenate(
                [sp_ref[c, tile : tile + 1, :], sp_ref[c, tile + 1 : tile + 2, :]], axis=1
            )
            term = found[c * source_rows : (c + 1) * source_rows, :] * factor
            total = term if total is None else total + term
        levels = lax.broadcasted_iota(jnp.int32, (source_rows, 2 * LANES), 0)
        total = jnp.sum(jnp.where(levels == high, total, 0.0), axis=0, keepdims=True)
        first_ref[tile : tile + 1, :] = res_ref[tile : tile + 1, :] - total[:, :LANES]
        first_ref[tile + 1 : tile + 2, :] = res_ref[tile + 1 : tile + 2, :] - total[:, LANES:]
    weights = w_ref[...]
    first = first_ref[...]
    basis = spline_basis(ph_ref[...])
    axes = [ap_ref[c] for c in range(3)]
    products = [weights * axes[a] * axes[b] for a, b in pairs_of(3)]
    rights = [weights * axes[a] * first for a in range(3)]
    place = 0
    for i_ in range(4):
        for d in range(4 - i_):
            both = basis[i_] * basis[i_ + d]
            for product in products:
                att[place * tiles : (place + 1) * tiles, :] = both * product
                place += 1
    for i_ in range(4):
        for right in rights:
            att[place * tiles : (place + 1) * tiles, :] = basis[i_] * right
            place += 1
    base = t * (tiles * KPT)
    by_node[...] = jnp.zeros_like(by_node)
    for tile in range(0, tiles, 2):
        spots = one_hot(two_rows(kn_ref, tile) - (base + tile * KPT), 16)
        part = None
        for piece in split_two(two_tiles(att, tile, ATT_ROWS, tiles)):
            term = dot_nt(spots, piece)
            part = term if part is None else part + term
        by_node[tile * KPT : (tile + 2) * KPT, 0:ATT_ROWS] = part[0 : 2 * KPT, :]
    acc_att[...] = jnp.transpose(by_node[...])[0:ATT_ROWS, :]
    band = [None] * 5
    place = 0
    for i_ in range(4):
        for d in list(range(4 - i_)):
            rows = acc_att[place : place + 6, :]
            rows = pltpu.roll(rows, i_, 1) if i_ else rows
            band[d] = rows if band[d] is None else band[d] + rows
            place += 6
    for i_ in range(4):
        rows = acc_att[place : place + 3, :]
        rows = pltpu.roll(rows, i_, 1) if i_ else rows
        band[4] = rows if band[4] is None else band[4] + rows
        place += 3
    for d in range(4):
        normal_ref[d * 6 : (d + 1) * 6, :] = band[d]
    normal_ref[24:27, :] = band[4]
    normal_ref[27:, :] = jnp.zeros((NORMAL_ROWS - 27, LANES), F32)
    sides = has_before.astype(jnp.int32) + has_after.astype(jnp.int32)
    pl.semaphore_wait(barrier, depth - 1 + plane - 1 + groups * sides)

    def near_copy(offset, k):
        slot = (1 - offset) * groups + g
        return pltpu.make_async_remote_copy(
            src_ref=normal_ref.at[0:27],
            dst_ref=near.at[slot, 0:27],
            send_sem=near_s.at[0],
            recv_sem=near_r.at[0],
            device_id={"tm": t + offset, "grp": peer_grp(k)},
            device_id_type=MESH,
        )

    def each_near(do):
        for k in range(1, groups):
            do(0, k)

        @pl.when(has_before)
        def _():
            for k in reversed(range(groups)):
                do(-1, k)

        @pl.when(has_after)
        def _():
            for k in reversed(range(groups)):
                do(1, k)

    def drain_near(sem):
        inside = jnp.logical_and(has_before, has_after)

        @pl.when(inside)
        def _():
            drain(att.at[0 : 27 * (3 * groups - 1)], sem)

        @pl.when(jnp.logical_not(inside))
        def _():
            drain(att.at[0 : 27 * (2 * groups - 1)], sem)

    each_near(lambda offset, k: near_copy(offset, k).start())

    loaded(2)
    place = 0
    for a, b in pairs_of(CPAR):
        cal[place * tiles : (place + 1) * tiles, :] = weights * cp_ref[a] * cp_ref[b]
        place += 1
    cal[place * tiles :, :] = jnp.zeros(((UNIT_ROWS - place) * tiles, LANES), F32)
    global_rows = fold_slots(
        [
            jnp.sum(weights * gp_ref[a] * gp_ref[b], axis=0, keepdims=True)
            for a, b in pairs_of(GPAR)
        ],
        slots,
    )
    acc_cal[...] = jnp.zeros_like(acc_cal)

    def bin_units(no, carry):
        tile = no * 2
        units = two_rows(ci_ref, tile)
        upper, lower = lax.shift_right_logical(units, 8), lax.bitwise_and(units, 255)
        lhs = jnp.concatenate(
            [
                by_high(piece.astype(F32), upper)
                for piece in split_two(two_tiles(cal, tile, UNIT_ROWS, tiles))
            ],
            axis=0,
        )
        acc_cal[...] = acc_cal[...] + dot_nt(lhs, one_hot(lower, LOW))
        return carry

    lax.fori_loop(0, tiles // 2, bin_units, 0, unroll=6)
    lo_rows = UNIT_ROWS * (UNITS // LOW)
    for b_, at, h, start in block_pieces(blocks):
        row = h * UNIT_ROWS
        mats_ref[b_, 0:UNIT_ROWS, at : at + LANES] = (
            acc_cal[row : row + UNIT_ROWS, start : start + LANES]
            + acc_cal[lo_rows + row : lo_rows + row + UNIT_ROWS, start : start + LANES]
        )
    if mats_rows > UNIT_ROWS:
        mats_ref[:, UNIT_ROWS:, :] = jnp.zeros((blocks, mats_rows - UNIT_ROWS, width), F32)
    for b_ in range(blocks):
        for no, pieces in enumerate(global_rows):
            for j, piece in enumerate(pieces):
                mats_ref[b_, PAIRS + no : PAIRS + no + 1, j * LANES : (j + 1) * LANES] = piece

    def to_owners(source, target, recv):
        def copy(k):
            p = partner(block, k, blocks)
            pltpu.make_async_remote_copy(
                src_ref=source.at[p],
                dst_ref=target.at[m],
                send_sem=sent.at[0],
                recv_sem=recv.at[0],
                device_id=member(2 * p + 1),
                device_id_type=MESH,
            ).start()

        for k in reversed(range(1, blocks)):
            copy(k)

        @pl.when(follower)
        def _():
            copy(0)

        @pl.when(owner)
        def _():
            target[m] = source[block]

    def to_levels(target, recv, chosen):
        for k in range(depth):
            @pl.when(chosen(k))
            def _():
                pltpu.make_async_remote_copy(
                    src_ref=target.at[z],
                    dst_ref=target.at[z],
                    send_sem=sent.at[0],
                    recv_sem=recv.at[0],
                    device_id={"tm": k * inner + i, "grp": g},
                    device_id_type=MESH,
                ).start()

    def other(k):
        return z != k

    def late(k):
        return z - k > 1 if k else z < 0

    def soon(k):
        return jnp.logical_and(other(k), jnp.logical_not(late(k)))

    def slots_total(buffer, number):
        out = buffer[0]
        for k in range(1, number):
            out = out + buffer[k]
        return out

    to_owners(mats_ref, pmat, pmat_r)
    for no in range(tiles // 2):
        unit_spots[no] = one_hot(
            lax.bitwise_and(two_rows(ci_ref, no * 2), LANES - 1), LANES
        )
    near[groups + g] = normal_ref[...]

    @pl.when(jnp.logical_not(has_before))
    def _():
        near[0:groups] = jnp.zeros((groups, NORMAL_ROWS, LANES), F32)

    @pl.when(jnp.logical_not(has_after))
    def _():
        near[2 * groups :] = jnp.zeros((groups, NORMAL_ROWS, LANES), F32)

    drain_near(near_r.at[0])
    sums = []
    for s in range(3):
        part = near[s * groups]
        for q in range(1, groups):
            part = part + near[s * groups + q]
        sums.append(part)
    lane = lax.broadcasted_iota(jnp.int32, (NORMAL_ROWS, LANES), 1)
    before = pltpu.roll(sums[0], (HALO - nodes_dev) % LANES, 1)
    own = pltpu.roll(sums[1], HALO, 1)
    after = pltpu.roll(sums[2], (HALO + nodes_dev) % LANES, 1)
    end = nodes_dev + HALO
    normals = (
        own
        + jnp.where((lane >= 3) & (lane < HALO + 3), before, 0.0)
        + jnp.where((lane >= end) & (lane < end + HALO), after, 0.0)
    )
    spot = lax.broadcasted_iota(jnp.int32, (1, LANES), 1)
    exists = (spot >= jnp.where(has_before, 0, HALO)) & (
        spot < jnp.where(has_after, LANES, end)
    )
    normals = jnp.where(exists, normals, 0.0)
    index = {}
    for position, (a, b) in enumerate(pairs_of(3)):
        index[a, b] = index[b, a] = position
    band = [[normals[d * 6 + p : d * 6 + p + 1, :] for p in range(6)] for d in range(4)]
    right = [normals[24 + c : 25 + c, :] for c in range(3)]
    lower, inverse = cholesky_lists(symmetric(band[0], 3), 3)

    low = [
        [inverse[0]],
        [-lower[1][0] * inverse[0] * inverse[1], inverse[1]],
        [None, -lower[2][1] * inverse[1] * inverse[2], inverse[2]],
    ]
    low[2][0] = -(lower[2][0] * low[0][0] + lower[2][1] * low[1][0]) * inverse[2]
    damped = {}
    for a, b in pairs_of(3):
        entry = tree_sum([low[k][a] * low[k][b] for k in range(b, 3)])
        damped[a, b] = damped[b, a] = OMEGA * entry

    def precondition(vector):
        return [tree_sum([damped[a, b] * vector[b] for b in range(3)]) for a in range(3)]

    turned = [
        pltpu.roll(normals[d * 6 : (d + 1) * 6], d, 1) if d else None for d in range(4)
    ]
    behind = [
        [turned[d][p : p + 1, :] for p in range(6)] if d else None for d in range(4)
    ]
    x = precondition(right)
    for _ in range(1, ATT_SWEEPS):
        out = [
            right[a] - x[a] - tree_sum([band[0][index[a, b]] * x[b] for b in range(3)])
            for a in range(3)
        ]
        terms = [[] for _ in range(3)]
        for d in range(1, 4):
            ahead = [pltpu.roll(x[c], LANES - d, 1) for c in range(3)]
            back = [pltpu.roll(x[c], d, 1) for c in range(3)]
            for a in range(3):
                for b in range(3):
                    terms[a].append(band[d][index[a, b]] * ahead[b])
                    terms[a].append(behind[d][index[a, b]] * back[b])
        out = [out[a] - tree_sum(terms[a]) for a in range(3)]
        change = precondition(out)
        x = [jnp.where(exists, x[c] + change[c], 0.0) for c in range(3)]

    local = kn_ref[...] - base + HALO
    tables = [jnp.broadcast_to(x[c], (tiles, LANES)) for c in range(3)]
    second = first
    for i_ in range(4):
        moved = ap_ref[0] * lane_pick(tables[0], local + i_)
        for c in range(1, 3):
            moved = moved + ap_ref[c] * lane_pick(tables[c], local + i_)
        second = second - basis[i_] * moved
    out_ref[...] = second
    weighted = weights * second
    for a in range(CPAR):
        rcal[a * tiles : (a + 1) * tiles, :] = weighted * cp_ref[a]
    global_rows = fold_slots(
        [jnp.sum(weighted * gp_ref[a], axis=0, keepdims=True) for a in range(GPAR)], 2
    )
    unit_rows = lax.broadcasted_iota(jnp.int32, (CPAR * parts, 2 * LANES), 0)
    level_of_row = lax.rem(unit_rows, parts)
    acc = None
    for no in range(tiles // 2):
        tile = no * 2
        upper = lax.shift_right_logical(two_rows(ci_ref, tile), 7)
        value = None
        for c in range(CPAR):
            row = jnp.concatenate(
                [
                    rcal[c * tiles + tile : c * tiles + tile + 1, :],
                    rcal[c * tiles + tile + 1 : c * tiles + tile + 2, :],
                ],
                axis=1,
            )
            row = jnp.broadcast_to(row, (CPAR * parts, 2 * LANES))
            value = row if c == 0 else jnp.where(unit_rows >= c * parts, row, value)
        lhs = jnp.concatenate(
            [
                jnp.where(level_of_row + b_ * parts == upper, piece.astype(F32), 0.0)
                for piece in split_two(value)
                for b_ in range(blocks)
            ],
            axis=0,
        ).astype(BF16)
        part = dot_nt(lhs, unit_spots[no])
        acc = part if acc is None else acc + part
    rows = CPAR * parts
    total = acc[0 : blocks * rows, :] + acc[blocks * rows :, :]
    for b_ in range(blocks):
        rhs_ref[b_, 0:rows, :] = total[b_ * rows : (b_ + 1) * rows, :]
        for no, pieces in enumerate(global_rows):
            rhs_ref[b_, rows + no : rows + no + 1, :] = pieces[0]
        first_free = rows + len(global_rows)
        if first_free < rhs_rows:
            rhs_ref[b_, first_free:, :] = jnp.zeros((rhs_rows - first_free, LANES), F32)
    to_owners(rhs_ref, prhs, prhs_r)

    for c in range(3):
        scaled = lower[c][c] * x[c]
        for k in range(c + 1, 3):
            scaled = scaled + lower[k][c] * x[k]
        moved = pltpu.roll(scaled, LANES - HALO, 1)
        step_ref[c : c + 1, :] = moved[:, 0:nodes_dev]

    def spread(source, target, recv, shared):
        for p in reversed(range(1, plane)):
            to = partner(m, p, plane)
            pltpu.make_async_remote_copy(
                src_ref=source,
                dst_ref=target.at[block],
                send_sem=sent.at[0],
                recv_sem=recv.at[0 if shared else p // 2],
                device_id=member(to),
                device_id_type=MESH,
            ).start()

    @pl.when(owner)
    def _():
        drain(pmat.at[0 : plane - 1], pmat_r.at[0])
        zmat[z] = slots_total(pmat, plane)
        to_levels(zmat, zmat_r, soon)

        drain(prhs.at[0 : plane - 1], prhs_r.at[0])
        zrhs[z] = slots_total(prhs, plane)
        to_levels(zrhs, zrhs_r, other)
        to_levels(zmat, zmat_r, late)

        drain(zmat.at[0 : depth - 1], zmat_r.at[0])
        unit_total = slots_total(zmat, depth)
        matrix = [unit_total[p : p + 1, :] for p in range(PAIRS)]
        lower, inverse = cholesky_lists(symmetric(matrix, CPAR), CPAR)
        upper_g = [
            slot_sum(unit_total, PAIRS, p, slots) for p in range(GPAR * (GPAR + 1) // 2)
        ]
        lower_g, inverse_g = cholesky_lists(symmetric(upper_g, GPAR), GPAR)

        drain(zrhs.at[0 : depth - 1], zrhs_r.at[0])
        total = slots_total(zrhs, depth)
        right = [
            jnp.concatenate(
                [total[c * parts + j : c * parts + j + 1, :] for j in range(parts)], axis=1
            )
            for c in range(CPAR)
        ]
        white = solve_lower(lower, inverse, right)
        solved = solve_upper(lower, inverse, white)
        for c in range(CPAR):
            for j in range(parts):
                row = c * parts + j
                solved_ref[row : row + 1, :] = solved[c][:, j * LANES : (j + 1) * LANES]
        spread(solved_ref, solved_all, solved_r, False)
        for c in range(CPAR):
            for j in range(parts):
                row = c * parts + j
                white_ref[row : row + 1, :] = white[c][:, j * LANES : (j + 1) * LANES]
        right_g = [slot_sum(total, CPAR * parts, c, 2) for c in range(GPAR)]
        white_g = solve_lower(lower_g, inverse_g, right_g)
        solved_g = solve_upper(lower_g, inverse_g, white_g)
        spot = lax.broadcasted_iota(jnp.int32, (1, LANES), 1)
        packed = jnp.zeros((1, LANES), F32)
        for c in range(GPAR):
            packed = jnp.where(spot == c, white_g[c], packed)
            packed = jnp.where(spot == GPAR + c, solved_g[c], packed)
        white_ref[CPAR * parts : CPAR * parts + 1, :] = packed
        spread(white_ref, white_all, white_r, True)
        solved_all[block] = solved_ref[...]
        white_all[block] = white_ref[...]

    units = ci_ref[...]
    high, low = lax.shift_right_logical(units, 7), lax.bitwise_and(units, 127)
    slices = [(at, min(8, tiles - at)) for at in range(0, tiles, 8)]
    highs = [high[at : at + size] for at, size in slices]
    lows = [low[at : at + size] for at, size in slices]
    picked = [[jnp.zeros((size, LANES), F32) for _, size in slices] for _ in range(CPAR)]
    for k in range(blocks):
        source = partner(block, k, blocks)
        if k:
            drain(solved_ref, solved_r.at[k])
        else:
            @pl.when(follower)
            def _():
                drain(solved_ref, solved_r.at[0])
        for n, (_, size) in enumerate(slices):
            for j in range(parts):
                here = highs[n] == source * parts + j
                for c in range(CPAR):
                    row = c * parts + j
                    table = jnp.broadcast_to(
                        solved_all[source, row : row + 1, :], (size, LANES)
                    )
                    picked[c][n] = jnp.where(here, lane_pick(table, lows[n]), picked[c][n])
    picked = [jnp.concatenate(rows, axis=0) for rows in picked]
    out = out_ref[...]
    for c in range(CPAR):
        out = out - cp_ref[c] * picked[c]

    @pl.when(owner)
    def _():
        drain(white_all.at[0 : blocks - 1], white_r.at[0])

    @pl.when(follower)
    def _():
        drain(white_all, white_r.at[0])

    for b_ in range(blocks):
        for c in range(CPAR):
            for j in range(parts):
                start = b_ * width + j * LANES
                row = c * parts + j
                cstep_ref[c : c + 1, start : start + LANES] = white_all[b_, row : row + 1, :]
    packed = white_all[0, CPAR * parts : CPAR * parts + 1, :]
    glob_ref[...] = packed[:, 0:GPAR]
    for c in range(GPAR):
        value = packed[:, GPAR + c : GPAR + c + 1]
        out = out - gp_ref[c] * jnp.broadcast_to(value, (1, LANES))
    out_ref[...] = out
    drain_near(near_s.at[0])
    size = width // LANES * mats_rows + rhs_rows

    @pl.when(owner)
    def _():
        ready = 2 * CPAR * parts + 1
        drain(
            att.at[0 : (blocks - 1 + depth - 1) * size + (plane - 1) * ready], sent.at[0]
        )

    @pl.when(follower)
    def _():
        drain(att.at[0 : blocks * size], sent.at[0])


def final_kernel(*refs):
    half = len(refs) // 2
    copies = [
        pltpu.make_async_copy(refs[no], refs[half + no], refs[-1].at[no]) for no in range(half)
    ]
    for copy in copies:
        copy.start()
    for copy in copies:
        copy.wait()


def per_device(
    shape, residual, weight, source_part, source_index, source_delta, attitude_part,
    spline_phase, knot_index, calib_part, calib_index, global_part,
):
    count, groups, inner = shape
    plane, blocks, width, slots, mats_rows, rhs_rows, parts = layout(shape)
    depth = count // inner
    row_count = residual.shape[-1]
    tiles = row_count // TILE
    nodes_dev = tiles * KPT

    def flat(value):
        return value.reshape(tiles, TILE)

    def deep(value):
        return value.reshape(value.shape[0], -1, LANES)

    args = (
        flat(residual), flat(weight), deep(source_part), flat(source_index),
        deep(source_delta), deep(attitude_part), flat(spline_phase), flat(knot_index),
        deep(calib_part), flat(calib_index), deep(global_part),
    )

    def vmem(*dims):
        return pltpu.VMEM(dims, F32)

    dma = pltpu.SemaphoreType.DMA
    results = pl.pallas_call(
        functools.partial(step_kernel, shape, nodes_dev),
        out_shape=(
            vmem(tiles, LANES), vmem(3, nodes_dev), vmem(CPAR, UNITS), vmem(1, GPAR),
        ),
        scratch_shapes=[pltpu.VMEM(arg.shape, arg.dtype) for arg in args] + [
            vmem(tiles, LANES),
            vmem(ATT_ROWS * tiles, LANES),
            vmem(LANES, LANES),
            pltpu.VMEM((tiles // 2, LANES, 2 * LANES), BF16),
            vmem(UNIT_ROWS * tiles, LANES),
            vmem(CPAR * tiles, LANES),
            vmem(ATT_ROWS, LANES),
            vmem(2 * UNIT_ROWS * (UNITS // LOW), LOW),
            vmem(NORMAL_ROWS, LANES),
            vmem(blocks, mats_rows, width),
            vmem(blocks, rhs_rows, LANES),
            vmem(3 * groups, NORMAL_ROWS, LANES),
            vmem(plane, mats_rows, width),
            vmem(plane, rhs_rows, LANES),
            vmem(depth, mats_rows, width),
            vmem(depth, rhs_rows, LANES),
            vmem(CPAR * parts, LANES),
            vmem(blocks, CPAR * parts, LANES),
            vmem(CPAR * parts + 1, LANES),
            vmem(blocks, CPAR * parts + 1, LANES),
            dma((3,)), dma((1,)), dma((1,)), dma((1,)),
            dma((1,)), dma((1,)), dma((1,)), dma((1,)),
            dma((blocks,)), dma((1,)),
        ],
        in_specs=[pl.BlockSpec(memory_space=pl.ANY)] * len(args),
        compiler_params=pltpu.CompilerParams(collective_id=0, has_side_effects=True),
        name="step",
    )(*args)
    final, attitude_out, calib_step, global_step = pl.pallas_call(
        final_kernel,
        out_shape=tuple(jax.ShapeDtypeStruct(value.shape, F32) for value in results),
        in_specs=[pl.BlockSpec(memory_space=pltpu.VMEM)] * len(results),
        out_specs=(pl.BlockSpec(memory_space=pltpu.HBM),) * len(results),
        scratch_shapes=[dma((len(results),))],
        name="final",
    )(*[pltpu.with_memory_space_constraint(value, pltpu.VMEM) for value in results])
    return final.reshape(residual.shape), attitude_out, calib_step, global_step.reshape(GPAR)


def solution(mesh):
    count, groups = mesh.shape["tm"], mesh.shape["grp"]
    inner = 1 << (int(math.log2(count)) // 2)
    return jax.shard_map(
        functools.partial(per_device, (count, groups, inner)),
        mesh=mesh,
        in_specs=(
            P("tm", "grp", None),
            P("tm", "grp", None),
            P(None, "tm", "grp", None),
            P("tm", "grp", None),
            P(None, "tm", None),
            P(None, "tm", "grp", None),
            P("tm", "grp", None),
            P("tm", "grp", None),
            P(None, "tm", "grp", None),
            P("tm", "grp", None),
            P(None, "tm", "grp", None),
        ),
        out_specs=(P("tm", "grp", None), P(None, "tm"), P(), P()),
        check_vma=False,
    )
```

```python
import functools
import math

import jax
import jax.numpy as jnp
from jax import lax
from jax.experimental import pallas as pl
from jax.experimental.pallas import tpu as pltpu
from jax.sharding import PartitionSpec as P

TILE = 128
KPT = 4
UNITS = 2048
CPAR = 6
GPAR = 4
ATT_SWEEPS = 4

OMEGA = 0.6
RIDGE = 1.0
LANES = 128
LOW = 256
HALO = 3 * ATT_SWEEPS
MESH = pl.DeviceIdType.MESH
F32 = jnp.float32
BF16 = jnp.bfloat16

ATT_ROWS = 72
UNIT_ROWS = 24
PAIRS = CPAR * (CPAR + 1) // 2
HALF = 64
NORMAL_ROWS = 32


def pairs_of(extent):
    return [(a, b) for a in range(extent) for b in range(a, extent)]


def lane_pick(table, index):
    return lax.gather(
        table,
        index[..., None],
        lax.GatherDimensionNumbers(
            offset_dims=(),
            collapsed_slice_dims=(1,),
            start_index_map=(1,),
            operand_batching_dims=(0,),
            start_indices_batching_dims=(0,),
        ),
        (1, 1),
        mode=lax.GatherScatterMode.PROMISE_IN_BOUNDS,
    )


def spline_basis(phase):
    inverse = 1.0 - phase
    square = phase * phase
    cubed = square * phase
    return [
        inverse * inverse * inverse / 6.0,
        (3.0 * cubed - 6.0 * square + 4.0) / 6.0,
        (-3.0 * cubed + 3.0 * square + 3.0 * phase + 1.0) / 6.0,
        cubed / 6.0,
    ]


def cholesky_lists(matrix, extent):
    lower = [[None] * extent for _ in range(extent)]
    inverse = [None] * extent
    for column in range(extent):
        pivot = matrix[column][column]
        for k in range(column):
            pivot = pivot - lower[column][k] * lower[column][k]
        root = jnp.sqrt(pivot)
        lower[column][column] = root
        inverse[column] = 1.0 / root
        for row in range(column + 1, extent):
            entry = matrix[row][column]
            for k in range(column):
                entry = entry - lower[row][k] * lower[column][k]
            lower[row][column] = entry * inverse[column]
    return lower, inverse


def tree_sum(values):
    while len(values) > 1:
        values = [
            values[k] + values[k + 1] if k + 1 < len(values) else values[k]
            for k in range(0, len(values), 2)
        ]
    return values[0]


def solve_lower(lower, inverse, vector):
    result = []
    for row in range(len(vector)):
        running = vector[row]
        for k in range(row):
            running = running - lower[row][k] * result[k]
        result.append(running * inverse[row])
    return result


def solve_upper(lower, inverse, vector):
    extent = len(vector)
    result = [None] * extent
    for row in reversed(range(extent)):
        running = vector[row]
        for k in range(row + 1, extent):
            running = running - lower[k][row] * result[k]
        result[row] = running * inverse[row]
    return result


def symmetric(upper, extent):
    matrix = [[None] * extent for _ in range(extent)]
    for position, (a, b) in enumerate(pairs_of(extent)):
        value = upper[position] + (RIDGE if a == b else 0.0)
        matrix[a][b] = value
        matrix[b][a] = value
    return matrix


def split_two(value):
    first = value.astype(BF16)
    return [first, (value - first.astype(F32)).astype(BF16)]


def dot_nt(left, right):
    return lax.dot_general(
        left, right, (((1,), (1,)), ((), ())), preferred_element_type=F32
    )


def two_tiles(ref, tile, rows, tiles):
    return jnp.concatenate(
        [ref[pl.ds(tile, rows, stride=tiles), :], ref[pl.ds(tile + 1, rows, stride=tiles), :]],
        axis=1,
    )


def two_rows(ref, tile):
    return jnp.concatenate([ref[pl.ds(tile, 1), :], ref[pl.ds(tile + 1, 1), :]], axis=1)


def one_hot(row, extent):
    spots = lax.broadcasted_iota(jnp.int32, (extent, row.shape[1]), 0)
    return jnp.where(spots == row, 1.0, 0.0).astype(BF16)


def by_high(part, high):
    return jnp.concatenate(
        [jnp.where(high == h, part, 0.0) for h in range(UNITS // LOW)], axis=0
    ).astype(BF16)


def block_pieces(blocks):
    width = UNITS // blocks
    for piece in range(UNITS // LANES):
        unit = piece * LANES
        yield unit // width, unit % width, unit // LOW, unit % LOW


def round_up(value, unit):
    return -(-value // unit) * unit


def layout(shape):
    count, groups, inner = shape
    plane = groups * inner
    blocks = plane // 2
    width = UNITS // blocks
    slots = width // HALF
    mats_rows = round_up(PAIRS + -(-(GPAR * (GPAR + 1) // 2) // slots), 8)
    parts = width // LANES
    rhs_rows = CPAR * parts + -(-GPAR // 2)
    return plane, blocks, width, slots, mats_rows, rhs_rows, parts


def partner(place, k, size):
    if size & (size - 1):
        return lax.rem(place + k, size)
    other, bit = place, 1
    while bit < size:
        if k & bit:
            other = other + bit - 2 * bit * lax.rem(lax.div(place, bit), 2)
        bit *= 2
    return other


def fold_slots(rows, slots):
    lane = lax.broadcasted_iota(jnp.int32, (1, LANES), 1)
    folded = [row + pltpu.roll(row, HALF, 1) for row in rows]
    folded.append(jnp.zeros((1, LANES), F32))
    packed = []
    for start in range(0, len(rows), slots):
        parts = []
        for k in range(start, start + slots, 2):
            left, right = folded[min(k, len(rows))], folded[min(k + 1, len(rows))]
            parts.append(jnp.where(lane < HALF, left, right))
        packed.append(parts)
    return packed


def slot_sum(table, first_row, no, slots):
    row, at = first_row + no // slots, no % slots
    start = (at // 2) * LANES
    lane = lax.broadcasted_iota(jnp.int32, (1, LANES), 1)
    half = (lane < HALF) if at % 2 == 0 else (lane >= HALF)
    values = jnp.where(half, table[row : row + 1, start : start + LANES], 0.0)
    return jnp.broadcast_to(jnp.sum(values, axis=1, keepdims=True), (1, LANES))


def step_kernel(
    shape, nodes_dev,
    res_h, w_h, sp_h, si_h, sd_h, ap_h, ph_h, kn_h, cp_h, ci_h, gp_h,
    out_ref, step_ref, cstep_ref, glob_ref,
    res_ref, w_ref, sp_ref, si_ref, sd_ref, ap_ref, ph_ref, kn_ref, cp_ref, ci_ref, gp_ref,
    first_ref, att, by_node, unit_spots, cal, rcal, acc_att, acc_cal,
    normal_ref, mats_ref, rhs_ref,
    near, pmat, prhs, zmat, zrhs, solved_ref, solved_all, white_ref, white_all,
    load_s, near_s, near_r, sent, pmat_r, prhs_r, zmat_r, zrhs_r, solved_r, white_r,
):
    count, groups, inner = shape
    plane, blocks, width, slots, mats_rows, rhs_rows, parts = layout(shape)
    depth = count // inner
    t, g = lax.axis_index("tm"), lax.axis_index("grp")
    has_before, has_after = t > 0, t < count - 1
    z, i = lax.div(t, inner), lax.rem(t, inner)
    m = g * inner + i
    block = lax.div(m, 2)
    owner = lax.rem(m, 2) == 1
    follower = jnp.logical_not(owner)

    pairs = [
        (si_h, si_ref), (sd_h, sd_ref), (sp_h, sp_ref), (res_h, res_ref), (w_h, w_ref),
        (ap_h, ap_ref), (ph_h, ph_ref), (kn_h, kn_ref), (cp_h, cp_ref), (ci_h, ci_ref),
        (gp_h, gp_ref),
    ]
    stages = [pairs[:4], pairs[4:8], pairs[8:]]
    loads = [
        pltpu.make_async_copy(source, target, load_s.at[no])
        for no, stage in enumerate(stages)
        for source, target in stage
    ]
    for load in loads:
        load.start()

    def drain(ref, sem):
        pltpu.make_async_copy(ref, ref, sem).wait()

    def loaded(no):
        size = sum(math.prod(target.shape) for _, target in stages[no]) // LANES
        drain(att.at[0:size], load_s.at[no])

    def peer_grp(k):
        return lax.rem(g + k, groups)

    def member(p):
        return {"tm": z * inner + lax.rem(p, inner), "grp": lax.div(p, inner)}

    def level(k):
        return {"tm": partner(z, k, depth) * inner + i, "grp": g}

    barrier = pltpu.get_barrier_semaphore()

    def greet(where):
        pl.semaphore_signal(barrier, inc=1, device_id=where, device_id_type=MESH)

    for k in range(1, depth):
        greet(level(k))

    @pl.when(has_before)
    def _():
        for k in range(groups):
            greet({"tm": t - 1, "grp": peer_grp(k)})

    @pl.when(has_after)
    def _():
        for k in range(groups):
            greet({"tm": t + 1, "grp": peer_grp(k)})

    for k in range(1, plane):
        greet(member(partner(m, k, plane)))

    loaded(0)
    loaded(1)
    tiles = res_ref.shape[0]
    source_rows = sd_ref.shape[1]
    table = jnp.concatenate(
        split_two(sd_ref[...].reshape(5 * source_rows, LANES)), axis=1
    )
    for tile in range(0, tiles, 2):
        sources = two_rows(si_ref, tile)
        high, low = lax.shift_right_logical(sources, 7), lax.bitwise_and(sources, 127)
        spots = one_hot(low, LANES)
        found = jnp.dot(
            table, jnp.concatenate([spots, spots], axis=0), preferred_element_type=F32
        )
        total = None
        for c in range(5):
            factor = jnp.concatenate(
                [sp_ref[c, tile : tile + 1, :], sp_ref[c, tile + 1 : tile + 2, :]], axis=1
            )
            term = found[c * source_rows : (c + 1) * source_rows, :] * factor
            total = term if total is None else total + term
        levels = lax.broadcasted_iota(jnp.int32, (source_rows, 2 * LANES), 0)
        total = jnp.sum(jnp.where(levels == high, total, 0.0), axis=0, keepdims=True)
        first_ref[tile : tile + 1, :] = res_ref[tile : tile + 1, :] - total[:, :LANES]
        first_ref[tile + 1 : tile + 2, :] = res_ref[tile + 1 : tile + 2, :] - total[:, LANES:]
    weights = w_ref[...]
    first = first_ref[...]
    basis = spline_basis(ph_ref[...])
    axes = [ap_ref[c] for c in range(3)]
    products = [weights * axes[a] * axes[b] for a, b in pairs_of(3)]
    rights = [weights * axes[a] * first for a in range(3)]
    place = 0
    for i_ in range(4):
        for d in range(4 - i_):
            both = basis[i_] * basis[i_ + d]
            for product in products:
                att[place * tiles : (place + 1) * tiles, :] = both * product
                place += 1
    for i_ in range(4):
        for right in rights:
            att[place * tiles : (place + 1) * tiles, :] = basis[i_] * right
            place += 1
    base = t * (tiles * KPT)
    by_node[...] = jnp.zeros_like(by_node)
    for tile in range(0, tiles, 2):
        spots = one_hot(two_rows(kn_ref, tile) - (base + tile * KPT), 16)
        part = None
        for piece in split_two(two_tiles(att, tile, ATT_ROWS, tiles)):
            term = dot_nt(spots, piece)
            part = term if part is None else part + term
        by_node[tile * KPT : (tile + 2) * KPT, 0:ATT_ROWS] = part[0 : 2 * KPT, :]
    acc_att[...] = jnp.transpose(by_node[...])[0:ATT_ROWS, :]
    band = [None] * 5
    place = 0
    for i_ in range(4):
        for d in list(range(4 - i_)):
            rows = acc_att[place : place + 6, :]
            rows = pltpu.roll(rows, i_, 1) if i_ else rows
            band[d] = rows if band[d] is None else band[d] + rows
            place += 6
    for i_ in range(4):
        rows = acc_att[place : place + 3, :]
        rows = pltpu.roll(rows, i_, 1) if i_ else rows
        band[4] = rows if band[4] is None else band[4] + rows
        place += 3
    for d in range(4):
        normal_ref[d * 6 : (d + 1) * 6, :] = band[d]
    normal_ref[24:27, :] = band[4]
    normal_ref[27:, :] = jnp.zeros((NORMAL_ROWS - 27, LANES), F32)
    sides = has_before.astype(jnp.int32) + has_after.astype(jnp.int32)
    pl.semaphore_wait(barrier, depth - 1 + plane - 1 + groups * sides)

    def near_copy(offset, k):
        slot = (1 - offset) * groups + g
        return pltpu.make_async_remote_copy(
            src_ref=normal_ref.at[0:27],
            dst_ref=near.at[slot, 0:27],
            send_sem=near_s.at[0],
            recv_sem=near_r.at[0],
            device_id={"tm": t + offset, "grp": peer_grp(k)},
            device_id_type=MESH,
        )

    def each_near(do):
        for k in range(1, groups):
            do(0, k)

        @pl.when(has_before)
        def _():
            for k in reversed(range(groups)):
                do(-1, k)

        @pl.when(has_after)
        def _():
            for k in reversed(range(groups)):
                do(1, k)

    def drain_near(sem):
        inside = jnp.logical_and(has_before, has_after)

        @pl.when(inside)
        def _():
            drain(att.at[0 : 27 * (3 * groups - 1)], sem)

        @pl.when(jnp.logical_not(inside))
        def _():
            drain(att.at[0 : 27 * (2 * groups - 1)], sem)

    each_near(lambda offset, k: near_copy(offset, k).start())

    loaded(2)
    place = 0
    for a, b in pairs_of(CPAR):
        cal[place * tiles : (place + 1) * tiles, :] = weights * cp_ref[a] * cp_ref[b]
        place += 1
    cal[place * tiles :, :] = jnp.zeros(((UNIT_ROWS - place) * tiles, LANES), F32)
    global_rows = fold_slots(
        [
            jnp.sum(weights * gp_ref[a] * gp_ref[b], axis=0, keepdims=True)
            for a, b in pairs_of(GPAR)
        ],
        slots,
    )
    acc_cal[...] = jnp.zeros_like(acc_cal)

    def bin_units(no, carry):
        tile = no * 2
        units = two_rows(ci_ref, tile)
        upper, lower = lax.shift_right_logical(units, 8), lax.bitwise_and(units, 255)
        lhs = jnp.concatenate(
            [
                by_high(piece.astype(F32), upper)
                for piece in split_two(two_tiles(cal, tile, UNIT_ROWS, tiles))
            ],
            axis=0,
        )
        acc_cal[...] = acc_cal[...] + dot_nt(lhs, one_hot(lower, LOW))
        return carry

    lax.fori_loop(0, tiles // 2, bin_units, 0, unroll=6)
    lo_rows = UNIT_ROWS * (UNITS // LOW)
    for b_, at, h, start in block_pieces(blocks):
        row = h * UNIT_ROWS
        mats_ref[b_, 0:UNIT_ROWS, at : at + LANES] = (
            acc_cal[row : row + UNIT_ROWS, start : start + LANES]
            + acc_cal[lo_rows + row : lo_rows + row + UNIT_ROWS, start : start + LANES]
        )
    if mats_rows > UNIT_ROWS:
        mats_ref[:, UNIT_ROWS:, :] = jnp.zeros((blocks, mats_rows - UNIT_ROWS, width), F32)
    for b_ in range(blocks):
        for no, pieces in enumerate(global_rows):
            for j, piece in enumerate(pieces):
                mats_ref[b_, PAIRS + no : PAIRS + no + 1, j * LANES : (j + 1) * LANES] = piece

    def to_owners(source, target, recv):
        def copy(k):
            p = partner(block, k, blocks)
            pltpu.make_async_remote_copy(
                src_ref=source.at[p],
                dst_ref=target.at[m],
                send_sem=sent.at[0],
                recv_sem=recv.at[0],
                device_id=member(2 * p + 1),
                device_id_type=MESH,
            ).start()

        for k in reversed(range(1, blocks)):
            copy(k)

        @pl.when(follower)
        def _():
            copy(0)

        @pl.when(owner)
        def _():
            target[m] = source[block]

    def to_levels(target, recv, chosen):
        for k in range(depth):
            @pl.when(chosen(k))
            def _():
                pltpu.make_async_remote_copy(
                    src_ref=target.at[z],
                    dst_ref=target.at[z],
                    send_sem=sent.at[0],
                    recv_sem=recv.at[0],
                    device_id={"tm": k * inner + i, "grp": g},
                    device_id_type=MESH,
                ).start()

    def other(k):
        return z != k

    def late(k):
        return z - k > 1 if k else z < 0

    def soon(k):
        return jnp.logical_and(other(k), jnp.logical_not(late(k)))

    def slots_total(buffer, number):
        out = buffer[0]
        for k in range(1, number):
            out = out + buffer[k]
        return out

    to_owners(mats_ref, pmat, pmat_r)
    for no in range(tiles // 2):
        unit_spots[no] = one_hot(
            lax.bitwise_and(two_rows(ci_ref, no * 2), LANES - 1), LANES
        )
    near[groups + g] = normal_ref[...]

    @pl.when(jnp.logical_not(has_before))
    def _():
        near[0:groups] = jnp.zeros((groups, NORMAL_ROWS, LANES), F32)

    @pl.when(jnp.logical_not(has_after))
    def _():
        near[2 * groups :] = jnp.zeros((groups, NORMAL_ROWS, LANES), F32)

    drain_near(near_r.at[0])
    sums = []
    for s in range(3):
        part = near[s * groups]
        for q in range(1, groups):
            part = part + near[s * groups + q]
        sums.append(part)
    lane = lax.broadcasted_iota(jnp.int32, (NORMAL_ROWS, LANES), 1)
    before = pltpu.roll(sums[0], (HALO - nodes_dev) % LANES, 1)
    own = pltpu.roll(sums[1], HALO, 1)
    after = pltpu.roll(sums[2], (HALO + nodes_dev) % LANES, 1)
    end = nodes_dev + HALO
    normals = (
        own
        + jnp.where((lane >= 3) & (lane < HALO + 3), before, 0.0)
        + jnp.where((lane >= end) & (lane < end + HALO), after, 0.0)
    )
    spot = lax.broadcasted_iota(jnp.int32, (1, LANES), 1)
    exists = (spot >= jnp.where(has_before, 0, HALO)) & (
        spot < jnp.where(has_after, LANES, end)
    )
    normals = jnp.where(exists, normals, 0.0)
    index = {}
    for position, (a, b) in enumerate(pairs_of(3)):
        index[a, b] = index[b, a] = position
    band = [[normals[d * 6 + p : d * 6 + p + 1, :] for p in range(6)] for d in range(4)]
    right = [normals[24 + c : 25 + c, :] for c in range(3)]
    lower, inverse = cholesky_lists(symmetric(band[0], 3), 3)

    low = [
        [inverse[0]],
        [-lower[1][0] * inverse[0] * inverse[1], inverse[1]],
        [None, -lower[2][1] * inverse[1] * inverse[2], inverse[2]],
    ]
    low[2][0] = -(lower[2][0] * low[0][0] + lower[2][1] * low[1][0]) * inverse[2]
    damped = {}
    for a, b in pairs_of(3):
        entry = tree_sum([low[k][a] * low[k][b] for k in range(b, 3)])
        damped[a, b] = damped[b, a] = OMEGA * entry

    def precondition(vector):
        return [tree_sum([damped[a, b] * vector[b] for b in range(3)]) for a in range(3)]

    turned = [
        pltpu.roll(normals[d * 6 : (d + 1) * 6], d, 1) if d else None for d in range(4)
    ]
    behind = [
        [turned[d][p : p + 1, :] for p in range(6)] if d else None for d in range(4)
    ]
    x = precondition(right)
    for _ in range(1, ATT_SWEEPS):
        out = [
            right[a] - x[a] - tree_sum([band[0][index[a, b]] * x[b] for b in range(3)])
            for a in range(3)
        ]
        terms = [[] for _ in range(3)]
        for d in range(1, 4):
            ahead = [pltpu.roll(x[c], LANES - d, 1) for c in range(3)]
            back = [pltpu.roll(x[c], d, 1) for c in range(3)]
            for a in range(3):
                for b in range(3):
                    terms[a].append(band[d][index[a, b]] * ahead[b])
                    terms[a].append(behind[d][index[a, b]] * back[b])
        out = [out[a] - tree_sum(terms[a]) for a in range(3)]
        change = precondition(out)
        x = [jnp.where(exists, x[c] + change[c], 0.0) for c in range(3)]

    local = kn_ref[...] - base + HALO
    tables = [jnp.broadcast_to(x[c], (tiles, LANES)) for c in range(3)]
    second = first
    for i_ in range(4):
        moved = ap_ref[0] * lane_pick(tables[0], local + i_)
        for c in range(1, 3):
            moved = moved + ap_ref[c] * lane_pick(tables[c], local + i_)
        second = second - basis[i_] * moved
    out_ref[...] = second
    weighted = weights * second
    for a in range(CPAR):
        rcal[a * tiles : (a + 1) * tiles, :] = weighted * cp_ref[a]
    global_rows = fold_slots(
        [jnp.sum(weighted * gp_ref[a], axis=0, keepdims=True) for a in range(GPAR)], 2
    )
    unit_rows = lax.broadcasted_iota(jnp.int32, (CPAR * parts, 2 * LANES), 0)
    level_of_row = lax.rem(unit_rows, parts)
    acc = None
    for no in range(tiles // 2):
        tile = no * 2
        upper = lax.shift_right_logical(two_rows(ci_ref, tile), 7)
        value = None
        for c in range(CPAR):
            row = jnp.concatenate(
                [
                    rcal[c * tiles + tile : c * tiles + tile + 1, :],
                    rcal[c * tiles + tile + 1 : c * tiles + tile + 2, :],
                ],
                axis=1,
            )
            row = jnp.broadcast_to(row, (CPAR * parts, 2 * LANES))
            value = row if c == 0 else jnp.where(unit_rows >= c * parts, row, value)
        lhs = jnp.concatenate(
            [
                jnp.where(level_of_row + b_ * parts == upper, piece.astype(F32), 0.0)
                for piece in split_two(value)
                for b_ in range(blocks)
            ],
            axis=0,
        ).astype(BF16)
        part = dot_nt(lhs, unit_spots[no])
        acc = part if acc is None else acc + part
    rows = CPAR * parts
    total = acc[0 : blocks * rows, :] + acc[blocks * rows :, :]
    for b_ in range(blocks):
        rhs_ref[b_, 0:rows, :] = total[b_ * rows : (b_ + 1) * rows, :]
        for no, pieces in enumerate(global_rows):
            rhs_ref[b_, rows + no : rows + no + 1, :] = pieces[0]
        first_free = rows + len(global_rows)
        if first_free < rhs_rows:
            rhs_ref[b_, first_free:, :] = jnp.zeros((rhs_rows - first_free, LANES), F32)
    to_owners(rhs_ref, prhs, prhs_r)

    for c in range(3):
        scaled = lower[c][c] * x[c]
        for k in range(c + 1, 3):
            scaled = scaled + lower[k][c] * x[k]
        moved = pltpu.roll(scaled, LANES - HALO, 1)
        step_ref[c : c + 1, :] = moved[:, 0:nodes_dev]

    def spread(source, target, recv, shared):
        for k in range(plane):
            slot = 0 if shared else partner(block, k // 2, blocks)

            @pl.when(m != k)
            def _():
                pltpu.make_async_remote_copy(
                    src_ref=source,
                    dst_ref=target.at[block],
                    send_sem=sent.at[0],
                    recv_sem=recv.at[slot],
                    device_id={"tm": z * inner + k % inner, "grp": k // inner},
                    device_id_type=MESH,
                ).start()

    @pl.when(owner)
    def _():
        drain(pmat.at[0 : plane - 1], pmat_r.at[0])
        zmat[z] = slots_total(pmat, plane)
        to_levels(zmat, zmat_r, soon)

        drain(prhs.at[0 : plane - 1], prhs_r.at[0])
        zrhs[z] = slots_total(prhs, plane)
        to_levels(zrhs, zrhs_r, other)
        to_levels(zmat, zmat_r, late)

        drain(zmat.at[0 : depth - 1], zmat_r.at[0])
        unit_total = slots_total(zmat, depth)
        matrix = [unit_total[p : p + 1, :] for p in range(PAIRS)]
        lower, inverse = cholesky_lists(symmetric(matrix, CPAR), CPAR)
        upper_g = [
            slot_sum(unit_total, PAIRS, p, slots) for p in range(GPAR * (GPAR + 1) // 2)
        ]
        lower_g, inverse_g = cholesky_lists(symmetric(upper_g, GPAR), GPAR)

        drain(zrhs.at[0 : depth - 1], zrhs_r.at[0])
        total = slots_total(zrhs, depth)
        right = [
            jnp.concatenate(
                [total[c * parts + j : c * parts + j + 1, :] for j in range(parts)], axis=1
            )
            for c in range(CPAR)
        ]
        white = solve_lower(lower, inverse, right)
        solved = solve_upper(lower, inverse, white)
        for c in range(CPAR):
            for j in range(parts):
                row = c * parts + j
                solved_ref[row : row + 1, :] = solved[c][:, j * LANES : (j + 1) * LANES]
        spread(solved_ref, solved_all, solved_r, False)
        for c in range(CPAR):
            for j in range(parts):
                row = c * parts + j
                white_ref[row : row + 1, :] = white[c][:, j * LANES : (j + 1) * LANES]
        right_g = [slot_sum(total, CPAR * parts, c, 2) for c in range(GPAR)]
        white_g = solve_lower(lower_g, inverse_g, right_g)
        solved_g = solve_upper(lower_g, inverse_g, white_g)
        spot = lax.broadcasted_iota(jnp.int32, (1, LANES), 1)
        packed = jnp.zeros((1, LANES), F32)
        for c in range(GPAR):
            packed = jnp.where(spot == c, white_g[c], packed)
            packed = jnp.where(spot == GPAR + c, solved_g[c], packed)
        white_ref[CPAR * parts : CPAR * parts + 1, :] = packed
        spread(white_ref, white_all, white_r, True)
        solved_all[block] = solved_ref[...]
        white_all[block] = white_ref[...]

    units = ci_ref[...]
    high, low = lax.shift_right_logical(units, 7), lax.bitwise_and(units, 127)
    slices = [(at, min(8, tiles - at)) for at in range(0, tiles, 8)]
    highs = [high[at : at + size] for at, size in slices]
    lows = [low[at : at + size] for at, size in slices]
    picked = [[jnp.zeros((size, LANES), F32) for _, size in slices] for _ in range(CPAR)]
    for k in range(blocks):
        source = partner(block, k, blocks)
        if k:
            drain(solved_ref, solved_r.at[k])
        else:
            @pl.when(follower)
            def _():
                drain(solved_ref, solved_r.at[0])
        for n, (_, size) in enumerate(slices):
            for j in range(parts):
                here = highs[n] == source * parts + j
                for c in range(CPAR):
                    row = c * parts + j
                    table = jnp.broadcast_to(
                        solved_all[source, row : row + 1, :], (size, LANES)
                    )
                    picked[c][n] = jnp.where(here, lane_pick(table, lows[n]), picked[c][n])
    picked = [jnp.concatenate(rows, axis=0) for rows in picked]
    out = out_ref[...]
    for c in range(CPAR):
        out = out - cp_ref[c] * picked[c]

    @pl.when(owner)
    def _():
        drain(white_all.at[0 : blocks - 1], white_r.at[0])

    @pl.when(follower)
    def _():
        drain(white_all, white_r.at[0])

    for b_ in range(blocks):
        for c in range(CPAR):
            for j in range(parts):
                start = b_ * width + j * LANES
                row = c * parts + j
                cstep_ref[c : c + 1, start : start + LANES] = white_all[b_, row : row + 1, :]
    packed = white_all[0, CPAR * parts : CPAR * parts + 1, :]
    glob_ref[...] = packed[:, 0:GPAR]
    for c in range(GPAR):
        value = packed[:, GPAR + c : GPAR + c + 1]
        out = out - gp_ref[c] * jnp.broadcast_to(value, (1, LANES))
    out_ref[...] = out
    drain_near(near_s.at[0])
    size = width // LANES * mats_rows + rhs_rows

    @pl.when(owner)
    def _():
        ready = 2 * CPAR * parts + 1
        drain(
            att.at[0 : (blocks - 1 + depth - 1) * size + (plane - 1) * ready], sent.at[0]
        )

    @pl.when(follower)
    def _():
        drain(att.at[0 : blocks * size], sent.at[0])


def final_kernel(*refs):
    half = len(refs) // 2
    copies = [
        pltpu.make_async_copy(refs[no], refs[half + no], refs[-1].at[no]) for no in range(half)
    ]
    for copy in copies:
        copy.start()
    for copy in copies:
        copy.wait()


def per_device(
    shape, residual, weight, source_part, source_index, source_delta, attitude_part,
    spline_phase, knot_index, calib_part, calib_index, global_part,
):
    count, groups, inner = shape
    plane, blocks, width, slots, mats_rows, rhs_rows, parts = layout(shape)
    depth = count // inner
    row_count = residual.shape[-1]
    tiles = row_count // TILE
    nodes_dev = tiles * KPT

    def flat(value):
        return value.reshape(tiles, TILE)

    def deep(value):
        return value.reshape(value.shape[0], -1, LANES)

    args = (
        flat(residual), flat(weight), deep(source_part), flat(source_index),
        deep(source_delta), deep(attitude_part), flat(spline_phase), flat(knot_index),
        deep(calib_part), flat(calib_index), deep(global_part),
    )

    def vmem(*dims):
        return pltpu.VMEM(dims, F32)

    dma = pltpu.SemaphoreType.DMA
    results = pl.pallas_call(
        functools.partial(step_kernel, shape, nodes_dev),
        out_shape=(
            vmem(tiles, LANES), vmem(3, nodes_dev), vmem(CPAR, UNITS), vmem(1, GPAR),
        ),
        scratch_shapes=[pltpu.VMEM(arg.shape, arg.dtype) for arg in args] + [
            vmem(tiles, LANES),
            vmem(ATT_ROWS * tiles, LANES),
            vmem(LANES, LANES),
            pltpu.VMEM((tiles // 2, LANES, 2 * LANES), BF16),
            vmem(UNIT_ROWS * tiles, LANES),
            vmem(CPAR * tiles, LANES),
            vmem(ATT_ROWS, LANES),
            vmem(2 * UNIT_ROWS * (UNITS // LOW), LOW),
            vmem(NORMAL_ROWS, LANES),
            vmem(blocks, mats_rows, width),
            vmem(blocks, rhs_rows, LANES),
            vmem(3 * groups, NORMAL_ROWS, LANES),
            vmem(plane, mats_rows, width),
            vmem(plane, rhs_rows, LANES),
            vmem(depth, mats_rows, width),
            vmem(depth, rhs_rows, LANES),
            vmem(CPAR * parts, LANES),
            vmem(blocks, CPAR * parts, LANES),
            vmem(CPAR * parts + 1, LANES),
            vmem(blocks, CPAR * parts + 1, LANES),
            dma((3,)), dma((1,)), dma((1,)), dma((1,)),
            dma((1,)), dma((1,)), dma((1,)), dma((1,)),
            dma((blocks,)), dma((1,)),
        ],
        in_specs=[pl.BlockSpec(memory_space=pl.ANY)] * len(args),
        compiler_params=pltpu.CompilerParams(collective_id=0, has_side_effects=True),
        name="step",
    )(*args)
    final, attitude_out, calib_step, global_step = pl.pallas_call(
        final_kernel,
        out_shape=tuple(jax.ShapeDtypeStruct(value.shape, F32) for value in results),
        in_specs=[pl.BlockSpec(memory_space=pltpu.VMEM)] * len(results),
        out_specs=(pl.BlockSpec(memory_space=pltpu.HBM),) * len(results),
        scratch_shapes=[dma((len(results),))],
        name="final",
    )(*[pltpu.with_memory_space_constraint(value, pltpu.VMEM) for value in results])
    return final.reshape(residual.shape), attitude_out, calib_step, global_step.reshape(GPAR)


def solution(mesh):
    count, groups = mesh.shape["tm"], mesh.shape["grp"]
    inner = 1 << (int(math.log2(count)) // 2)
    return jax.shard_map(
        functools.partial(per_device, (count, groups, inner)),
        mesh=mesh,
        in_specs=(
            P("tm", "grp", None),
            P("tm", "grp", None),
            P(None, "tm", "grp", None),
            P("tm", "grp", None),
            P(None, "tm", None),
            P(None, "tm", "grp", None),
            P("tm", "grp", None),
            P("tm", "grp", None),
            P(None, "tm", "grp", None),
            P("tm", "grp", None),
            P(None, "tm", "grp", None),
        ),
        out_specs=(P("tm", "grp", None), P(None, "tm"), P(), P()),
        check_vma=False,
    )
```
